32 devices in a mesh: section: 2 (over core), dp: 4 (over z), tensor: 4 (over y, x).
Axes of the slice: x: 2, y: 2, z: 4, core: 2. Of those that a mesh axis runs over, the one named last changes fastest.
Arguments:
- inputs: bfloat16 [2, 512, 4096], P(None, 'dp', 'tensor'), may hold values from -6 to 6
- adapter_down: bfloat16 [2, 4096, 128], P('section', 'tensor'), may hold values from -0.09375 to 0.09375
- adapter_up: bfloat16 [2, 128, 4096], P('section', None, 'tensor'), may hold values from -0.5 to 0.5
- gains: bfloat16 [2, 4096], P('section', 'tensor'), may hold values from 0.25 to 1.75
- head: bfloat16 [4096, 128], P('tensor'), may hold values from -0.375 to 0.375
- labels: int32 [2, 512], P(None, 'dp'), may hold values from 0 to 127
- valid: int32 [2, 512], P(None, 'dp'), may hold values from 0 to 1, as said below
Outputs:
- grads_down: float32 [2, 4096, 128], P('section', 'tensor', 'dp')
- grads_up: float32 [2, 128, 4096], P('section', 'dp', 'tensor')
- grads_gain: float32 [2, 4096], P('section', 'tensor')
The draws below stay inside these ranges and needn't reach their ends.
Inputs may be any that keep to these rules, and one draw needn't show every extreme that they name: In each microbatch the first of every 128 consecutive tokens is valid.
All inputs are finite; a program needn't handle non-finite values.
Results may differ from the reference program's by a relative error of at most 0.015.
Values may be sent and summed in bfloat16 or wider, within the bound.
No kernel may reach another device: no remote copies, remote signals or barrier semaphores. Data moves between devices by JAX's collectives and lax.ppermute only.
A program may use at most 64 MiB of HBM per device.

```python
import jax
import jax.numpy as jnp
from jax import lax

D = 4096
RANK = 128
LABELS = 128
TOK_DEV = 128
MICRO = 2
SECTIONS = 2
TOKENS = 512


def draw_valid(key, part):
    column = jnp.arange(TOKENS, dtype=jnp.int32)
    replica = column // TOK_DEV
    groups = TOKENS // TOK_DEV
    threshold = 256 + 512 * replica // max(groups - 1, 1)
    random_bits = jax.random.randint(key, (MICRO, TOKENS), 0, 1024, dtype=jnp.int32)
    chosen = (random_bits < threshold[None, :]) | (column % TOK_DEV == 0)[None, :]
    return chosen.astype(jnp.int32)


def with_ends(values, stream_key, smallest, top_value):
    spot = [jax.random.randint(jax.random.fold_in(stream_key, axis), (), 0, length) for axis, length in enumerate(values.shape)]
    main_axis = values.shape.index(max(values.shape))
    beside = spot[:main_axis] + [(spot[main_axis] + 1) % values.shape[main_axis]] + spot[main_axis + 1:]
    return values.at[tuple(spot)].set(smallest).at[tuple(beside)].set(top_value)


def block_levels(own_key, dims, cuts, low, largest):
    gain = 1.0
    for axis_at, shards_of in cuts:
        steps = jax.random.uniform(jax.random.fold_in(jax.random.fold_in(own_key, 6), axis_at), (shards_of,), jnp.float32, low / len(cuts), largest / len(cuts))
        gain = gain * jnp.repeat(jnp.exp(steps), dims[axis_at] // shards_of).reshape((-1,) + (1,) * (len(dims) - 1 - axis_at))
    return gain


def centred(own_key, extent, width, reach, pieces=(), held_as=jnp.bfloat16):
    entries = jax.random.normal(own_key, extent, jnp.float32) * width
    if len(pieces) > 0:
        entries = block_levels(own_key, extent, pieces, -0.22, 0.18) * entries
    return jnp.clip(entries, min=-reach, max=reach).astype(held_as)


def setup_inputs(seed: int = 0) -> dict:
    key_list = jax.random.split(jax.random.key(seed), 8)
    inputs = centred(key_list[0], (MICRO, TOKENS, D), 1.0, 6.0, ((1, 4), (2, 4)))
    adapter_down = centred(key_list[1], (SECTIONS, D, RANK), D ** -0.5, 0.09375, ((0, 2), (1, 4)))
    adapter_up = centred(key_list[2], (SECTIONS, RANK, D), RANK ** -0.5, 0.5, ((0, 2), (2, 4)))
    gains = jnp.clip(1.0 + 0.15 * jax.random.normal(key_list[3], (SECTIONS, D), jnp.float32), 0.25, 1.75).astype(jnp.bfloat16)
    head = centred(key_list[4], (D, LABELS), (D // 16) ** -0.5, 0.375, ((0, 4),))
    labels = with_ends(jax.random.randint(key_list[5], (MICRO, TOKENS), 0, LABELS), jax.random.fold_in(key_list[5], 1), 0, LABELS - 1).astype(jnp.int32)
    valid = draw_valid(jax.random.fold_in(key_list[7], 71), 0)
    return dict(inputs=inputs, adapter_down=adapter_down, adapter_up=adapter_up, gains=gains, head=head, labels=labels, valid=valid)


epsilon = 1e-05

def layer_forward(inbound, gain_row, down_weight, up_weight):
    values = inbound.astype(jnp.float32)
    squares = lax.optimization_barrier(jnp.sum(values * values, axis=1))
    inverse = lax.rsqrt(squares / D + epsilon)
    scaled = (values * gain_row).astype(jnp.bfloat16)
    projected = jnp.dot(scaled, down_weight, preferred_element_type=jnp.float32)
    hidden = jax.nn.silu(inverse[:, None] * projected).astype(jnp.bfloat16)
    outbound = (values + jnp.dot(hidden, up_weight, preferred_element_type=jnp.float32)).astype(jnp.bfloat16)
    return (outbound, projected, inverse)

def head_backward(final_state, head, label_row, valid_row):
    values = final_state.astype(jnp.float32)
    squares = lax.optimization_barrier(jnp.sum(values * values, axis=1))
    inverse = lax.rsqrt(squares / D + epsilon)
    logit_base = jnp.dot(final_state, head, preferred_element_type=jnp.float32)
    logits = inverse[:, None] * logit_base
    shifted = logits - lax.optimization_barrier(jnp.max(logits, axis=1, keepdims=True))
    expo_terms = jnp.exp(shifted)
    softmax_prob = expo_terms / lax.optimization_barrier(jnp.sum(expo_terms, axis=1, keepdims=True))
    classes = lax.broadcasted_iota(jnp.int32, logits.shape, 1)
    onehot = (classes == label_row[:, None]).astype(jnp.float32)
    cotangent = (softmax_prob - onehot) * valid_row[:, None].astype(jnp.float32)
    radial = lax.optimization_barrier(jnp.sum(cotangent * logit_base, axis=1))
    weighted = (inverse[:, None] * cotangent).astype(jnp.bfloat16)
    back_term = jnp.dot(weighted, head.T, preferred_element_type=jnp.float32)
    result = back_term - (inverse ** 3 / D * radial)[:, None] * values
    return result.astype(jnp.bfloat16)

def layer_backward(cotangent, inbound, projected, inverse, gain_row, down_weight, up_weight):
    hidden_grad = jnp.dot(cotangent, up_weight.T, preferred_element_type=jnp.float32)
    pre_act = inverse[:, None] * projected
    sigmoid_val = jax.nn.sigmoid(pre_act)
    act_grad = hidden_grad * sigmoid_val * (1.0 + pre_act * (1.0 - sigmoid_val))
    radial = lax.optimization_barrier(jnp.sum(act_grad * projected, axis=1))
    weighted = (inverse[:, None] * act_grad).astype(jnp.bfloat16)
    scaled_grad = jnp.dot(weighted, down_weight.T, preferred_element_type=jnp.float32)
    values = inbound.astype(jnp.float32)
    outbound = (cotangent.astype(jnp.float32) + gain_row * scaled_grad - (inverse ** 3 / D * radial)[:, None] * values).astype(jnp.bfloat16)
    scaled = (values * gain_row).astype(jnp.bfloat16)
    hidden = jax.nn.silu(pre_act).astype(jnp.bfloat16)
    down_grad = jnp.dot(scaled.T, weighted, preferred_element_type=jnp.float32)
    up_grad = jnp.dot(hidden.T, cotangent, preferred_element_type=jnp.float32)
    gain_grad = lax.optimization_barrier(jnp.sum(scaled_grad * values, axis=0))
    return (outbound, down_grad, up_grad, gain_grad)

def reference(inputs, adapter_down, adapter_up, gains, head, labels, valid):
    down_sums = [jnp.zeros((D, RANK), jnp.float32) for layer in range(SECTIONS)]
    up_sums = [jnp.zeros((RANK, D), jnp.float32) for layer in range(SECTIONS)]
    gain_sums = [jnp.zeros((D,), jnp.float32) for layer in range(SECTIONS)]
    for micro_index in range(MICRO):
        state = inputs[micro_index]
        saved = []
        for layer in range(SECTIONS):
            outbound, projected, inverse = layer_forward(state, gains[layer].astype(jnp.float32), adapter_down[layer], adapter_up[layer])
            saved.append((state, projected, inverse))
            state = outbound
        cotangent = head_backward(state, head, labels[micro_index], valid[micro_index])
        for layer in reversed(range(SECTIONS)):
            inbound, projected, inverse = saved[layer]
            cotangent, down_grad, up_grad, gain_grad = layer_backward(cotangent, inbound, projected, inverse, gains[layer].astype(jnp.float32), adapter_down[layer], adapter_up[layer])
            down_sums[layer] = down_sums[layer] + down_grad
            up_sums[layer] = up_sums[layer] + up_grad
            gain_sums[layer] = gain_sums[layer] + gain_grad
    total_count = jnp.sum(valid.astype(jnp.float32))
    return (jnp.stack(down_sums) / total_count, jnp.stack(up_sums) / total_count, jnp.stack(gain_sums) / total_count)
```

```python
import jax
import jax.numpy as jnp
from jax import lax
from jax.sharding import PartitionSpec as P

epsilon = 1e-05
F32 = jnp.float32
BF16 = jnp.bfloat16


def dot(a, b):
    return jnp.dot(a, b, preferred_element_type=F32)


def dot_nt(a, b):
    return lax.dot_general(a, b, (((1,), (1,)), ((), ())), preferred_element_type=F32)


def dot_tn(a, b):
    return lax.dot_general(a, b, (((0,), (0,)), ((), ())), preferred_element_type=F32)


def partner_pairs(axis, step):
    size = lax.axis_size(axis)
    if size & (size - 1) == 0:
        return [(i, i ^ step) for i in range(size)]
    return [(i, (i + step) % size) for i in range(size)]


def from_all(value, axis):
    return [
        lax.ppermute(value, axis, partner_pairs(axis, step))
        for step in range(1, lax.axis_size(axis))
    ]


def high_low(value):
    high = value.astype(BF16)
    return high, (value - high.astype(F32)).astype(BF16)


def chain(width, squares, proj0, proj1, cross0, cross1, base, grams, labels, valid):
    m01, b0h, b0b0, b1h, b1b1, b0b1 = grams
    inv0 = lax.rsqrt(squares / width + epsilon)
    pre0 = inv0 * proj0
    sig0 = jax.nn.sigmoid(pre0)
    hidden0 = (pre0 * sig0).astype(BF16)
    hid0 = hidden0.astype(F32)
    one_b0 = cross0 + dot(hidden0, b0b0)
    squares1 = squares + jnp.sum(hid0 * (cross0 + one_b0), axis=1, keepdims=True)
    inv1 = lax.rsqrt(squares1 / width + epsilon)
    proj1 = proj1 + dot(hidden0, m01)
    pre1 = inv1 * proj1
    sig1 = jax.nn.sigmoid(pre1)
    hidden1 = (pre1 * sig1).astype(BF16)
    hid1 = hidden1.astype(F32)
    one_b1 = cross1 + dot(hidden0, b0b1)
    two_b0 = one_b0 + dot_nt(hidden1, b0b1)
    two_b1 = one_b1 + dot(hidden1, b1b1)
    squares2 = squares1 + jnp.sum(hid1 * (one_b1 + two_b1), axis=1, keepdims=True)
    inv2 = lax.rsqrt(squares2 / width + epsilon)
    base = base + dot(hidden0, b0h) + dot(hidden1, b1h)
    logits = inv2 * base
    expo = jnp.exp(logits - jnp.max(logits, axis=1, keepdims=True))
    prob = expo / jnp.sum(expo, axis=1, keepdims=True)
    classes = lax.broadcasted_iota(jnp.int32, logits.shape, 1)
    onehot = (classes == labels).astype(F32)
    cot = (prob - onehot) * valid.astype(F32)
    factor2 = inv2**3 / width * jnp.sum(cot * base, axis=1, keepdims=True)
    weighted2 = (inv2 * cot).astype(BF16)
    grad1 = dot_nt(weighted2, b1h) - factor2 * two_b1
    act1 = grad1 * sig1 * (1.0 + pre1 * (1.0 - sig1))
    factor1 = inv1**3 / width * jnp.sum(act1 * proj1, axis=1, keepdims=True)
    weighted1 = (inv1 * act1).astype(BF16)
    grad0 = dot_nt(weighted2, b0h) - factor2 * two_b0 + dot_nt(weighted1, m01) - factor1 * one_b0
    act0 = grad0 * sig0 * (1.0 + pre0 * (1.0 - sig0))
    weighted0 = (inv0 * act0).astype(BF16)
    scaled0 = ((factor2 + factor1) * hid0).astype(BF16)
    scaled1 = (factor2 * hid1).astype(BF16)
    return hidden0, hidden1, weighted0, weighted1, weighted2, scaled0, scaled1


def local(inputs, adapter_down, adapter_up, gains, head, labels, valid):
    sections, tensors, dps = (lax.axis_size(a) for a in ("section", "tensor", "dp"))
    first = lax.axis_index("section") == 0
    features = inputs.shape[2]
    width = features * tensors
    rank = adapter_down.shape[2]
    states = inputs.reshape(-1, features)
    rows = states.shape[0]
    half = rows // sections
    offset = lax.axis_index("section") * half
    gain = gains.astype(F32)
    down_t = adapter_down[0].T
    scaled_down = (down_t.astype(F32) * gain).astype(BF16)
    up = adapter_up[0]
    swap = partner_pairs("section", 1)

    own = jnp.concatenate([scaled_down, up], axis=0)
    other = lax.ppermute(own, "section", swap)
    third = jnp.where(first, other[:rank], other[rank:])
    mine = lax.dynamic_slice_in_dim(states, offset, half, 0)
    mine32 = mine.astype(F32)
    squares = jnp.sum(mine32 * mine32, axis=1)
    both = dot_nt(states, own)
    logit = dot(mine, head)
    gram = jnp.concatenate([dot_nt(up, third), dot(up, head), dot_nt(up, up)], axis=1)
    square_parts = jnp.stack(high_low(squares), axis=1)
    packed = jnp.concatenate(
        [
            both[:, :rank],
            both[:, rank:],
            logit,
            gram[:, :rank],
            gram[:, rank : 2 * rank],
            gram[:, 2 * rank :],
        ],
        axis=0,
    ).astype(BF16)
    wide = from_all(packed, "tensor")
    small = from_all(square_parts, "tensor")
    total = packed.astype(F32) + sum(w.astype(F32) for w in wide)
    squares = squares + sum(jnp.sum(s.astype(F32), axis=1) for s in small)
    proj, cross = total[:rows], total[rows : 2 * rows]
    logit = total[2 * rows : 2 * rows + half]
    gram = total[2 * rows + half :].astype(BF16)
    away = half - offset
    sent = jnp.concatenate(
        [
            lax.dynamic_slice_in_dim(proj, away, half, 0).astype(BF16),
            lax.dynamic_slice_in_dim(cross, away, half, 0).astype(BF16),
            gram,
        ],
        axis=0,
    )
    got = lax.ppermute(sent, "section", swap)
    own_proj = lax.dynamic_slice_in_dim(proj, offset, half, 0)
    own_cross = lax.dynamic_slice_in_dim(cross, offset, half, 0)
    got_proj, got_cross = got[:half].astype(F32), got[half : 2 * half].astype(F32)
    got_gram = got[2 * half :]

    def ordered(a, b):
        return jnp.where(first, a, b), jnp.where(first, b, a)

    proj0, proj1 = ordered(own_proj, got_proj)
    cross0, cross1 = ordered(own_cross, got_cross)
    gram0, gram1 = ordered(gram, got_gram)
    m01, b0h, b0b0 = jnp.split(gram0, 3, axis=0)
    b1b0, b1h, b1b1 = jnp.split(gram1, 3, axis=0)
    label_rows = lax.dynamic_slice_in_dim(labels.reshape(-1, 1), offset, half, 0)
    valid_rows = lax.dynamic_slice_in_dim(valid.reshape(-1, 1), offset, half, 0)
    hidden0, hidden1, weighted0, weighted1, weighted2, scaled0, scaled1 = chain(
        width,
        squares[:, None],
        proj0,
        proj1,
        cross0,
        cross1,
        logit,
        (m01, b0h, b0b0, b1h, b1b1, b1b0.T),
        label_rows,
        valid_rows,
    )
    made = jnp.stack([hidden0, hidden1, weighted0, weighted1, weighted2, scaled0, scaled1])
    met = lax.ppermute(made, "section", swap)
    front, back = ordered(made, met)
    hidden0, hidden1, weighted0, weighted1, weighted2, scaled0, scaled1 = jnp.concatenate(
        [front, back], axis=1
    )
    own_hidden = jnp.where(first, hidden0, hidden1)
    own_weighted = jnp.where(first, weighted0, weighted1)
    own_scaled = jnp.where(first, scaled0, scaled1)
    up0 = jnp.where(first, up, other[rank:])
    up1 = jnp.where(first, other[rank:], up)
    zero = jnp.zeros((rank, rank), BF16)
    mix_down = jnp.where(first, zero, dot_tn(weighted1, hidden0).astype(BF16))
    down_grad = dot_tn(own_weighted, states) + dot(mix_down, up0)
    gain_grad = jnp.sum(down_grad * down_t.astype(F32), axis=0)
    mix_head = dot_tn(own_hidden, weighted2).astype(BF16)
    mix_up0 = dot_tn(own_scaled, hidden0).astype(BF16)
    mix_up1 = jnp.where(first, dot_tn(hidden0, scaled1), dot_tn(scaled1, hidden1)).astype(BF16)
    mix_down1 = jnp.where(first, dot_tn(hidden0, weighted1).astype(BF16), zero)
    up_grad = (
        dot_nt(mix_head, head)
        - dot_tn(own_scaled, states)
        - dot(mix_up0, up0)
        - dot(mix_up1, up1)
        + dot(mix_down1, other[:rank])
    )
    down_grad = down_grad * gain
    count = jnp.sum(valid.astype(F32))
    slim = rank // dps
    tail = jnp.stack([*high_low(gain_grad), *high_low(jnp.broadcast_to(count, gain_grad.shape))])
    index = lax.axis_index("dp")
    parts = jnp.concatenate(
        [down_grad.reshape(dps, slim, features), up_grad.reshape(dps, slim, features)], axis=1
    )
    summed = lax.dynamic_index_in_dim(parts, index, 0, keepdims=False)
    parts = parts.astype(BF16)
    gain_sum, count_sum = gain_grad, count
    for step in range(1, dps):
        pairs = partner_pairs("dp", step)
        target = jnp.array([t for _, t in sorted(pairs)])[index]
        part = lax.dynamic_index_in_dim(parts, target, 0, keepdims=False)
        got = lax.ppermute(jnp.concatenate([part, tail], axis=0), "dp", pairs).astype(F32)
        summed = summed + got[: 2 * slim]
        gain_sum = gain_sum + got[2 * slim] + got[2 * slim + 1]
        count_sum = count_sum + got[2 * slim + 2, 0] + got[2 * slim + 3, 0]
    scale = 1.0 / count_sum
    summed = summed * scale
    return summed[:slim].T[None], summed[slim:][None], (gain_sum * scale)[None]


def solution(mesh):
    return jax.shard_map(
        local,
        mesh=mesh,
        in_specs=(
            P(None, "dp", "tensor"),
            P("section", "tensor", None),
            P("section", None, "tensor"),
            P("section", "tensor"),
            P("tensor", None),
            P(None, "dp"),
            P(None, "dp"),
        ),
        out_specs=(
            P("section", "tensor", "dp"),
            P("section", "dp", "tensor"),
            P("section", "tensor"),
        ),
        check_vma=False,
    )
```

```python
import functools

import jax
import jax.numpy as jnp
from jax import lax
from jax.experimental import pallas as pl
from jax.experimental.pallas import tpu as pltpu
from jax.sharding import PartitionSpec as P

epsilon = 1e-05
F32 = jnp.float32
BF16 = jnp.bfloat16
PACK = 16


def dot(a, b):
    return jnp.dot(a, b, preferred_element_type=F32)


def dot_nt(a, b):
    return lax.dot_general(a, b, (((1,), (1,)), ((), ())), preferred_element_type=F32)


def dot_tn(a, b):
    return lax.dot_general(a, b, (((0,), (0,)), ((), ())), preferred_element_type=F32)


def rows_of(start, count):
    return pl.ds(pl.multiple_of(start, count), count)


def transposed(value):
    return value.astype(F32).T.astype(value.dtype)


def partner(index, step, size):
    if size & (size - 1) == 0:
        return index ^ step
    return (index + step) % size


def from_partner(value, axis, step):
    size = lax.axis_size(axis)
    return lax.ppermute(value, axis, [(i, partner(i, step, size)) for i in range(size)])


def high_low(value):
    high = value.astype(BF16).astype(F32)
    return jnp.concatenate([high, value - high], axis=0).astype(BF16)


def call(kernel, out, flops, *args):
    moved = sum(a.size * a.dtype.itemsize for a in args)
    return pl.pallas_call(
        kernel,
        out_shape=out,
        cost_estimate=pl.CostEstimate(flops=flops, bytes_accessed=moved, transcendentals=0),
        compiler_params=pltpu.CompilerParams(vmem_limit_bytes=24 * 2**20),
    )(*args)


def project_kernel(x_ref, down_ref, up_ref, gain_ref, down2_ref, up2_ref, gain2_ref, head_ref, out_ref):
    half, rank = x_ref.shape[0], down_ref.shape[1]
    me = lax.axis_index("section")
    it = 1 - me
    x, up, up2, head = x_ref[...], up_ref[...], up2_ref[...], head_ref[...]
    x32 = x.astype(F32)
    gain, gain2 = gain_ref[...].astype(F32), gain2_ref[...].astype(F32)
    out_ref[rows_of(me * half, half), :] = dot((x32 * gain).astype(BF16), down_ref[...]).astype(BF16)
    out_ref[rows_of(it * half, half), :] = dot((x32 * gain2).astype(BF16), down2_ref[...]).astype(BF16)
    out_ref[rows_of((2 + me) * half, half), :] = dot_nt(x, up).astype(BF16)
    out_ref[rows_of((2 + it) * half, half), :] = dot_nt(x, up2).astype(BF16)
    out_ref[4 * half : 5 * half, :] = dot(x, head).astype(BF16)
    base = 5 * half

    @pl.when(me == 0)
    def _():
        scaled = (up.astype(F32) * gain2).astype(BF16)
        out_ref[base : base + rank, :] = dot(scaled, down2_ref[...]).astype(BF16)

    @pl.when(me != 0)
    def _():
        out_ref[base : base + rank, :] = dot_nt(up, up2).astype(BF16)

    out_ref[base + rank : base + 2 * rank, :] = dot(up, head).astype(BF16)
    out_ref[base + 2 * rank : base + 3 * rank, :] = dot_nt(up, up).astype(BF16)
    squares = jnp.sum(x32 * x32, axis=1, keepdims=True)
    squares = jnp.broadcast_to(squares, (half, rank)).T
    out_ref[base + 3 * rank :, :] = high_low(squares[: PACK // 2])


def prepare_kernel(down_ref, head_ref, down2_ref, up2_ref, gain2_ref, down_t_ref, head_t_ref, mixed_ref):
    down_t_ref[...] = transposed(down_ref[...])
    head_t_ref[...] = transposed(head_ref[...])
    me = lax.axis_index("section")

    @pl.when(me == 0)
    def _():
        mixed_ref[...] = (down2_ref[...].astype(F32).T * gain2_ref[...].astype(F32)).astype(BF16)

    @pl.when(me != 0)
    def _():
        mixed_ref[...] = up2_ref[...]


def chain_kernel(width, count, *refs):
    parts, (gram_ref, gram2_ref, label_ref, valid_ref, mine_ref, theirs_ref) = refs[:count], refs[count:]
    rank = gram_ref.shape[1]
    half = label_ref.shape[1]
    me = lax.axis_index("section")
    first = me == 0

    def total(start, size):
        return sum(r[start : start + size, :].astype(F32) for r in parts)

    def spread(row):
        return jnp.broadcast_to(row, (rank, half)).T

    gram, gram2 = gram_ref[...], gram2_ref[...]
    gram0, gram1 = jnp.where(first, gram, gram2), jnp.where(first, gram2, gram)
    m01, b0h, b0b0 = (gram0[i * rank : (i + 1) * rank] for i in range(3))
    b1b0, b1h, b1b1 = (gram1[i * rank : (i + 1) * rank] for i in range(3))
    tail = total(5 * half + 3 * rank, PACK)
    squares0 = spread(tail[:1] + tail[PACK // 2 : PACK // 2 + 1])
    inv0 = lax.rsqrt(squares0 / width + epsilon)
    proj0 = total(0, half)
    pre0 = inv0 * proj0
    sig0 = jax.nn.sigmoid(pre0)
    hidden0 = (pre0 * sig0).astype(BF16)
    hid0 = hidden0.astype(F32)
    proj1 = total(half, half) + dot(hidden0, m01)
    cross0 = total(2 * half, half)
    one_b0 = cross0 + dot(hidden0, b0b0)
    squares1 = squares0 + jnp.sum(hid0 * (cross0 + one_b0), axis=1, keepdims=True)
    inv1 = lax.rsqrt(squares1 / width + epsilon)
    pre1 = inv1 * proj1
    sig1 = jax.nn.sigmoid(pre1)
    hidden1 = (pre1 * sig1).astype(BF16)
    hid1 = hidden1.astype(F32)
    one_b1 = total(3 * half, half) + dot_nt(hidden0, b1b0)
    two_b0 = one_b0 + dot(hidden1, b1b0)
    two_b1 = one_b1 + dot(hidden1, b1b1)
    squares2 = squares1 + jnp.sum(hid1 * (one_b1 + two_b1), axis=1, keepdims=True)
    inv2 = lax.rsqrt(squares2 / width + epsilon)
    base = total(4 * half, half) + dot(hidden0, b0h) + dot(hidden1, b1h)
    logits = inv2 * base
    expo = jnp.exp(logits - jnp.max(logits, axis=1, keepdims=True))
    prob = expo / jnp.sum(expo, axis=1, keepdims=True)
    labels = spread(label_ref[pl.ds(me, 1), :].astype(F32))
    valid = spread(valid_ref[pl.ds(me, 1), :].astype(F32))
    classes = lax.broadcasted_iota(jnp.int32, logits.shape, 1).astype(F32)
    cot = (prob - (classes == labels).astype(F32)) * valid
    factor2 = inv2 * inv2 * inv2 / width * jnp.sum(cot * base, axis=1, keepdims=True)
    weighted2 = (inv2 * cot).astype(BF16)
    grad1 = dot_nt(weighted2, b1h) - factor2 * two_b1
    act1 = grad1 * sig1 * (1.0 + pre1 * (1.0 - sig1))
    factor1 = inv1 * inv1 * inv1 / width * jnp.sum(act1 * proj1, axis=1, keepdims=True)
    weighted1 = (inv1 * act1).astype(BF16)
    grad0 = dot_nt(weighted2, b0h) - factor2 * two_b0 + dot_nt(weighted1, m01) - factor1 * one_b0
    act0 = grad0 * sig0 * (1.0 + pre0 * (1.0 - sig0))
    weighted0 = (inv0 * act0).astype(BF16)
    scaled0 = ((factor2 + factor1) * hid0).astype(BF16)
    scaled1 = (factor2 * hid1).astype(BF16)
    front = (hidden0, weighted2, scaled0, weighted0, weighted1, scaled1)
    back = (hidden1, weighted2, scaled1, weighted1, hidden0, hidden0)
    for slot, (a, b) in enumerate(zip(front, back)):
        mine_ref[slot * half : (slot + 1) * half, :] = jnp.where(first, a, b)
        theirs_ref[slot * half : (slot + 1) * half, :] = jnp.where(first, b, a)


def mix_kernel(replicas, mine_ref, theirs_ref, *refs):
    out_refs, tall_ref, mix_ref = refs[:replicas], refs[replicas], refs[replicas + 1]
    rank = mine_ref.shape[1]
    half = mine_ref.shape[0] // 6
    slim = rank // replicas
    first = lax.axis_index("section") == 0
    mine, theirs = mine_ref[...], theirs_ref[...]
    front, back = jnp.where(first, mine, theirs), jnp.where(first, theirs, mine)
    hidden, last, scaled, weighted, extra1, extra2 = (
        [v[i * half : (i + 1) * half] for v in (front, back)] for i in range(6)
    )
    hidden_t, scaled_t, weighted_t = ([transposed(v) for v in s] for s in (hidden, scaled, weighted))

    def product(left, right):
        return sum(dot(a, b) for a, b in zip(left, right))

    left_oth = [jnp.where(first, a, b) for a, b in zip(hidden_t, scaled_t)]
    left_mix = [jnp.where(first, a, b) for a, b in zip(hidden_t, weighted_t)]
    mix = product(left_mix, extra1).astype(BF16)
    for slot, value in enumerate(
        (
            product(hidden_t, last).astype(BF16),
            (-product(scaled_t, hidden)).astype(BF16),
            (-product(left_oth, extra2)).astype(BF16),
            mix,
            weighted_t[0],
            weighted_t[1],
            scaled_t[0],
            scaled_t[1],
        )
    ):
        tall_ref[slot * rank : (slot + 1) * rank, :] = value
    mix_ref[:rank, :] = mix
    mix_ref[rank : 2 * rank, :] = weighted_t[0]
    mix_ref[2 * rank :, :] = weighted_t[1]
    me = lax.axis_index("dp")
    for step, out_ref in enumerate(out_refs):
        target = partner(me, step, replicas)
        for slot in range(8):
            out_ref[slot * slim : (slot + 1) * slim, :] = tall_ref[rows_of(slot * rank + target * slim, slim), :]


def gain_kernel(x_ref, mix_ref, part_ref, mixed_ref, down_t_ref, valid_ref, acc_ref, tail_ref):
    features = x_ref.shape[1]
    rank = mix_ref.shape[1]
    half = x_ref.shape[0] // 2
    slim = part_ref.shape[0] // 8
    first = lax.axis_index("section") == 0
    x0, x1 = x_ref[:half, :], x_ref[half:, :]
    mix = jnp.where(first, jnp.zeros((rank, rank), BF16), mix_ref[:rank, :])
    grad = dot(mix_ref[rank : 2 * rank, :], x0) + dot(mix_ref[2 * rank :, :], x1) + dot(mix, mixed_ref[...])
    gain = jnp.sum(grad * down_t_ref[...].astype(F32), axis=0, keepdims=True)
    gain = jnp.concatenate(
        [gain[:, i * rank : (i + 1) * rank] for i in range(features // rank)], axis=0
    )
    count = jnp.sum(valid_ref[...].astype(F32), keepdims=True)
    count = jnp.broadcast_to(count, (PACK // 2, rank))
    tail_ref[...] = jnp.concatenate([high_low(gain), high_low(count)], axis=0)
    accumulate(x0, x1, part_ref, slim, acc_ref)


def accumulate(x0, x1, part_ref, slim, acc_ref, before=None):
    for slot in (0, 1):
        start = (4 + 2 * slot) * slim
        value = dot(part_ref[start : start + slim, :], x0)
        value = value + dot(part_ref[start + slim : start + 2 * slim, :], x1)
        if before is not None:
            value = value + before[slot * slim : (slot + 1) * slim, :]
        acc_ref[slot * slim : (slot + 1) * slim, :] = value


def add_kernel(part_ref, own_ref, far_ref, before_ref, acc_ref):
    first = lax.axis_index("section") == 0
    own, far = own_ref[...], far_ref[...]
    x0, x1 = jnp.where(first, own, far), jnp.where(first, far, own)
    accumulate(x0, x1, part_ref, part_ref.shape[0] // 8, acc_ref, before_ref)


def last_kernel(replicas, *refs):
    parts, refs = refs[:replicas], refs[replicas:]
    tails, refs = refs[:replicas], refs[replicas:]
    acc_ref, head_t_ref, up_ref, up2_ref, mixed_ref, gain_ref, down_out, up_out, gain_out = refs
    slim = parts[0].shape[0] // 8
    rank = parts[0].shape[1]
    first = lax.axis_index("section") == 0
    tail = sum(t[...].astype(F32) for t in tails)
    lines = tail.shape[0] - PACK
    scale = 1.0 / (tail[lines : lines + 1, :1] + tail[lines + PACK // 2 : lines + PACK // 2 + 1, :1])
    gain = (tail[: lines // 2] + tail[lines // 2 : lines]) * scale
    for i in range(lines // 2):
        gain_out[:, i * rank : (i + 1) * rank] = gain[i : i + 1, :]
    head_mix, own_mix, oth_mix, mix = (
        sum(p[slot * slim : (slot + 1) * slim, :].astype(F32) for p in parts).astype(BF16) for slot in range(4)
    )
    mixed = dot(mix, mixed_ref[...])
    none = jnp.zeros_like(mixed)
    down = acc_ref[:slim, :] + jnp.where(first, none, mixed)
    down_out[...] = (down * gain_ref[...].astype(F32) * scale).T
    up = dot(head_mix, head_t_ref[...]) + dot(own_mix, up_ref[...]) + dot(oth_mix, up2_ref[...])
    up_out[...] = (up + jnp.where(first, mixed, none) - acc_ref[slim:, :]) * scale


def local(inputs, adapter_down, adapter_up, gains, head, labels, valid):
    sections, tensors, replicas = (lax.axis_size(a) for a in ("section", "tensor", "dp"))
    me = lax.axis_index("section")
    features = inputs.shape[2]
    width = features * tensors
    rank = adapter_down.shape[2]
    states = inputs.reshape(-1, features)
    half = states.shape[0] // sections
    assert sections == 2 and half == rank and head.shape[1] == rank and features % rank == 0
    slim = rank // replicas
    lines = features // rank
    down, up = adapter_down[0], adapter_up[0]
    labels, valid = labels.reshape(sections, half), valid.reshape(sections, half)
    shape = jax.ShapeDtypeStruct

    down2, up2, gains2 = (from_partner(v, "section", 1) for v in (down, up, gains))
    mine = lax.dynamic_slice_in_dim(states, me * half, half, 0)
    small = 2 * rank * rank * features
    packed = call(
        project_kernel,
        shape((5 * half + 3 * rank + PACK, rank), BF16),
        8 * small,
        mine, down, up, gains, down2, up2, gains2, head,
    )
    wide = [packed] + [from_partner(packed, "tensor", step) for step in range(1, tensors)]
    far = [from_partner(mine, "dp", step) for step in range(1, replicas)]
    down_t, head_t, mixed = call(
        prepare_kernel,
        [shape((rank, features), BF16)] * 3,
        small,
        down, head, down2, up2, gains2,
    )
    gram = sum(w[5 * half : 5 * half + 3 * rank].astype(F32) for w in wide).astype(BF16)
    gram2 = from_partner(gram, "section", 1)
    made, theirs = call(
        functools.partial(chain_kernel, width, tensors),
        [shape((6 * half, rank), BF16)] * 2,
        16 * 2 * half * rank * rank,
        *wide, gram, gram2, labels, valid,
    )
    met = from_partner(theirs, "section", 1)
    *parts, _, mix = call(
        functools.partial(mix_kernel, replicas),
        [shape((8 * slim, rank), BF16)] * replicas
        + [shape((8 * rank, rank), BF16), shape((3 * rank, rank), BF16)],
        16 * 2 * half * rank * rank,
        made, met,
    )
    parts = [parts[0]] + [from_partner(parts[step], "dp", step) for step in range(1, replicas)]
    acc, tail = call(
        gain_kernel,
        [shape((2 * slim, features), F32), shape((2 * lines + PACK, rank), BF16)],
        4 * small,
        states, mix, parts[0], mixed, down_t, valid,
    )
    tails = [tail] + [from_partner(tail, "dp", step) for step in range(1, replicas)]
    crossed = [from_partner(f, "section", 1) for f in far]
    for part, own, other in zip(parts[1:], far, crossed):
        acc = call(add_kernel, shape(acc.shape, F32), small, part, own, other, acc)
    return tuple(
        v[None] if v.shape[0] != 1 else v
        for v in call(
            functools.partial(last_kernel, replicas),
            [shape((features, slim), F32), shape((slim, features), F32), shape((1, features), F32)],
            4 * small,
            *parts, *tails, acc, head_t, up, up2, mixed, gains,
        )
    )


def solution(mesh):
    return jax.shard_map(
        local,
        mesh=mesh,
        in_specs=(
            P(None, "dp", "tensor"),
            P("section", "tensor", None),
            P("section", None, "tensor"),
            P("section", "tensor"),
            P("tensor", None),
            P(None, "dp"),
            P(None, "dp"),
        ),
        out_specs=(
            P("section", "tensor", "dp"),
            P("section", "dp", "tensor"),
            P("section", "tensor"),
        ),
        check_vma=False,
    )
```

```python
import functools

import jax
import jax.numpy as jnp
from jax import lax
from jax.experimental import pallas as pl
from jax.experimental.pallas import tpu as pltpu
from jax.sharding import PartitionSpec as P

epsilon = 1e-05
F32 = jnp.float32
BF16 = jnp.bfloat16
PACK = 16


def dot(a, b):
    return jnp.dot(a, b, preferred_element_type=F32)


def dot_nt(a, b):
    return lax.dot_general(a, b, (((1,), (1,)), ((), ())), preferred_element_type=F32)


def dot_tn(a, b):
    return lax.dot_general(a, b, (((0,), (0,)), ((), ())), preferred_element_type=F32)


def rows_of(start, count):
    return pl.ds(pl.multiple_of(start, count), count)


def transposed(value):
    return value.astype(F32).T.astype(value.dtype)


def partner(index, step, size):
    if size & (size - 1) == 0:
        return index ^ step
    return (index + step) % size


def from_partner(value, axis, step):
    size = lax.axis_size(axis)
    return lax.ppermute(value, axis, [(i, partner(i, step, size)) for i in range(size)])


def high_low(value):
    high = value.astype(BF16).astype(F32)
    return jnp.concatenate([high, value - high], axis=0).astype(BF16)


def call(kernel, out, flops, *args):
    moved = sum(a.size * a.dtype.itemsize for a in args)
    return pl.pallas_call(
        kernel,
        out_shape=out,
        cost_estimate=pl.CostEstimate(flops=flops, bytes_accessed=moved, transcendentals=0),
        compiler_params=pltpu.CompilerParams(vmem_limit_bytes=24 * 2**20),
    )(*args)


def gain_kernel(gain_ref, out_ref):
    out_ref[...] = gain_ref[...].astype(F32)


def own_kernel(x_ref, down_ref, up_ref, head_ref, gain_ref, out_ref):
    rank = down_ref.shape[1]
    half = x_ref.shape[0] // lax.axis_size("section")
    x, up, head = x_ref[rows_of(lax.axis_index("section") * half, half), :], up_ref[...], head_ref[...]
    x32 = x.astype(F32)
    scaled = (x32 * gain_ref[...]).astype(BF16)
    out_ref[:half, :] = dot(scaled, down_ref[...]).astype(BF16)
    out_ref[half : 2 * half, :] = dot_nt(x, up).astype(BF16)
    out_ref[2 * half : 3 * half, :] = dot(x, head).astype(BF16)
    out_ref[3 * half : 3 * half + rank, :] = dot(up, head).astype(BF16)
    out_ref[3 * half + rank : 3 * half + 2 * rank, :] = dot_nt(up, up).astype(BF16)
    squares = jnp.sum(x32 * x32, axis=1, keepdims=True)
    squares = jnp.broadcast_to(squares, (half, rank)).T
    out_ref[3 * half + 2 * rank :, :] = high_low(squares[: PACK // 2])


def other_kernel(x_ref, up_ref, own_ref, down2_ref, up2_ref, gain2_ref, out_ref):
    rank = down2_ref.shape[1]
    half = x_ref.shape[0] // lax.axis_size("section")
    me = lax.axis_index("section")
    it = 1 - me
    x = x_ref[rows_of(me * half, half), :]
    gain2 = gain2_ref[...].astype(F32)
    base = 5 * half
    out_ref[rows_of(me * half, half), :] = own_ref[:half, :]
    out_ref[rows_of((2 + me) * half, half), :] = own_ref[half : 2 * half, :]
    out_ref[4 * half : base, :] = own_ref[2 * half : 3 * half, :]
    out_ref[base + rank :, :] = own_ref[3 * half :, :]
    scaled = (x.astype(F32) * gain2).astype(BF16)
    out_ref[rows_of(it * half, half), :] = dot(scaled, down2_ref[...]).astype(BF16)
    out_ref[rows_of((2 + it) * half, half), :] = dot_nt(x, up2_ref[...]).astype(BF16)

    @pl.when(me == 0)
    def _():
        scaled = (up_ref[...].astype(F32) * gain2).astype(BF16)
        out_ref[base : base + rank, :] = dot(scaled, down2_ref[...]).astype(BF16)

    @pl.when(me != 0)
    def _():
        out_ref[base : base + rank, :] = dot_nt(up_ref[...], up2_ref[...]).astype(BF16)


def prepare_kernel(down_ref, head_ref, down2_ref, up2_ref, gain2_ref, down_t_ref, head_t_ref, mixed_ref):
    down_t_ref[...] = transposed(down_ref[...])
    head_t_ref[...] = transposed(head_ref[...])
    me = lax.axis_index("section")

    @pl.when(me == 0)
    def _():
        mixed_ref[...] = (down2_ref[...].astype(F32).T * gain2_ref[...].astype(F32)).astype(BF16)

    @pl.when(me != 0)
    def _():
        mixed_ref[...] = up2_ref[...]


def chain_kernel(width, count, *refs):
    parts, (gram_ref, gram2_ref, label_ref, valid_ref, mine_ref, theirs_ref) = refs[:count], refs[count:]
    rank = gram_ref.shape[1]
    half = label_ref.shape[1]
    me = lax.axis_index("section")
    first = me == 0

    def total(start, size):
        return sum(r[start : start + size, :].astype(F32) for r in parts)

    def spread(row):
        return jnp.broadcast_to(row, (rank, half)).T

    gram, gram2 = gram_ref[...], gram2_ref[...]
    gram0, gram1 = jnp.where(first, gram, gram2), jnp.where(first, gram2, gram)
    m01, b0h, b0b0 = (gram0[i * rank : (i + 1) * rank] for i in range(3))
    b1b0, b1h, b1b1 = (gram1[i * rank : (i + 1) * rank] for i in range(3))
    tail = total(5 * half + 3 * rank, PACK)
    squares0 = spread(tail[:1] + tail[PACK // 2 : PACK // 2 + 1])
    inv0 = lax.rsqrt(squares0 / width + epsilon)
    proj0 = total(0, half)
    pre0 = inv0 * proj0
    sig0 = jax.nn.sigmoid(pre0)
    hidden0 = (pre0 * sig0).astype(BF16)
    hid0 = hidden0.astype(F32)
    proj1 = total(half, half) + dot(hidden0, m01)
    cross0 = total(2 * half, half)
    one_b0 = cross0 + dot(hidden0, b0b0)
    squares1 = squares0 + jnp.sum(hid0 * (cross0 + one_b0), axis=1, keepdims=True)
    inv1 = lax.rsqrt(squares1 / width + epsilon)
    pre1 = inv1 * proj1
    sig1 = jax.nn.sigmoid(pre1)
    hidden1 = (pre1 * sig1).astype(BF16)
    hid1 = hidden1.astype(F32)
    one_b1 = total(3 * half, half) + dot_nt(hidden0, b1b0)
    two_b0 = one_b0 + dot(hidden1, b1b0)
    two_b1 = one_b1 + dot(hidden1, b1b1)
    squares2 = squares1 + jnp.sum(hid1 * (one_b1 + two_b1), axis=1, keepdims=True)
    inv2 = lax.rsqrt(squares2 / width + epsilon)
    base = total(4 * half, half) + dot(hidden0, b0h) + dot(hidden1, b1h)
    logits = inv2 * base
    expo = jnp.exp(logits - jnp.max(logits, axis=1, keepdims=True))
    prob = expo / jnp.sum(expo, axis=1, keepdims=True)
    labels = spread(label_ref[pl.ds(me, 1), :].astype(F32))
    valid = spread(valid_ref[pl.ds(me, 1), :].astype(F32))
    classes = lax.broadcasted_iota(jnp.int32, logits.shape, 1).astype(F32)
    cot = (prob - (classes == labels).astype(F32)) * valid
    factor2 = inv2 * inv2 * inv2 / width * jnp.sum(cot * base, axis=1, keepdims=True)
    weighted2 = (inv2 * cot).astype(BF16)
    grad1 = dot_nt(weighted2, b1h) - factor2 * two_b1
    act1 = grad1 * sig1 * (1.0 + pre1 * (1.0 - sig1))
    factor1 = inv1 * inv1 * inv1 / width * jnp.sum(act1 * proj1, axis=1, keepdims=True)
    weighted1 = (inv1 * act1).astype(BF16)
    grad0 = dot_nt(weighted2, b0h) - factor2 * two_b0 + dot_nt(weighted1, m01) - factor1 * one_b0
    act0 = grad0 * sig0 * (1.0 + pre0 * (1.0 - sig0))
    weighted0 = (inv0 * act0).astype(BF16)
    scaled0 = ((factor2 + factor1) * hid0).astype(BF16)
    scaled1 = (factor2 * hid1).astype(BF16)
    front = (hidden0, weighted2, scaled0, weighted0, weighted1, scaled1)
    back = (hidden1, weighted2, scaled1, weighted1, hidden0, hidden0)
    for slot, (a, b) in enumerate(zip(front, back)):
        mine_ref[slot * half : (slot + 1) * half, :] = jnp.where(first, a, b)
        theirs_ref[slot * half : (slot + 1) * half, :] = jnp.where(first, b, a)


def grad_kernel(replicas, mine_ref, theirs_ref, x_ref, down_t_ref, head_t_ref, up_ref, up2_ref, mixed_ref, gain_ref, valid_ref, *refs):
    out_refs, all_ref = refs[:replicas], refs[replicas]
    rank = mine_ref.shape[1]
    half = mine_ref.shape[0] // 6
    features = x_ref.shape[1]
    slim = rank // replicas
    first = lax.axis_index("section") == 0
    mine, theirs = mine_ref[...], theirs_ref[...]
    front, back = jnp.where(first, mine, theirs), jnp.where(first, theirs, mine)
    hidden, last, scaled, weighted, extra1, extra2 = (
        [v[i * half : (i + 1) * half] for v in (front, back)] for i in range(6)
    )
    hidden_t, scaled_t, weighted_t = ([transposed(v) for v in s] for s in (hidden, scaled, weighted))

    def product(left, right):
        return sum(dot(a, b) for a, b in zip(left, right))

    left_oth = [jnp.where(first, a, b) for a, b in zip(hidden_t, scaled_t)]
    left_mix = [jnp.where(first, a, b) for a, b in zip(hidden_t, weighted_t)]
    head_mix = product(hidden_t, last).astype(BF16)
    own_mix = product(scaled_t, hidden).astype(BF16)
    oth_mix = product(left_oth, extra2).astype(BF16)
    mix = product(left_mix, extra1).astype(BF16)
    none = jnp.zeros_like(mix)
    halves = [x_ref[i * half : (i + 1) * half, :] for i in range(2)]
    mixed = mixed_ref[...]
    grad = product(weighted_t, halves) + dot(jnp.where(first, none, mix), mixed)
    gain = jnp.sum(grad * down_t_ref[...].astype(F32), axis=0, keepdims=True)
    grad = (grad * gain_ref[...].astype(F32)).astype(BF16)
    rest = dot(head_mix, head_t_ref[...]) + dot(jnp.where(first, mix, none), mixed)
    rest = rest - dot(own_mix, up_ref[...]) - dot(oth_mix, up2_ref[...]) - product(scaled_t, halves)
    rest = rest.astype(BF16)
    for c in range(replicas):
        all_ref[2 * c * slim : (2 * c + 1) * slim, :] = grad[c * slim : (c + 1) * slim]
        all_ref[(2 * c + 1) * slim : (2 * c + 2) * slim, :] = rest[c * slim : (c + 1) * slim]
    count = jnp.sum(valid_ref[...].astype(F32), keepdims=True)
    lines = features // rank
    tail = jnp.concatenate(
        [gain[:, i * rank : (i + 1) * rank] for i in range(lines)] + [jnp.broadcast_to(count, (PACK - lines, rank))],
        axis=0,
    ).astype(BF16)
    me = lax.axis_index("dp")
    for step, out_ref in enumerate(out_refs):
        block = all_ref[rows_of(partner(me, step, replicas) * 2 * slim, 2 * slim), :]
        for i in range(lines):
            out_ref[i * 2 * slim : (i + 1) * 2 * slim, :] = block[:, i * rank : (i + 1) * rank]
        out_ref[lines * 2 * slim :, :] = tail


def last_kernel(*refs):
    parts, (down_out, up_out, gain_out) = refs[:-3], refs[-3:]
    rank = parts[0].shape[1]
    slim, features = down_out.shape
    lines = features // rank

    def total(start, size):
        return sum(p[start : start + size, :].astype(F32) for p in parts)

    tail = total(lines * 2 * slim, PACK)
    scale = 1.0 / tail[lines : lines + 1, :1]
    for i in range(lines):
        lanes = slice(i * rank, (i + 1) * rank)
        down_out[:, lanes] = total(i * 2 * slim, slim) * scale
        up_out[:, lanes] = total((2 * i + 1) * slim, slim) * scale
        gain_out[:, lanes] = tail[i : i + 1, :] * scale


def local(inputs, adapter_down, adapter_up, gains, head, labels, valid):
    sections, tensors, replicas = (lax.axis_size(a) for a in ("section", "tensor", "dp"))
    me = lax.axis_index("section")
    features = inputs.shape[2]
    width = features * tensors
    rank = adapter_down.shape[2]
    states = inputs.reshape(-1, features)
    half = states.shape[0] // sections
    assert sections == 2 and half == rank and head.shape[1] == rank and features % rank == 0
    slim = rank // replicas
    lines = features // rank
    down, up = adapter_down[0], adapter_up[0]
    labels, valid = labels.reshape(sections, half), valid.reshape(sections, half)
    shape = jax.ShapeDtypeStruct

    down2, up2, gains2 = (from_partner(v, "section", 1) for v in (down, up, gains))
    small = 2 * rank * rank * features
    own = call(
        own_kernel,
        shape((3 * half + 2 * rank + PACK, rank), BF16),
        5 * small,
        states, down, up, head, call(gain_kernel, shape(gains.shape, F32), 40 * small, gains),
    )
    packed = call(
        other_kernel,
        shape((5 * half + 3 * rank + PACK, rank), BF16),
        3 * small,
        states, up, own, down2, up2, gains2,
    )
    wide = [packed] + [from_partner(packed, "tensor", step) for step in range(1, tensors)]
    down_t, head_t, mixed = call(
        prepare_kernel,
        [shape((rank, features), BF16)] * 3,
        small,
        down, head, down2, up2, gains2,
    )
    gram = sum(w[5 * half : 5 * half + 3 * rank].astype(F32) for w in wide).astype(BF16)
    gram2 = from_partner(gram, "section", 1)
    made, theirs = call(
        functools.partial(chain_kernel, width, tensors),
        [shape((6 * half, rank), BF16)] * 2,
        16 * 2 * half * rank * rank,
        *wide, gram, gram2, labels, valid,
    )
    met = from_partner(theirs, "section", 1)
    *parts, _ = call(
        functools.partial(grad_kernel, replicas),
        [shape((lines * 2 * slim + PACK, rank), BF16)] * replicas + [shape((2 * rank, features), BF16)],
        16 * small,
        made, met, states, down_t, head_t, up, up2, mixed, gains, valid,
    )
    parts = [parts[0]] + [from_partner(parts[step], "dp", step) for step in range(1, replicas)]
    down_grad, up_grad, gain_grad = call(
        last_kernel,
        [shape((slim, features), F32), shape((slim, features), F32), shape((1, features), F32)],
        small,
        *parts,
    )
    return down_grad.T[None], up_grad[None], gain_grad


def solution(mesh):
    return jax.shard_map(
        local,
        mesh=mesh,
        in_specs=(
            P(None, "dp", "tensor"),
            P("section", "tensor", None),
            P("section", None, "tensor"),
            P("section", "tensor"),
            P("tensor", None),
            P(None, "dp"),
            P(None, "dp"),
        ),
        out_specs=(
            P("section", "tensor", "dp"),
            P("section", "dp", "tensor"),
            P("section", "tensor"),
        ),
        check_vma=False,
    )
```

```python
import functools

import jax
import jax.numpy as jnp
from jax import lax
from jax.experimental import pallas as pl
from jax.experimental.pallas import tpu as pltpu
from jax.sharding import PartitionSpec as P


epsilon = 1e-05
F32 = jnp.float32
BF16 = jnp.bfloat16
PACK = 16


def dot(a, b):
    return jnp.dot(a, b, preferred_element_type=F32)


def dot_nt(a, b):
    return lax.dot_general(a, b, (((1,), (1,)), ((), ())), preferred_element_type=F32)


def rows_of(start, count):
    return pl.ds(pl.multiple_of(start, count), count)


def transposed(value):
    return value.astype(F32).T.astype(value.dtype)


def partner(index, step, size):
    if size & (size - 1) == 0:
        return index ^ step
    return (index + step) % size


def from_partner(value, axis, step):
    size = lax.axis_size(axis)
    return lax.ppermute(value, axis, [(i, partner(i, step, size)) for i in range(size)])


def high_low(value):
    high = value.astype(BF16).astype(F32)
    return jnp.concatenate([high, value - high], axis=0).astype(BF16)


def call(kernel, out, flops, *args):
    moved = sum(a.size * a.dtype.itemsize for a in args)
    return pl.pallas_call(
        kernel,
        out_shape=out,
        cost_estimate=pl.CostEstimate(flops=flops, bytes_accessed=moved, transcendentals=0),
        compiler_params=pltpu.CompilerParams(vmem_limit_bytes=24 * 2**20),
    )(*args)


def gain_kernel(gain_ref, out_ref):
    out_ref[...] = gain_ref[...].astype(F32)


def own_kernel(x_ref, down_ref, up_ref, head_ref, gain_ref, out_ref):
    rank = down_ref.shape[1]
    half = x_ref.shape[0] // lax.axis_size("section")
    x, up, head = x_ref[rows_of(lax.axis_index("section") * half, half), :], up_ref[...], head_ref[...]
    x32 = x.astype(F32)
    scaled = (x32 * gain_ref[...]).astype(BF16)
    out_ref[:half, :] = dot(scaled, down_ref[...]).astype(BF16)
    out_ref[half : 2 * half, :] = dot_nt(x, up).astype(BF16)
    out_ref[2 * half : 3 * half, :] = dot(x, head).astype(BF16)
    out_ref[3 * half : 3 * half + rank, :] = dot(up, head).astype(BF16)
    out_ref[3 * half + rank : 3 * half + 2 * rank, :] = dot_nt(up, up).astype(BF16)
    squares = jnp.sum(x32 * x32, axis=1, keepdims=True)
    squares = jnp.broadcast_to(squares, (half, rank)).T
    out_ref[3 * half + 2 * rank :, :] = high_low(squares[: PACK // 2])


def other_kernel(x_ref, up_ref, own_ref, down2_ref, up2_ref, gain2_ref, out_ref, gram_ref):
    rank = down2_ref.shape[1]
    half = x_ref.shape[0] // lax.axis_size("section")
    me = lax.axis_index("section")
    it = 1 - me
    x = x_ref[rows_of(me * half, half), :]
    gain2 = gain2_ref[...].astype(F32)
    out_ref[rows_of(me * half, half), :] = own_ref[:half, :]
    out_ref[rows_of((2 + me) * half, half), :] = own_ref[half : 2 * half, :]
    out_ref[4 * half : 5 * half, :] = own_ref[2 * half : 3 * half, :]
    out_ref[5 * half :, :] = own_ref[3 * half + 2 * rank :, :]
    gram_ref[rank:, :] = own_ref[3 * half : 3 * half + 2 * rank, :]
    scaled = (x.astype(F32) * gain2).astype(BF16)
    out_ref[rows_of(it * half, half), :] = dot(scaled, down2_ref[...]).astype(BF16)
    out_ref[rows_of((2 + it) * half, half), :] = dot_nt(x, up2_ref[...]).astype(BF16)

    @pl.when(me == 0)
    def _():
        scaled = (up_ref[...].astype(F32) * gain2).astype(BF16)
        gram_ref[:rank, :] = dot(scaled, down2_ref[...]).astype(BF16)

    @pl.when(me != 0)
    def _():
        gram_ref[:rank, :] = dot_nt(up_ref[...], up2_ref[...]).astype(BF16)


def add_kernel(*refs):
    refs[-1][...] = sum(r[...].astype(F32) for r in refs[:-1]).astype(BF16)


def prepare_kernel(down_ref, head_ref, down2_ref, up2_ref, gain2_ref, down_t_ref, head_t_ref, mixed_ref):
    down_t_ref[...] = transposed(down_ref[...])
    head_t_ref[...] = transposed(head_ref[...])
    me = lax.axis_index("section")

    @pl.when(me == 0)
    def _():
        mixed_ref[...] = (down2_ref[...].astype(F32).T * gain2_ref[...].astype(F32)).astype(BF16)

    @pl.when(me != 0)
    def _():
        mixed_ref[...] = up2_ref[...]


def chain_kernel(width, count, *refs):
    parts, (gram_ref, gram2_ref, label_ref, valid_ref, mine_ref, theirs_ref) = refs[:count], refs[count:]
    rank = gram_ref.shape[1]
    half = label_ref.shape[1]
    me = lax.axis_index("section")
    first = me == 0

    def total(start, size):
        return sum(r[start : start + size, :].astype(F32) for r in parts)

    def spread(row):
        return jnp.broadcast_to(row, (rank, half)).T

    gram, gram2 = gram_ref[...], gram2_ref[...]
    gram0, gram1 = jnp.where(first, gram, gram2), jnp.where(first, gram2, gram)
    m01, b0h, b0b0 = (gram0[i * rank : (i + 1) * rank] for i in range(3))
    b1b0, b1h, b1b1 = (gram1[i * rank : (i + 1) * rank] for i in range(3))
    tail = total(5 * half, PACK)
    squares0 = spread(tail[:1] + tail[PACK // 2 : PACK // 2 + 1])
    inv0 = lax.rsqrt(squares0 / width + epsilon)
    proj0 = total(0, half)
    pre0 = inv0 * proj0
    sig0 = jax.nn.sigmoid(pre0)
    hidden0 = (pre0 * sig0).astype(BF16)
    hid0 = hidden0.astype(F32)
    proj1 = total(half, half) + dot(hidden0, m01)
    cross0 = total(2 * half, half)
    one_b0 = cross0 + dot(hidden0, b0b0)
    squares1 = squares0 + jnp.sum(hid0 * (cross0 + one_b0), axis=1, keepdims=True)
    inv1 = lax.rsqrt(squares1 / width + epsilon)
    pre1 = inv1 * proj1
    sig1 = jax.nn.sigmoid(pre1)
    hidden1 = (pre1 * sig1).astype(BF16)
    hid1 = hidden1.astype(F32)
    one_b1 = total(3 * half, half) + dot_nt(hidden0, b1b0)
    two_b0 = one_b0 + dot(hidden1, b1b0)
    two_b1 = one_b1 + dot(hidden1, b1b1)
    squares2 = squares1 + jnp.sum(hid1 * (one_b1 + two_b1), axis=1, keepdims=True)
    inv2 = lax.rsqrt(squares2 / width + epsilon)
    base = total(4 * half, half) + dot(hidden0, b0h) + dot(hidden1, b1h)
    logits = inv2 * base
    expo = jnp.exp(logits - jnp.max(logits, axis=1, keepdims=True))
    prob = expo / jnp.sum(expo, axis=1, keepdims=True)
    labels = spread(label_ref[pl.ds(me, 1), :].astype(F32))
    valid = spread(valid_ref[pl.ds(me, 1), :].astype(F32))
    classes = lax.broadcasted_iota(jnp.int32, logits.shape, 1).astype(F32)
    cot = (prob - (classes == labels).astype(F32)) * valid
    factor2 = inv2 * inv2 * inv2 / width * jnp.sum(cot * base, axis=1, keepdims=True)
    weighted2 = (inv2 * cot).astype(BF16)
    grad1 = dot_nt(weighted2, b1h) - factor2 * two_b1
    act1 = grad1 * sig1 * (1.0 + pre1 * (1.0 - sig1))
    factor1 = inv1 * inv1 * inv1 / width * jnp.sum(act1 * proj1, axis=1, keepdims=True)
    weighted1 = (inv1 * act1).astype(BF16)
    grad0 = dot_nt(weighted2, b0h) - factor2 * two_b0 + dot_nt(weighted1, m01) - factor1 * one_b0
    act0 = grad0 * sig0 * (1.0 + pre0 * (1.0 - sig0))
    weighted0 = (inv0 * act0).astype(BF16)
    scaled0 = ((factor2 + factor1) * hid0).astype(BF16)
    scaled1 = (factor2 * hid1).astype(BF16)
    front = (hidden0, weighted2, scaled0, weighted0, weighted1, scaled1)
    back = (hidden1, weighted2, scaled1, weighted1, hidden0, hidden0)
    for slot, (a, b) in enumerate(zip(front, back)):
        mine_ref[slot * half : (slot + 1) * half, :] = jnp.where(first, a, b)
        theirs_ref[slot * half : (slot + 1) * half, :] = jnp.where(first, b, a)


def products(made, x):
    half = x.shape[0]
    first = lax.axis_index("section") == 0
    hidden, last, scaled, weighted, extra1, extra2 = (made[i * half : (i + 1) * half] for i in range(6))
    hidden_t, scaled_t, weighted_t = (transposed(v) for v in (hidden, scaled, weighted))
    mixes = (
        dot(hidden_t, last),
        dot(scaled_t, hidden),
        dot(jnp.where(first, hidden_t, scaled_t), extra2),
        dot(jnp.where(first, hidden_t, weighted_t), extra1),
    )
    return mixes, dot(weighted_t, x), dot(scaled_t, x)


def mine_kernel(made_ref, x_ref, mix_ref, acc_ref):
    rank = made_ref.shape[1]
    half = made_ref.shape[0] // 6
    x = x_ref[rows_of(lax.axis_index("section") * half, half), :]
    mixes, grad, rest = products(made_ref[...], x)
    for i, mix in enumerate(mixes):
        mix_ref[i * rank : (i + 1) * rank, :] = mix
    acc_ref[:rank, :] = grad
    acc_ref[rank:, :] = rest


def grad_kernel(
    replicas, made_ref, mix_ref, acc_ref, x_ref, down_t_ref, head_t_ref, up_ref, up2_ref, mixed_ref, gain_ref,
    valid_ref, *refs
):
    out_refs, all_ref = refs[:replicas], refs[replicas]
    rank = made_ref.shape[1]
    half = made_ref.shape[0] // 6
    features = x_ref.shape[1]
    slim = rank // replicas
    me = lax.axis_index("section")
    first = me == 0
    x = x_ref[rows_of((1 - me) * half, half), :]
    mixes, grad, rest = products(made_ref[...], x)
    head_mix, own_mix, oth_mix, mix = (
        (m + mix_ref[i * rank : (i + 1) * rank, :]).astype(BF16) for i, m in enumerate(mixes)
    )
    none = jnp.zeros_like(mix)
    mixed = mixed_ref[...]
    grad = grad + acc_ref[:rank, :] + dot(jnp.where(first, none, mix), mixed)
    gain = jnp.sum(grad * down_t_ref[...].astype(F32), axis=0, keepdims=True)
    grad = (grad * gain_ref[...]).astype(BF16)
    rest = dot(head_mix, head_t_ref[...]) + dot(jnp.where(first, mix, none), mixed) - rest - acc_ref[rank:, :]
    rest = rest - dot(own_mix, up_ref[...]) - dot(oth_mix, up2_ref[...])
    rest = rest.astype(BF16)
    for c in range(replicas):
        all_ref[2 * c * slim : (2 * c + 1) * slim, :] = grad[c * slim : (c + 1) * slim]
        all_ref[(2 * c + 1) * slim : (2 * c + 2) * slim, :] = rest[c * slim : (c + 1) * slim]
    count = jnp.sum(valid_ref[...].astype(F32), keepdims=True)
    lines = features // rank
    tail = jnp.concatenate(
        [gain[:, i * rank : (i + 1) * rank] for i in range(lines)] + [jnp.broadcast_to(count, (PACK - lines, rank))],
        axis=0,
    ).astype(BF16)
    place = lax.axis_index("dp")
    for step, out_ref in enumerate(out_refs):
        block = all_ref[rows_of(partner(place, step, replicas) * 2 * slim, 2 * slim), :]
        for i in range(lines):
            out_ref[i * 2 * slim : (i + 1) * 2 * slim, :] = block[:, i * rank : (i + 1) * rank]
        out_ref[lines * 2 * slim :, :] = tail


def last_kernel(*refs):
    parts, (down_out, up_out, gain_out) = refs[:-3], refs[-3:]
    rank = parts[0].shape[1]
    slim, features = down_out.shape
    lines = features // rank

    def total(start, size):
        return sum(p[start : start + size, :].astype(F32) for p in parts)

    tail = total(lines * 2 * slim, PACK)
    scale = 1.0 / tail[lines : lines + 1, :1]
    for i in range(lines):
        lanes = slice(i * rank, (i + 1) * rank)
        down_out[:, lanes] = total(i * 2 * slim, slim) * scale
        up_out[:, lanes] = total((2 * i + 1) * slim, slim) * scale
        gain_out[:, lanes] = tail[i : i + 1, :] * scale


def local(inputs, adapter_down, adapter_up, gains, head, labels, valid):
    sections, tensors, replicas = (lax.axis_size(a) for a in ("section", "tensor", "dp"))
    features = inputs.shape[2]
    width = features * tensors
    rank = adapter_down.shape[2]
    states = inputs.reshape(-1, features)
    half = states.shape[0] // sections
    assert sections == 2 and half == rank and head.shape[1] == rank and features % rank == 0
    slim = rank // replicas
    lines = features // rank
    down, up = adapter_down[0], adapter_up[0]
    labels, valid = labels.reshape(sections, half), valid.reshape(sections, half)
    shape = jax.ShapeDtypeStruct

    down2, up2, gains2 = (from_partner(v, "section", 1) for v in (down, up, gains))
    small = 2 * rank * rank * features
    wide_gain = call(gain_kernel, shape(gains.shape, F32), 40 * small, gains)
    own = call(
        own_kernel,
        shape((3 * half + 2 * rank + PACK, rank), BF16),
        5 * small,
        states, down, up, head, wide_gain,
    )
    packed, gram = call(
        other_kernel,
        [shape((5 * half + PACK, rank), BF16), shape((3 * rank, rank), BF16)],
        3 * small,
        states, up, own, down2, up2, gains2,
    )
    wide = [packed]
    for step in range(1, tensors):
        wide.append(from_partner(packed, "tensor", step))
    down_t, head_t, mixed = call(
        prepare_kernel,
        [shape((rank, features), BF16)] * 3,
        small,
        down, head, down2, up2, gains2,
    )
    if tensors & (tensors - 1) == 0:
        step = 1
        while step < tensors:
            gram = call(add_kernel, shape(gram.shape, BF16), small // 8, gram, from_partner(gram, "tensor", step))
            step *= 2
    else:
        gram = call(
            add_kernel,
            shape(gram.shape, BF16),
            small // 8,
            gram,
            *(from_partner(gram, "tensor", step) for step in range(1, tensors)),
        )
    gram2 = from_partner(gram, "section", 1)
    made, theirs = call(
        functools.partial(chain_kernel, width, tensors),
        [shape((6 * half, rank), BF16)] * 2,
        16 * 2 * half * rank * rank,
        *wide, gram, gram2, labels, valid,
    )
    met = from_partner(theirs, "section", 1)
    mixes, acc = call(
        mine_kernel,
        [shape((4 * rank, rank), F32), shape((2 * rank, features), F32)],
        4 * small,
        made, states,
    )
    *parts, _ = call(
        functools.partial(grad_kernel, replicas),
        [shape((lines * 2 * slim + PACK, rank), BF16)] * replicas + [shape((2 * rank, features), BF16)],
        16 * small,
        met, mixes, acc, states, down_t, head_t, up, up2, mixed, wide_gain, valid,
    )
    for step in range(1, replicas):
        parts[step] = from_partner(parts[step], "dp", step)
    down_grad, up_grad, gain_grad = call(
        last_kernel,
        [shape((slim, features), F32), shape((slim, features), F32), shape((1, features), F32)],
        small,
        *parts,
    )
    return down_grad.T[None], up_grad[None], gain_grad


def solution(mesh):
    return jax.shard_map(
        local,
        mesh=mesh,
        in_specs=(
            P(None, "dp", "tensor"),
            P("section", "tensor", None),
            P("section", None, "tensor"),
            P("section", "tensor"),
            P("tensor", None),
            P(None, "dp"),
            P(None, "dp"),
        ),
        out_specs=(
            P("section", "tensor", "dp"),
            P("section", "dp", "tensor"),
            P("section", "tensor"),
        ),
        check_vma=False,
    )
```

```python
import functools

import jax
import jax.numpy as jnp
from jax import lax
from jax.experimental import pallas as pl
from jax.experimental.pallas import tpu as pltpu
from jax.sharding import PartitionSpec as P


epsilon = 1e-05
F32 = jnp.float32
BF16 = jnp.bfloat16
PACK = 16


def dot(a, b):
    return jnp.dot(a, b, preferred_element_type=F32)


def dot_nt(a, b):
    return lax.dot_general(a, b, (((1,), (1,)), ((), ())), preferred_element_type=F32)


def rows_of(start, count):
    return pl.ds(pl.multiple_of(start, count), count)


def transposed(value):
    return value.astype(F32).T.astype(value.dtype)


def partner(index, step, size):
    if size & (size - 1) == 0:
        return index ^ step
    return (index + step) % size


def from_partner(value, axis, step):
    size = lax.axis_size(axis)
    return lax.ppermute(value, axis, [(i, partner(i, step, size)) for i in range(size)])


def high_low(value):
    high = value.astype(BF16).astype(F32)
    return jnp.concatenate([high, value - high], axis=0).astype(BF16)


def call(kernel, out, flops, *args):
    moved = sum(a.size * a.dtype.itemsize for a in args)
    return pl.pallas_call(
        kernel,
        out_shape=out,
        cost_estimate=pl.CostEstimate(flops=flops, bytes_accessed=moved, transcendentals=0),
        compiler_params=pltpu.CompilerParams(vmem_limit_bytes=24 * 2**20),
    )(*args)


def gain_kernel(gain_ref, out_ref):
    out_ref[...] = gain_ref[...].astype(F32)


def own_kernel(x_ref, down_ref, up_ref, head_ref, gain_ref, out_ref):
    rank = down_ref.shape[1]
    half = x_ref.shape[0] // lax.axis_size("section")
    x, up, head = x_ref[rows_of(lax.axis_index("section") * half, half), :], up_ref[...], head_ref[...]
    x32 = x.astype(F32)
    scaled = (x32 * gain_ref[...]).astype(BF16)
    out_ref[:half, :] = dot(scaled, down_ref[...]).astype(BF16)
    out_ref[half : 2 * half, :] = dot_nt(x, up).astype(BF16)
    out_ref[2 * half : 3 * half, :] = dot(x, head).astype(BF16)
    out_ref[3 * half : 3 * half + rank, :] = dot(up, head).astype(BF16)
    out_ref[3 * half + rank : 3 * half + 2 * rank, :] = dot_nt(up, up).astype(BF16)
    squares = jnp.sum(x32 * x32, axis=1, keepdims=True)
    squares = jnp.broadcast_to(squares, (half, rank)).T
    out_ref[3 * half + 2 * rank :, :] = high_low(squares[: PACK // 2])


def other_kernel(x_ref, up_ref, own_ref, down2_ref, up2_ref, gain2_ref, out_ref, gram_ref):
    rank = down2_ref.shape[1]
    half = x_ref.shape[0] // lax.axis_size("section")
    me = lax.axis_index("section")
    it = 1 - me
    x = x_ref[rows_of(me * half, half), :]
    gain2 = gain2_ref[...].astype(F32)
    out_ref[rows_of(me * half, half), :] = own_ref[:half, :]
    out_ref[rows_of((2 + me) * half, half), :] = own_ref[half : 2 * half, :]
    out_ref[4 * half : 5 * half, :] = own_ref[2 * half : 3 * half, :]
    out_ref[5 * half :, :] = own_ref[3 * half + 2 * rank :, :]
    gram_ref[rank:, :] = own_ref[3 * half : 3 * half + 2 * rank, :]
    scaled = (x.astype(F32) * gain2).astype(BF16)
    out_ref[rows_of(it * half, half), :] = dot(scaled, down2_ref[...]).astype(BF16)
    out_ref[rows_of((2 + it) * half, half), :] = dot_nt(x, up2_ref[...]).astype(BF16)

    @pl.when(me == 0)
    def _():
        scaled = (up_ref[...].astype(F32) * gain2).astype(BF16)
        gram_ref[:rank, :] = dot(scaled, down2_ref[...]).astype(BF16)

    @pl.when(me != 0)
    def _():
        gram_ref[:rank, :] = dot_nt(up_ref[...], up2_ref[...]).astype(BF16)


def add_kernel(*refs):
    refs[-1][...] = sum(r[...].astype(F32) for r in refs[:-1]).astype(BF16)


def prepare_kernel(down_ref, head_ref, up_ref, down2_ref, up2_ref, gain2_ref, x_ref, down_t_ref, stack_ref):
    rank = up_ref.shape[0]
    half = x_ref.shape[0] // lax.axis_size("section")
    down_t_ref[...] = transposed(down_ref[...])
    stack_ref[:rank, :] = transposed(head_ref[...])
    stack_ref[rank : 2 * rank, :] = up_ref[...]
    stack_ref[2 * rank : 3 * rank, :] = up2_ref[...]
    me = lax.axis_index("section")

    @pl.when(me == 0)
    def _():
        stack_ref[3 * rank : 4 * rank, :] = (down2_ref[...].astype(F32).T * gain2_ref[...].astype(F32)).astype(BF16)

    @pl.when(me != 0)
    def _():
        stack_ref[3 * rank : 4 * rank, :] = up2_ref[...]

    stack_ref[4 * rank :, :] = x_ref[rows_of((1 - me) * half, half), :]


def chain_kernel(width, count, *refs):
    parts, (gram_ref, gram2_ref, label_ref, valid_ref, mine_ref, theirs_ref) = refs[:count], refs[count:]
    rank = gram_ref.shape[1]
    half = label_ref.shape[1]
    me = lax.axis_index("section")
    first = me == 0

    def total(start, size):
        return sum(r[start : start + size, :].astype(F32) for r in parts)

    def spread(row):
        return jnp.broadcast_to(row, (rank, half)).T

    gram, gram2 = gram_ref[...], gram2_ref[...]
    gram0, gram1 = jnp.where(first, gram, gram2), jnp.where(first, gram2, gram)
    m01, b0h, b0b0 = (gram0[i * rank : (i + 1) * rank] for i in range(3))
    b1b0, b1h, b1b1 = (gram1[i * rank : (i + 1) * rank] for i in range(3))
    tail = total(5 * half, PACK)
    squares0 = spread(tail[:1] + tail[PACK // 2 : PACK // 2 + 1])
    inv0 = lax.rsqrt(squares0 / width + epsilon)
    proj0 = total(0, half)
    pre0 = inv0 * proj0
    sig0 = jax.nn.sigmoid(pre0)
    hidden0 = (pre0 * sig0).astype(BF16)
    hid0 = hidden0.astype(F32)
    proj1 = total(half, half) + dot(hidden0, m01)
    cross0 = total(2 * half, half)
    one_b0 = cross0 + dot(hidden0, b0b0)
    squares1 = squares0 + jnp.sum(hid0 * (cross0 + one_b0), axis=1, keepdims=True)
    inv1 = lax.rsqrt(squares1 / width + epsilon)
    pre1 = inv1 * proj1
    sig1 = jax.nn.sigmoid(pre1)
    hidden1 = (pre1 * sig1).astype(BF16)
    hid1 = hidden1.astype(F32)
    one_b1 = total(3 * half, half) + dot_nt(hidden0, b1b0)
    two_b0 = one_b0 + dot(hidden1, b1b0)
    two_b1 = one_b1 + dot(hidden1, b1b1)
    squares2 = squares1 + jnp.sum(hid1 * (one_b1 + two_b1), axis=1, keepdims=True)
    inv2 = lax.rsqrt(squares2 / width + epsilon)
    base = total(4 * half, half) + dot(hidden0, b0h) + dot(hidden1, b1h)
    logits = inv2 * base
    expo = jnp.exp(logits - jnp.max(logits, axis=1, keepdims=True))
    prob = expo / jnp.sum(expo, axis=1, keepdims=True)
    labels = spread(label_ref[pl.ds(me, 1), :].astype(F32))
    valid = spread(valid_ref[pl.ds(me, 1), :].astype(F32))
    classes = lax.broadcasted_iota(jnp.int32, logits.shape, 1).astype(F32)
    cot = (prob - (classes == labels).astype(F32)) * valid
    factor2 = inv2 * inv2 * inv2 / width * jnp.sum(cot * base, axis=1, keepdims=True)
    weighted2 = (inv2 * cot).astype(BF16)
    grad1 = dot_nt(weighted2, b1h) - factor2 * two_b1
    act1 = grad1 * sig1 * (1.0 + pre1 * (1.0 - sig1))
    factor1 = inv1 * inv1 * inv1 / width * jnp.sum(act1 * proj1, axis=1, keepdims=True)
    weighted1 = (inv1 * act1).astype(BF16)
    grad0 = dot_nt(weighted2, b0h) - factor2 * two_b0 + dot_nt(weighted1, m01) - factor1 * one_b0
    act0 = grad0 * sig0 * (1.0 + pre0 * (1.0 - sig0))
    weighted0 = (inv0 * act0).astype(BF16)
    scaled0 = ((factor2 + factor1) * hid0).astype(BF16)
    scaled1 = (factor2 * hid1).astype(BF16)
    front = (hidden0, weighted2, scaled0, weighted0, weighted1, scaled1)
    back = (hidden1, weighted2, scaled1, weighted1, hidden0, hidden0)
    for slot, (a, b) in enumerate(zip(front, back)):
        mine_ref[slot * half : (slot + 1) * half, :] = jnp.where(first, a, b)
        theirs_ref[slot * half : (slot + 1) * half, :] = jnp.where(first, b, a)


def products(made):
    half = made.shape[0] // 6
    first = lax.axis_index("section") == 0
    hidden, last, scaled, weighted, extra1, extra2 = (made[i * half : (i + 1) * half] for i in range(6))
    hidden_t, scaled_t, weighted_t = (transposed(v) for v in (hidden, -scaled, weighted))
    mixes = (
        dot(hidden_t, last),
        dot(scaled_t, hidden),
        dot(jnp.where(first, -hidden_t, scaled_t), extra2),
        dot(jnp.where(first, hidden_t, weighted_t), extra1),
    )
    return mixes, weighted_t, scaled_t


def mine_kernel(made_ref, x_ref, mix_ref, acc_ref):
    rank = made_ref.shape[1]
    half = made_ref.shape[0] // 6
    x = x_ref[rows_of(lax.axis_index("section") * half, half), :]
    mixes, weighted_t, scaled_t = products(made_ref[...])
    for i, mix in enumerate(mixes):
        mix_ref[i * rank : (i + 1) * rank, :] = mix
    acc_ref[:rank, :] = dot(weighted_t, x)
    acc_ref[rank:, :] = dot(scaled_t, x)


def grad_kernel(replicas, made_ref, mix_ref, acc_ref, stack_ref, down_t_ref, gain_ref, valid_ref, *refs):
    out_refs, all_ref = refs[:replicas], refs[replicas]
    rank, features = down_t_ref.shape
    slim = rank // replicas
    first = lax.axis_index("section") == 0
    mixes, weighted_t, scaled_t = products(made_ref[...])
    head_mix, own_mix, oth_mix, mix = (
        (m + mix_ref[i * rank : (i + 1) * rank, :]).astype(BF16) for i, m in enumerate(mixes)
    )
    none = jnp.zeros_like(mix)
    left = jnp.concatenate([jnp.where(first, none, mix), weighted_t], axis=1)
    grad = acc_ref[:rank, :] + dot(left, stack_ref[3 * rank :, :])
    gain = jnp.sum(grad * down_t_ref[...].astype(F32), axis=0, keepdims=True)
    grad = (grad * gain_ref[...]).astype(BF16)
    left = jnp.concatenate([head_mix, own_mix, oth_mix, jnp.where(first, mix, none), scaled_t], axis=1)
    rest = (acc_ref[rank:, :] + dot(left, stack_ref[...])).astype(BF16)
    for c in range(replicas):
        all_ref[2 * c * slim : (2 * c + 1) * slim, :] = grad[c * slim : (c + 1) * slim]
        all_ref[(2 * c + 1) * slim : (2 * c + 2) * slim, :] = rest[c * slim : (c + 1) * slim]
    count = jnp.sum(valid_ref[...].astype(F32), keepdims=True)
    lines = features // rank
    tail = jnp.concatenate(
        [gain[:, i * rank : (i + 1) * rank] for i in range(lines)] + [jnp.broadcast_to(count, (PACK - lines, rank))],
        axis=0,
    ).astype(BF16)
    place = lax.axis_index("dp")
    for step, out_ref in enumerate(out_refs):
        block = all_ref[rows_of(partner(place, step, replicas) * 2 * slim, 2 * slim), :]
        for i in range(lines):
            out_ref[i * 2 * slim : (i + 1) * 2 * slim, :] = block[:, i * rank : (i + 1) * rank]
        out_ref[lines * 2 * slim :, :] = tail


def last_kernel(*refs):
    parts, (down_out, up_out, gain_out) = refs[:-3], refs[-3:]
    rank = parts[0].shape[1]
    slim, features = down_out.shape
    lines = features // rank

    def total(start, size):
        return sum(p[start : start + size, :].astype(F32) for p in parts)

    tail = total(lines * 2 * slim, PACK)
    scale = 1.0 / tail[lines : lines + 1, :1]
    for i in range(lines):
        lanes = slice(i * rank, (i + 1) * rank)
        down_out[:, lanes] = total(i * 2 * slim, slim) * scale
        up_out[:, lanes] = total((2 * i + 1) * slim, slim) * scale
        gain_out[:, lanes] = tail[i : i + 1, :] * scale


def local(inputs, adapter_down, adapter_up, gains, head, labels, valid):
    sections, tensors, replicas = (lax.axis_size(a) for a in ("section", "tensor", "dp"))
    features = inputs.shape[2]
    width = features * tensors
    rank = adapter_down.shape[2]
    states = inputs.reshape(-1, features)
    half = states.shape[0] // sections
    assert sections == 2 and half == rank and head.shape[1] == rank and features % rank == 0
    slim = rank // replicas
    lines = features // rank
    down, up = adapter_down[0], adapter_up[0]
    labels, valid = labels.reshape(sections, half), valid.reshape(sections, half)
    shape = jax.ShapeDtypeStruct

    down2, up2, gains2 = (from_partner(v, "section", 1) for v in (down, up, gains))
    small = 2 * rank * rank * features
    wide_gain = call(gain_kernel, shape(gains.shape, F32), 40 * small, gains)
    own = call(
        own_kernel,
        shape((3 * half + 2 * rank + PACK, rank), BF16),
        5 * small,
        states, down, up, head, wide_gain,
    )
    packed, gram = call(
        other_kernel,
        [shape((5 * half + PACK, rank), BF16), shape((3 * rank, rank), BF16)],
        3 * small,
        states, up, own, down2, up2, gains2,
    )
    wide = [packed]
    for step in range(1, tensors):
        wide.append(from_partner(packed, "tensor", step))
    down_t, stack = call(
        prepare_kernel,
        [shape((rank, features), BF16), shape((4 * rank + half, features), BF16)],
        small,
        down, head, up, down2, up2, gains2, states,
    )
    if tensors & (tensors - 1) == 0:
        step = 1
        while step < tensors:
            gram = call(add_kernel, shape(gram.shape, BF16), small // 8, gram, from_partner(gram, "tensor", step))
            step *= 2
    else:
        gram = call(
            add_kernel,
            shape(gram.shape, BF16),
            small // 8,
            gram,
            *(from_partner(gram, "tensor", step) for step in range(1, tensors)),
        )
    gram2 = from_partner(gram, "section", 1)
    made, theirs = call(
        functools.partial(chain_kernel, width, tensors),
        [shape((6 * half, rank), BF16)] * 2,
        16 * 2 * half * rank * rank,
        *wide, gram, gram2, labels, valid,
    )
    met = from_partner(theirs, "section", 1)
    mixes, acc = call(
        mine_kernel,
        [shape((4 * rank, rank), F32), shape((2 * rank, features), F32)],
        4 * small,
        made, states,
    )
    *parts, _ = call(
        functools.partial(grad_kernel, replicas),
        [shape((lines * 2 * slim + PACK, rank), BF16)] * replicas + [shape((2 * rank, features), BF16)],
        16 * small,
        met, mixes, acc, stack, down_t, wide_gain, valid,
    )
    for step in range(1, replicas):
        parts[step] = from_partner(parts[step], "dp", step)
    down_grad, up_grad, gain_grad = call(
        last_kernel,
        [shape((slim, features), F32), shape((slim, features), F32), shape((1, features), F32)],
        small,
        *parts,
    )
    return down_grad.T[None], up_grad[None], gain_grad


def solution(mesh):
    return jax.shard_map(
        local,
        mesh=mesh,
        in_specs=(
            P(None, "dp", "tensor"),
            P("section", "tensor", None),
            P("section", None, "tensor"),
            P("section", "tensor"),
            P("tensor", None),
            P(None, "dp"),
            P(None, "dp"),
        ),
        out_specs=(
            P("section", "tensor", "dp"),
            P("section", "dp", "tensor"),
            P("section", "tensor"),
        ),
        check_vma=False,
    )
```

```python
import functools

import jax
import jax.numpy as jnp
from jax import lax
from jax.experimental import pallas as pl
from jax.experimental.pallas import tpu as pltpu
from jax.sharding import PartitionSpec as P


epsilon = 1e-05
F32 = jnp.float32
BF16 = jnp.bfloat16
PACK = 16


def dot(a, b):
    return jnp.dot(a, b, preferred_element_type=F32)


def dot_nt(a, b):
    return lax.dot_general(a, b, (((1,), (1,)), ((), ())), preferred_element_type=F32)


def rows_of(start, count):
    return pl.ds(pl.multiple_of(start, count), count)


def transposed(value):
    return value.astype(F32).T.astype(value.dtype)


def partner(index, step, size):
    if size & (size - 1) == 0:
        return index ^ step
    return (index + step) % size


def from_partner(value, axis, step):
    size = lax.axis_size(axis)
    return lax.ppermute(value, axis, [(i, partner(i, step, size)) for i in range(size)])


def high_low(value):
    high = value.astype(BF16).astype(F32)
    return jnp.concatenate([high, value - high], axis=0).astype(BF16)


def call(kernel, out, flops, *args):
    moved = sum(a.size * a.dtype.itemsize for a in args)
    return pl.pallas_call(
        kernel,
        out_shape=out,
        cost_estimate=pl.CostEstimate(flops=flops, bytes_accessed=moved, transcendentals=0),
        compiler_params=pltpu.CompilerParams(vmem_limit_bytes=24 * 2**20),
    )(*args)


def gain_kernel(gain_ref, out_ref):
    out_ref[...] = gain_ref[...].astype(F32)


def own_kernel(x_ref, down_ref, up_ref, head_ref, gain_ref, out_ref):
    rank = down_ref.shape[1]
    half = x_ref.shape[0] // lax.axis_size("section")
    x, up, head = x_ref[rows_of(lax.axis_index("section") * half, half), :], up_ref[...], head_ref[...]
    x32 = x.astype(F32)
    scaled = (x32 * gain_ref[...]).astype(BF16)
    out_ref[:half, :] = dot(scaled, down_ref[...]).astype(BF16)
    out_ref[half : 2 * half, :] = dot_nt(x, up).astype(BF16)
    out_ref[2 * half : 3 * half, :] = dot(x, head).astype(BF16)
    out_ref[3 * half : 3 * half + rank, :] = dot(up, head).astype(BF16)
    out_ref[3 * half + rank : 3 * half + 2 * rank, :] = dot_nt(up, up).astype(BF16)
    squares = jnp.sum(x32 * x32, axis=1, keepdims=True)
    squares = jnp.broadcast_to(squares, (half, rank)).T
    out_ref[3 * half + 2 * rank :, :] = high_low(squares[: PACK // 2])


def other_kernel(x_ref, up_ref, own_ref, down2_ref, up2_ref, gain2_ref, out_ref, gram_ref):
    rank = down2_ref.shape[1]
    half = x_ref.shape[0] // lax.axis_size("section")
    me = lax.axis_index("section")
    it = 1 - me
    x = x_ref[rows_of(me * half, half), :]
    gain2 = gain2_ref[...].astype(F32)
    out_ref[rows_of(me * half, half), :] = own_ref[:half, :]
    out_ref[rows_of((2 + me) * half, half), :] = own_ref[half : 2 * half, :]
    out_ref[4 * half : 5 * half, :] = own_ref[2 * half : 3 * half, :]
    out_ref[5 * half :, :] = own_ref[3 * half + 2 * rank :, :]
    gram_ref[rank:, :] = own_ref[3 * half : 3 * half + 2 * rank, :]
    scaled = (x.astype(F32) * gain2).astype(BF16)
    out_ref[rows_of(it * half, half), :] = dot(scaled, down2_ref[...]).astype(BF16)
    out_ref[rows_of((2 + it) * half, half), :] = dot_nt(x, up2_ref[...]).astype(BF16)

    @pl.when(me == 0)
    def _():
        scaled = (up_ref[...].astype(F32) * gain2).astype(BF16)
        gram_ref[:rank, :] = dot(scaled, down2_ref[...]).astype(BF16)

    @pl.when(me != 0)
    def _():
        gram_ref[:rank, :] = dot_nt(up_ref[...], up2_ref[...]).astype(BF16)


def add_kernel(*refs):
    refs[-1][...] = sum(r[...].astype(F32) for r in refs[:-1]).astype(BF16)


def prepare_kernel(down_ref, head_ref, up_ref, down2_ref, up2_ref, gain2_ref, x_ref, down_t_ref, stack_ref):
    rank = up_ref.shape[0]
    half = x_ref.shape[0] // lax.axis_size("section")
    down_t_ref[...] = transposed(down_ref[...])
    stack_ref[:rank, :] = transposed(head_ref[...])
    stack_ref[rank : 2 * rank, :] = up_ref[...]
    stack_ref[2 * rank : 3 * rank, :] = up2_ref[...]
    me = lax.axis_index("section")

    @pl.when(me == 0)
    def _():
        stack_ref[3 * rank : 4 * rank, :] = (down2_ref[...].astype(F32).T * gain2_ref[...].astype(F32)).astype(BF16)

    @pl.when(me != 0)
    def _():
        stack_ref[3 * rank : 4 * rank, :] = up2_ref[...]

    stack_ref[4 * rank :, :] = x_ref[rows_of((1 - me) * half, half), :]


def chain_kernel(width, count, *refs):
    parts, (gram_ref, gram2_ref, label_ref, valid_ref, mine_ref, theirs_ref) = refs[:count], refs[count:]
    rank = gram_ref.shape[1]
    half = label_ref.shape[1]
    me = lax.axis_index("section")
    first = me == 0

    def total(start, size):
        return sum(r[start : start + size, :].astype(F32) for r in parts)

    def spread(row):
        return jnp.broadcast_to(row, (rank, half)).T

    gram, gram2 = gram_ref[...], gram2_ref[...]
    gram0, gram1 = jnp.where(first, gram, gram2), jnp.where(first, gram2, gram)
    m01, b0h, b0b0 = (gram0[i * rank : (i + 1) * rank] for i in range(3))
    b1b0, b1h, b1b1 = (gram1[i * rank : (i + 1) * rank] for i in range(3))
    tail = total(5 * half, PACK)
    squares0 = spread(tail[:1] + tail[PACK // 2 : PACK // 2 + 1])
    inv0 = lax.rsqrt(squares0 / width + epsilon)
    proj0 = total(0, half)
    pre0 = inv0 * proj0
    sig0 = jax.nn.sigmoid(pre0)
    hidden0 = (pre0 * sig0).astype(BF16)
    hid0 = hidden0.astype(F32)
    proj1 = total(half, half) + dot(hidden0, m01)
    cross0 = total(2 * half, half)
    one_b0 = cross0 + dot(hidden0, b0b0)
    squares1 = squares0 + jnp.sum(hid0 * (cross0 + one_b0), axis=1, keepdims=True)
    inv1 = lax.rsqrt(squares1 / width + epsilon)
    pre1 = inv1 * proj1
    sig1 = jax.nn.sigmoid(pre1)
    hidden1 = (pre1 * sig1).astype(BF16)
    hid1 = hidden1.astype(F32)
    one_b1 = total(3 * half, half) + dot_nt(hidden0, b1b0)
    two_b0 = one_b0 + dot(hidden1, b1b0)
    two_b1 = one_b1 + dot(hidden1, b1b1)
    squares2 = squares1 + jnp.sum(hid1 * (one_b1 + two_b1), axis=1, keepdims=True)
    inv2 = lax.rsqrt(squares2 / width + epsilon)
    base = total(4 * half, half) + dot(hidden0, b0h) + dot(hidden1, b1h)
    logits = inv2 * base
    expo = jnp.exp(logits - jnp.max(logits, axis=1, keepdims=True))
    prob = expo / jnp.sum(expo, axis=1, keepdims=True)
    labels = spread(label_ref[pl.ds(me, 1), :].astype(F32))
    valid = spread(valid_ref[pl.ds(me, 1), :].astype(F32))
    classes = lax.broadcasted_iota(jnp.int32, logits.shape, 1).astype(F32)
    cot = (prob - (classes == labels).astype(F32)) * valid
    factor2 = inv2 * inv2 * inv2 / width * jnp.sum(cot * base, axis=1, keepdims=True)
    weighted2 = (inv2 * cot).astype(BF16)
    grad1 = dot_nt(weighted2, b1h) - factor2 * two_b1
    act1 = grad1 * sig1 * (1.0 + pre1 * (1.0 - sig1))
    factor1 = inv1 * inv1 * inv1 / width * jnp.sum(act1 * proj1, axis=1, keepdims=True)
    weighted1 = (inv1 * act1).astype(BF16)
    grad0 = dot_nt(weighted2, b0h) - factor2 * two_b0 + dot_nt(weighted1, m01) - factor1 * one_b0
    act0 = grad0 * sig0 * (1.0 + pre0 * (1.0 - sig0))
    weighted0 = (inv0 * act0).astype(BF16)
    scaled0 = ((factor2 + factor1) * hid0).astype(BF16)
    scaled1 = (factor2 * hid1).astype(BF16)
    front = (hidden0, weighted2, scaled0, weighted0, weighted1, scaled1)
    back = (hidden1, weighted2, scaled1, weighted1, hidden0, hidden0)
    for slot, (a, b) in enumerate(zip(front, back)):
        mine_ref[slot * half : (slot + 1) * half, :] = jnp.where(first, a, b)
        theirs_ref[slot * half : (slot + 1) * half, :] = jnp.where(first, b, a)


def products(made):
    half = made.shape[0] // 6
    first = lax.axis_index("section") == 0
    hidden, last, scaled, weighted, extra1, extra2 = (made[i * half : (i + 1) * half] for i in range(6))
    hidden_t, scaled_t, weighted_t = (transposed(v) for v in (hidden, -scaled, weighted))
    mixes = (
        dot(hidden_t, last),
        dot(scaled_t, hidden),
        dot(jnp.where(first, -hidden_t, scaled_t), extra2),
        dot(jnp.where(first, hidden_t, weighted_t), extra1),
    )
    return mixes, weighted_t, scaled_t


def mine_kernel(made_ref, x_ref, mix_ref, acc_ref, left_ref):
    rank = made_ref.shape[1]
    half = made_ref.shape[0] // 6
    x = x_ref[rows_of(lax.axis_index("section") * half, half), :]
    mixes, weighted_t, scaled_t = products(made_ref[...])
    for i, mix in enumerate(mixes):
        mix_ref[i * rank : (i + 1) * rank, :] = mix
    left_ref[:rank, :] = weighted_t
    left_ref[rank:, :] = scaled_t
    acc_ref[:rank, :] = dot(weighted_t, x)
    acc_ref[rank:, :] = dot(scaled_t, x)


def grad_kernel(
    replicas, sections, made_ref, mix_ref, acc_ref, left_ref, stack_ref, down_t_ref, gain_ref, valid_ref, *refs
):
    out_refs, (all_ref, tall_ref) = refs[:replicas], refs[replicas:]
    rank, features = down_t_ref.shape
    slim = rank // replicas
    section = lax.axis_index("section")
    first = section == 0
    mixes, weighted_t, scaled_t = products(made_ref[...])
    mixes = [(m + mix_ref[i * rank : (i + 1) * rank, :]).astype(BF16) for i, m in enumerate(mixes)]
    for i, mix in enumerate(mixes):
        tall_ref[i * rank : (i + 1) * rank, :] = mix
    tall_ref[rows_of((4 + section) * rank, rank), :] = left_ref[:rank, :]
    tall_ref[rows_of((5 - section) * rank, rank), :] = weighted_t
    tall_ref[rows_of((6 + section) * rank, rank), :] = left_ref[rank:, :]
    tall_ref[rows_of((7 - section) * rank, rank), :] = scaled_t
    head_mix, own_mix, oth_mix, mix = mixes
    none = jnp.zeros_like(mix)
    left = jnp.concatenate([jnp.where(first, none, mix), weighted_t], axis=1)
    grad = acc_ref[:rank, :] + dot(left, stack_ref[3 * rank :, :])
    gain = jnp.sum(grad * down_t_ref[...].astype(F32), axis=0, keepdims=True)
    grad = (grad * gain_ref[...]).astype(BF16)
    left = jnp.concatenate([head_mix, own_mix, oth_mix, jnp.where(first, mix, none), scaled_t], axis=1)
    rest = (acc_ref[rank:, :] + dot(left, stack_ref[...])).astype(BF16)
    for c in range(replicas):
        all_ref[2 * c * slim : (2 * c + 1) * slim, :] = grad[c * slim : (c + 1) * slim]
        all_ref[(2 * c + 1) * slim : (2 * c + 2) * slim, :] = rest[c * slim : (c + 1) * slim]
    count = jnp.sum(valid_ref[...].astype(F32), keepdims=True)
    lines = features // rank
    tail = jnp.concatenate(
        [gain[:, i * rank : (i + 1) * rank] for i in range(lines)] + [jnp.broadcast_to(count, (PACK - lines, rank))],
        axis=0,
    ).astype(BF16)
    place = lax.axis_index("dp")
    for step, out_ref in enumerate(out_refs):
        target = partner(place, step, replicas)
        if step < replicas - sections:
            block = all_ref[rows_of(target * 2 * slim, 2 * slim), :]
            for i in range(lines):
                out_ref[i * 2 * slim : (i + 1) * 2 * slim, :] = block[:, i * rank : (i + 1) * rank]
        else:
            for i in range(8):
                out_ref[i * slim : (i + 1) * slim, :] = tall_ref[rows_of(i * rank + target * slim, slim), :]
        out_ref[-PACK:, :] = tail


def last_kernel(whole, *refs):
    parts, (far_ref, cross_ref, stack_ref, gain_ref, down_out, up_out, gain_out) = refs[:-7], refs[-7:]
    near, (a_ref, b_ref) = parts[:whole], parts[whole:]
    rank = a_ref.shape[1]
    slim, features = down_out.shape
    lines = features // rank
    first = lax.axis_index("section") == 0

    def total(start, size):
        return sum(p[start : start + size, :].astype(F32) for p in near)

    def left(ref):
        rows = [ref[i * slim : (i + 1) * slim, :] for i in range(4, 8)]
        return jnp.concatenate([jnp.concatenate(rows[:2], axis=1), jnp.concatenate(rows[2:], axis=1)], axis=0)

    tail = sum(p[-PACK:, :].astype(F32) for p in parts)
    scale = 1.0 / tail[lines : lines + 1, :1]
    left_a, left_b = left(a_ref), left(b_ref)
    moved = dot(jnp.where(first, left_a, left_b), far_ref[...])
    moved = moved + dot(jnp.where(first, left_b, left_a), cross_ref[...])
    mixes = [
        (a_ref[i * slim : (i + 1) * slim, :].astype(F32) + b_ref[i * slim : (i + 1) * slim, :].astype(F32)).astype(BF16)
        for i in range(4)
    ]
    none = jnp.zeros_like(mixes[3])
    down = moved[:slim] + dot(jnp.where(first, none, mixes[3]), stack_ref[3 * rank : 4 * rank, :])
    down = down * gain_ref[...]
    mixes = jnp.concatenate(mixes[:3] + [jnp.where(first, mixes[3], none)], axis=1)
    up = moved[slim:] + dot(mixes, stack_ref[: 4 * rank, :])
    for i in range(lines):
        lanes = slice(i * rank, (i + 1) * rank)
        down_out[:, lanes] = (total(i * 2 * slim, slim) + down[:, lanes]) * scale
        up_out[:, lanes] = (total((2 * i + 1) * slim, slim) + up[:, lanes]) * scale
        gain_out[:, lanes] = tail[i : i + 1, :] * scale


def local(inputs, adapter_down, adapter_up, gains, head, labels, valid):
    sections, tensors, replicas = (lax.axis_size(a) for a in ("section", "tensor", "dp"))
    features = inputs.shape[2]
    width = features * tensors
    rank = adapter_down.shape[2]
    states = inputs.reshape(-1, features)
    half = states.shape[0] // sections
    assert sections == 2 and half == rank and head.shape[1] == rank and features % rank == 0
    slim = rank // replicas
    lines = features // rank
    down, up = adapter_down[0], adapter_up[0]
    labels, valid = labels.reshape(sections, half), valid.reshape(sections, half)
    shape = jax.ShapeDtypeStruct

    others = []
    for value in (down, up, gains):
        others.append(from_partner(value, "section", 1))
    down2, up2, gains2 = others
    whole = replicas - sections
    assert whole > 0
    far = lax.ppermute(
        states,
        ("section", "dp"),
        [(s * replicas + i, s * replicas + partner(i, whole + s, replicas)) for s in range(sections) for i in range(replicas)],
    )
    small = 2 * rank * rank * features
    wide_gain = call(gain_kernel, shape(gains.shape, F32), 40 * small, gains)
    own = call(
        own_kernel,
        shape((3 * half + 2 * rank + PACK, rank), BF16),
        5 * small,
        states, down, up, head, wide_gain,
    )
    packed, gram = call(
        other_kernel,
        [shape((5 * half + PACK, rank), BF16), shape((3 * rank, rank), BF16)],
        3 * small,
        states, up, own, down2, up2, gains2,
    )
    wide = [packed]
    for step in range(1, tensors):
        wide.append(from_partner(packed, "tensor", step))
    down_t, stack = call(
        prepare_kernel,
        [shape((rank, features), BF16), shape((4 * rank + half, features), BF16)],
        small,
        down, head, up, down2, up2, gains2, states,
    )
    if tensors & (tensors - 1) == 0:
        step = 1
        while step < tensors:
            gram = call(add_kernel, shape(gram.shape, BF16), small // 8, gram, from_partner(gram, "tensor", step))
            step *= 2
    else:
        gram = call(
            add_kernel,
            shape(gram.shape, BF16),
            small // 8,
            gram,
            *(from_partner(gram, "tensor", step) for step in range(1, tensors)),
        )
    gram2 = from_partner(gram, "section", 1)
    made, theirs = call(
        functools.partial(chain_kernel, width, tensors),
        [shape((6 * half, rank), BF16)] * 2,
        16 * 2 * half * rank * rank,
        *wide, gram, gram2, labels, valid,
    )
    met = from_partner(theirs, "section", 1)
    mixes, acc, left = call(
        mine_kernel,
        [shape((4 * rank, rank), F32), shape((2 * rank, features), F32), shape((2 * rank, half), BF16)],
        4 * small,
        made, states,
    )
    *parts, _, _ = call(
        functools.partial(grad_kernel, replicas, sections),
        [shape((lines * 2 * slim + PACK, rank), BF16)] * whole
        + [shape((8 * slim + PACK, rank), BF16)] * sections
        + [shape((2 * rank, features), BF16), shape((8 * rank, rank), BF16)],
        16 * small,
        met, mixes, acc, left, stack, down_t, wide_gain, valid,
    )
    for step in range(1, replicas):
        parts[step] = from_partner(parts[step], "dp", step)
    cross = from_partner(far, "section", 1)
    down_grad, up_grad, gain_grad = call(
        functools.partial(last_kernel, whole),
        [shape((slim, features), F32), shape((slim, features), F32), shape((1, features), F32)],
        2 * small,
        *parts, far, cross, stack, wide_gain,
    )
    return down_grad.T[None], up_grad[None], gain_grad


def solution(mesh):
    return jax.shard_map(
        local,
        mesh=mesh,
        in_specs=(
            P(None, "dp", "tensor"),
            P("section", "tensor", None),
            P("section", None, "tensor"),
            P("section", "tensor"),
            P("tensor", None),
            P(None, "dp"),
            P(None, "dp"),
        ),
        out_specs=(
            P("section", "tensor", "dp"),
            P("section", "dp", "tensor"),
            P("section", "tensor"),
        ),
        check_vma=False,
    )
```

```python
import functools

import jax
import jax.numpy as jnp
from jax import lax
from jax.experimental import pallas as pl
from jax.experimental.pallas import tpu as pltpu
from jax.sharding import PartitionSpec as P


epsilon = 1e-05
F32 = jnp.float32
BF16 = jnp.bfloat16
PACK = 16


def dot(a, b):
    return jnp.dot(a, b, preferred_element_type=F32)


def dot_nt(a, b):
    return lax.dot_general(a, b, (((1,), (1,)), ((), ())), preferred_element_type=F32)


def rows_of(start, count):
    return pl.ds(pl.multiple_of(start, count), count)


def transposed(value):
    return value.astype(F32).T.astype(value.dtype)


def partner(index, step, size):
    if size & (size - 1) == 0:
        return index ^ step
    return (index + step) % size


def from_partner(value, axis, step):
    size = lax.axis_size(axis)
    return lax.ppermute(value, axis, [(i, partner(i, step, size)) for i in range(size)])


def high_low(value):
    high = value.astype(BF16).astype(F32)
    return jnp.concatenate([high, value - high], axis=0).astype(BF16)


def call(kernel, out, flops, *args):
    moved = sum(a.size * a.dtype.itemsize for a in args)
    return pl.pallas_call(
        kernel,
        out_shape=out,
        cost_estimate=pl.CostEstimate(flops=flops, bytes_accessed=moved, transcendentals=0),
        compiler_params=pltpu.CompilerParams(vmem_limit_bytes=24 * 2**20),
    )(*args)


def gain_kernel(gain_ref, out_ref):
    out_ref[...] = gain_ref[...].astype(F32)


def own_kernel(x_ref, down_ref, up_ref, head_ref, gain_ref, out_ref):
    rank = down_ref.shape[1]
    half = x_ref.shape[0] // lax.axis_size("section")
    x, up, head = x_ref[rows_of(lax.axis_index("section") * half, half), :], up_ref[...], head_ref[...]
    x32 = x.astype(F32)
    scaled = (x32 * gain_ref[...]).astype(BF16)
    out_ref[:half, :] = dot(scaled, down_ref[...]).astype(BF16)
    out_ref[half : 2 * half, :] = dot_nt(x, up).astype(BF16)
    out_ref[2 * half : 3 * half, :] = dot(x, head).astype(BF16)
    out_ref[3 * half : 3 * half + rank, :] = dot(up, head).astype(BF16)
    out_ref[3 * half + rank : 3 * half + 2 * rank, :] = dot_nt(up, up).astype(BF16)
    squares = jnp.sum(x32 * x32, axis=1, keepdims=True)
    squares = jnp.broadcast_to(squares, (half, rank)).T
    out_ref[3 * half + 2 * rank :, :] = high_low(squares[: PACK // 2])


def other_kernel(x_ref, up_ref, own_ref, down2_ref, up2_ref, gain2_ref, a_ref, b_ref, gram_ref):
    rank = down2_ref.shape[1]
    half = x_ref.shape[0] // lax.axis_size("section")
    me = lax.axis_index("section")
    it = 1 - me
    x = x_ref[rows_of(me * half, half), :]
    gain2 = gain2_ref[...].astype(F32)
    middle = 5 * half // 2
    a_ref[rows_of(me * half, half), :] = own_ref[:half, :]
    b_ref[rows_of(me * half, half), :] = own_ref[half : 2 * half, :]
    a_ref[2 * half : middle, :] = own_ref[2 * half : middle, :]
    b_ref[2 * half : middle, :] = own_ref[middle : 3 * half, :]
    a_ref[middle:, :] = own_ref[3 * half + 2 * rank :, :]
    gram_ref[rank:, :] = own_ref[3 * half : 3 * half + 2 * rank, :]
    scaled = (x.astype(F32) * gain2).astype(BF16)
    a_ref[rows_of(it * half, half), :] = dot(scaled, down2_ref[...]).astype(BF16)
    b_ref[rows_of(it * half, half), :] = dot_nt(x, up2_ref[...]).astype(BF16)

    @pl.when(me == 0)
    def _():
        scaled = (up_ref[...].astype(F32) * gain2).astype(BF16)
        gram_ref[:rank, :] = dot(scaled, down2_ref[...]).astype(BF16)

    @pl.when(me != 0)
    def _():
        gram_ref[:rank, :] = dot_nt(up_ref[...], up2_ref[...]).astype(BF16)


def add_kernel(*refs):
    refs[-1][...] = sum(r[...].astype(F32) for r in refs[:-1]).astype(BF16)


def prepare_kernel(down_ref, head_ref, up_ref, down2_ref, up2_ref, gain2_ref, x_ref, down_t_ref, stack_ref):
    rank = up_ref.shape[0]
    half = x_ref.shape[0] // lax.axis_size("section")
    down_t_ref[...] = transposed(down_ref[...])
    stack_ref[:rank, :] = transposed(head_ref[...])
    stack_ref[rank : 2 * rank, :] = up_ref[...]
    stack_ref[2 * rank : 3 * rank, :] = up2_ref[...]
    me = lax.axis_index("section")

    @pl.when(me == 0)
    def _():
        stack_ref[3 * rank : 4 * rank, :] = (down2_ref[...].astype(F32).T * gain2_ref[...].astype(F32)).astype(BF16)

    @pl.when(me != 0)
    def _():
        stack_ref[3 * rank : 4 * rank, :] = up2_ref[...]

    stack_ref[4 * rank :, :] = x_ref[rows_of((1 - me) * half, half), :]


def chain_kernel(width, count, *refs):
    a_refs, b_refs = refs[:count], refs[count : 2 * count]
    gram_ref, gram2_ref, label_ref, valid_ref, mine_ref, theirs_ref = refs[2 * count :]
    rank = gram_ref.shape[1]
    half = label_ref.shape[1]
    me = lax.axis_index("section")
    first = me == 0

    def total(parts, start, size):
        return sum(r[start : start + size, :].astype(F32) for r in parts)

    def spread(row):
        return jnp.broadcast_to(row, (rank, half)).T

    gram, gram2 = gram_ref[...], gram2_ref[...]
    gram0, gram1 = jnp.where(first, gram, gram2), jnp.where(first, gram2, gram)
    m01, b0h, b0b0 = (gram0[i * rank : (i + 1) * rank] for i in range(3))
    b1b0, b1h, b1b1 = (gram1[i * rank : (i + 1) * rank] for i in range(3))
    middle = 5 * half // 2
    tail = total(a_refs, middle, PACK)
    squares0 = spread(tail[:1] + tail[PACK // 2 : PACK // 2 + 1])
    inv0 = lax.rsqrt(squares0 / width + epsilon)
    proj0 = total(a_refs, 0, half)
    pre0 = inv0 * proj0
    sig0 = jax.nn.sigmoid(pre0)
    hidden0 = (pre0 * sig0).astype(BF16)
    hid0 = hidden0.astype(F32)
    proj1 = total(a_refs, half, half) + dot(hidden0, m01)
    cross0 = total(b_refs, 0, half)
    one_b0 = cross0 + dot(hidden0, b0b0)
    squares1 = squares0 + jnp.sum(hid0 * (cross0 + one_b0), axis=1, keepdims=True)
    inv1 = lax.rsqrt(squares1 / width + epsilon)
    pre1 = inv1 * proj1
    sig1 = jax.nn.sigmoid(pre1)
    hidden1 = (pre1 * sig1).astype(BF16)
    hid1 = hidden1.astype(F32)
    one_b1 = total(b_refs, half, half) + dot_nt(hidden0, b1b0)
    two_b0 = one_b0 + dot(hidden1, b1b0)
    two_b1 = one_b1 + dot(hidden1, b1b1)
    squares2 = squares1 + jnp.sum(hid1 * (one_b1 + two_b1), axis=1, keepdims=True)
    inv2 = lax.rsqrt(squares2 / width + epsilon)
    base = jnp.concatenate([total(r, 2 * half, half // 2) for r in (a_refs, b_refs)], axis=0)
    base = base + dot(hidden0, b0h) + dot(hidden1, b1h)
    logits = inv2 * base
    expo = jnp.exp(logits - jnp.max(logits, axis=1, keepdims=True))
    prob = expo / jnp.sum(expo, axis=1, keepdims=True)
    labels = spread(label_ref[pl.ds(me, 1), :].astype(F32))
    valid = spread(valid_ref[pl.ds(me, 1), :].astype(F32))
    classes = lax.broadcasted_iota(jnp.int32, logits.shape, 1).astype(F32)
    cot = (prob - (classes == labels).astype(F32)) * valid
    factor2 = inv2 * inv2 * inv2 / width * jnp.sum(cot * base, axis=1, keepdims=True)
    weighted2 = (inv2 * cot).astype(BF16)
    grad1 = dot_nt(weighted2, b1h) - factor2 * two_b1
    act1 = grad1 * sig1 * (1.0 + pre1 * (1.0 - sig1))
    factor1 = inv1 * inv1 * inv1 / width * jnp.sum(act1 * proj1, axis=1, keepdims=True)
    weighted1 = (inv1 * act1).astype(BF16)
    grad0 = dot_nt(weighted2, b0h) - factor2 * two_b0 + dot_nt(weighted1, m01) - factor1 * one_b0
    act0 = grad0 * sig0 * (1.0 + pre0 * (1.0 - sig0))
    weighted0 = (inv0 * act0).astype(BF16)
    scaled0 = ((factor2 + factor1) * hid0).astype(BF16)
    scaled1 = (factor2 * hid1).astype(BF16)
    front = (hidden0, weighted2, scaled0, weighted0, weighted1, scaled1)
    back = (hidden1, weighted2, scaled1, weighted1, hidden0, hidden0)
    for slot, (a, b) in enumerate(zip(front, back)):
        mine_ref[slot * half : (slot + 1) * half, :] = jnp.where(first, a, b)
        theirs_ref[slot * half : (slot + 1) * half, :] = jnp.where(first, b, a)


def products(made):
    half = made.shape[0] // 6
    first = lax.axis_index("section") == 0
    hidden, last, scaled, weighted, extra1, extra2 = (made[i * half : (i + 1) * half] for i in range(6))
    hidden_t, scaled_t, weighted_t = (transposed(v) for v in (hidden, -scaled, weighted))
    mixes = (
        dot(hidden_t, last),
        dot(scaled_t, hidden),
        dot(jnp.where(first, -hidden_t, scaled_t), extra2),
        dot(jnp.where(first, hidden_t, weighted_t), extra1),
    )
    return mixes, weighted_t, scaled_t


def mine_kernel(made_ref, x_ref, mix_ref, acc_ref, left_ref):
    rank = made_ref.shape[1]
    half = made_ref.shape[0] // 6
    x = x_ref[rows_of(lax.axis_index("section") * half, half), :]
    mixes, weighted_t, scaled_t = products(made_ref[...])
    for i, mix in enumerate(mixes):
        mix_ref[i * rank : (i + 1) * rank, :] = mix
    left_ref[:rank, :] = weighted_t
    left_ref[rank:, :] = scaled_t
    acc_ref[:rank, :] = dot(weighted_t, x)
    acc_ref[rank:, :] = dot(scaled_t, x)


def grad_kernel(
    replicas, sections, made_ref, mix_ref, acc_ref, left_ref, stack_ref, down_t_ref, gain_ref, valid_ref, *refs
):
    out_refs, (all_ref, tall_ref) = refs[:replicas], refs[replicas:]
    rank, features = down_t_ref.shape
    slim = rank // replicas
    section = lax.axis_index("section")
    first = section == 0
    mixes, weighted_t, scaled_t = products(made_ref[...])
    mixes = [(m + mix_ref[i * rank : (i + 1) * rank, :]).astype(BF16) for i, m in enumerate(mixes)]
    for i, mix in enumerate(mixes):
        tall_ref[i * rank : (i + 1) * rank, :] = mix
    tall_ref[rows_of((4 + section) * rank, rank), :] = left_ref[:rank, :]
    tall_ref[rows_of((5 - section) * rank, rank), :] = weighted_t
    tall_ref[rows_of((6 + section) * rank, rank), :] = left_ref[rank:, :]
    tall_ref[rows_of((7 - section) * rank, rank), :] = scaled_t
    head_mix, own_mix, oth_mix, mix = mixes
    none = jnp.zeros_like(mix)
    left = jnp.concatenate([jnp.where(first, none, mix), weighted_t], axis=1)
    grad = acc_ref[:rank, :] + dot(left, stack_ref[3 * rank :, :])
    gain = jnp.sum(grad * down_t_ref[...].astype(F32), axis=0, keepdims=True)
    grad = (grad * gain_ref[...]).astype(BF16)
    left = jnp.concatenate([head_mix, own_mix, oth_mix, jnp.where(first, mix, none), scaled_t], axis=1)
    rest = (acc_ref[rank:, :] + dot(left, stack_ref[...])).astype(BF16)
    for c in range(replicas):
        all_ref[2 * c * slim : (2 * c + 1) * slim, :] = grad[c * slim : (c + 1) * slim]
        all_ref[(2 * c + 1) * slim : (2 * c + 2) * slim, :] = rest[c * slim : (c + 1) * slim]
    count = jnp.sum(valid_ref[...].astype(F32), keepdims=True)
    lines = features // rank
    tail = jnp.concatenate(
        [gain[:, i * rank : (i + 1) * rank] for i in range(lines)] + [jnp.broadcast_to(count, (PACK - lines, rank))],
        axis=0,
    ).astype(BF16)
    place = lax.axis_index("dp")
    for step, out_ref in enumerate(out_refs):
        target = partner(place, step, replicas)
        if step < replicas - sections:
            block = all_ref[rows_of(target * 2 * slim, 2 * slim), :]
            for i in range(lines):
                out_ref[i * 2 * slim : (i + 1) * 2 * slim, :] = block[:, i * rank : (i + 1) * rank]
        else:
            for i in range(8):
                out_ref[i * slim : (i + 1) * slim, :] = tall_ref[rows_of(i * rank + target * slim, slim), :]
        out_ref[-PACK:, :] = tail


def last_kernel(whole, *refs):
    parts, (far_ref, cross_ref, stack_ref, gain_ref, down_out, up_out, gain_out) = refs[:-7], refs[-7:]
    near, (a_ref, b_ref) = parts[:whole], parts[whole:]
    rank = a_ref.shape[1]
    slim, features = down_out.shape
    lines = features // rank
    first = lax.axis_index("section") == 0

    def total(start, size):
        return sum(p[start : start + size, :].astype(F32) for p in near)

    def left(ref):
        rows = [ref[i * slim : (i + 1) * slim, :] for i in range(4, 8)]
        return jnp.concatenate([jnp.concatenate(rows[:2], axis=1), jnp.concatenate(rows[2:], axis=1)], axis=0)

    tail = sum(p[-PACK:, :].astype(F32) for p in parts)
    scale = 1.0 / tail[lines : lines + 1, :1]
    left_a, left_b = left(a_ref), left(b_ref)
    moved = dot(jnp.where(first, left_a, left_b), far_ref[...])
    moved = moved + dot(jnp.where(first, left_b, left_a), cross_ref[...])
    mixes = [
        (a_ref[i * slim : (i + 1) * slim, :].astype(F32) + b_ref[i * slim : (i + 1) * slim, :].astype(F32)).astype(BF16)
        for i in range(4)
    ]
    none = jnp.zeros_like(mixes[3])
    down = moved[:slim] + dot(jnp.where(first, none, mixes[3]), stack_ref[3 * rank : 4 * rank, :])
    down = down * gain_ref[...]
    mixes = jnp.concatenate(mixes[:3] + [jnp.where(first, mixes[3], none)], axis=1)
    up = moved[slim:] + dot(mixes, stack_ref[: 4 * rank, :])
    for i in range(lines):
        lanes = slice(i * rank, (i + 1) * rank)
        down_out[:, lanes] = (total(i * 2 * slim, slim) + down[:, lanes]) * scale
        up_out[:, lanes] = (total((2 * i + 1) * slim, slim) + up[:, lanes]) * scale
        gain_out[:, lanes] = tail[i : i + 1, :] * scale


def local(inputs, adapter_down, adapter_up, gains, head, labels, valid):
    sections, tensors, replicas = (lax.axis_size(a) for a in ("section", "tensor", "dp"))
    features = inputs.shape[2]
    width = features * tensors
    rank = adapter_down.shape[2]
    states = inputs.reshape(-1, features)
    half = states.shape[0] // sections
    assert sections == 2 and half == rank and head.shape[1] == rank and features % rank == 0
    slim = rank // replicas
    lines = features // rank
    down, up = adapter_down[0], adapter_up[0]
    labels, valid = labels.reshape(sections, half), valid.reshape(sections, half)
    shape = jax.ShapeDtypeStruct

    others = []
    for value in (down, up, gains):
        others.append(from_partner(value, "section", 1))
    down2, up2, gains2 = others
    whole = replicas - sections
    assert whole > 0
    far = lax.ppermute(
        states,
        ("section", "dp"),
        [(s * replicas + i, s * replicas + partner(i, whole + s, replicas)) for s in range(sections) for i in range(replicas)],
    )
    small = 2 * rank * rank * features
    wide_gain = call(gain_kernel, shape(gains.shape, F32), 40 * small, gains)
    own = call(
        own_kernel,
        shape((3 * half + 2 * rank + PACK, rank), BF16),
        5 * small,
        states, down, up, head, wide_gain,
    )
    lower = 5 * half // 2
    first_part, second_part, gram = call(
        other_kernel,
        [shape((lower + PACK, rank), BF16), shape((lower, rank), BF16), shape((3 * rank, rank), BF16)],
        3 * small,
        states, up, own, down2, up2, gains2,
    )
    doubling = [1 << i for i in range(tensors.bit_length() - 1)]

    def terms(value, steps):
        if tensors & (tensors - 1):
            return [value] + [from_partner(value, "tensor", step) for step in range(1, tensors)]
        for hop, step in enumerate(steps):
            got = from_partner(value, "tensor", step)
            if hop + 1 == len(steps):
                return [value, got]
            value = call(add_kernel, shape(value.shape, BF16), small // 8, value, got)

    gram = terms(gram, doubling)
    second_part = terms(second_part, doubling[::-1])
    first_part = terms(first_part, doubling)
    gram = call(add_kernel, shape(gram[0].shape, BF16), small // 8, *gram)
    down_t, stack = call(
        prepare_kernel,
        [shape((rank, features), BF16), shape((4 * rank + half, features), BF16)],
        small,
        down, head, up, down2, up2, gains2, states,
    )
    gram2 = from_partner(gram, "section", 1)
    made, theirs = call(
        functools.partial(chain_kernel, width, len(first_part)),
        [shape((6 * half, rank), BF16)] * 2,
        16 * 2 * half * rank * rank,
        *first_part, *second_part, gram, gram2, labels, valid,
    )
    met = from_partner(theirs, "section", 1)
    mixes, acc, left = call(
        mine_kernel,
        [shape((4 * rank, rank), F32), shape((2 * rank, features), F32), shape((2 * rank, half), BF16)],
        4 * small,
        made, states,
    )
    *parts, _, _ = call(
        functools.partial(grad_kernel, replicas, sections),
        [shape((lines * 2 * slim + PACK, rank), BF16)] * whole
        + [shape((8 * slim + PACK, rank), BF16)] * sections
        + [shape((2 * rank, features), BF16), shape((8 * rank, rank), BF16)],
        16 * small,
        met, mixes, acc, left, stack, down_t, wide_gain, valid,
    )
    for step in range(1, replicas):
        parts[step] = from_partner(parts[step], "dp", step)
    cross = from_partner(far, "section", 1)
    down_grad, up_grad, gain_grad = call(
        functools.partial(last_kernel, whole),
        [shape((slim, features), F32), shape((slim, features), F32), shape((1, features), F32)],
        2 * small,
        *parts, far, cross, stack, wide_gain,
    )
    return down_grad.T[None], up_grad[None], gain_grad


def solution(mesh):
    return jax.shard_map(
        local,
        mesh=mesh,
        in_specs=(
            P(None, "dp", "tensor"),
            P("section", "tensor", None),
            P("section", None, "tensor"),
            P("section", "tensor"),
            P("tensor", None),
            P(None, "dp"),
            P(None, "dp"),
        ),
        out_specs=(
            P("section", "tensor", "dp"),
            P("section", "dp", "tensor"),
            P("section", "tensor"),
        ),
        check_vma=False,
    )
```

```python
import functools

import jax
import jax.numpy as jnp
from jax import lax
from jax.experimental import pallas as pl
from jax.experimental.pallas import tpu as pltpu
from jax.sharding import PartitionSpec as P


epsilon = 1e-05
F32 = jnp.float32
BF16 = jnp.bfloat16
PACK = 16


def dot(a, b):
    return jnp.dot(a, b, preferred_element_type=F32)


def dot_nt(a, b):
    return lax.dot_general(a, b, (((1,), (1,)), ((), ())), preferred_element_type=F32)


def rows_of(start, count):
    return pl.ds(pl.multiple_of(start, count), count)


def transposed(value):
    return value.astype(F32).T.astype(value.dtype)


def partner(index, step, size):
    if size & (size - 1) == 0:
        return index ^ step
    return (index + step) % size


def from_partner(value, axis, step):
    size = lax.axis_size(axis)
    return lax.ppermute(value, axis, [(i, partner(i, step, size)) for i in range(size)])


def high_low(value):
    high = value.astype(BF16).astype(F32)
    return jnp.concatenate([high, value - high], axis=0).astype(BF16)


def call(kernel, out, flops, *args):
    moved = sum(a.size * a.dtype.itemsize for a in args)
    return pl.pallas_call(
        kernel,
        out_shape=out,
        cost_estimate=pl.CostEstimate(flops=flops, bytes_accessed=moved, transcendentals=0),
        compiler_params=pltpu.CompilerParams(vmem_limit_bytes=24 * 2**20),
    )(*args)


def gain_kernel(gain_ref, out_ref):
    out_ref[...] = gain_ref[...].astype(F32)


def own_kernel(x_ref, down_ref, up_ref, head_ref, gain_ref, out_ref, half_ref):
    rank = down_ref.shape[1]
    half = x_ref.shape[0] // lax.axis_size("section")
    x, up, head = x_ref[rows_of(lax.axis_index("section") * half, half), :], up_ref[...], head_ref[...]
    half_ref[...] = x
    x32 = x.astype(F32)
    scaled = (x32 * gain_ref[...]).astype(BF16)
    out_ref[:half, :] = dot(scaled, down_ref[...]).astype(BF16)
    out_ref[half : 2 * half, :] = dot_nt(x, up).astype(BF16)
    out_ref[2 * half : 3 * half, :] = dot(x, head).astype(BF16)
    out_ref[3 * half : 3 * half + rank, :] = dot(up, head).astype(BF16)
    out_ref[3 * half + rank : 3 * half + 2 * rank, :] = dot_nt(up, up).astype(BF16)
    squares = jnp.sum(x32 * x32, axis=1, keepdims=True)
    squares = jnp.broadcast_to(squares, (half, rank)).T
    out_ref[3 * half + 2 * rank :, :] = high_low(squares[: PACK // 2])


def other_kernel(x_ref, up_ref, own_ref, down2_ref, up2_ref, gain2_ref, a_ref, b_ref, gram_ref):
    rank = down2_ref.shape[1]
    half = x_ref.shape[0] // lax.axis_size("section")
    me = lax.axis_index("section")
    it = 1 - me
    x = x_ref[rows_of(me * half, half), :]
    gain2 = gain2_ref[...].astype(F32)
    middle = 5 * half // 2
    a_ref[rows_of(me * half, half), :] = own_ref[:half, :]
    b_ref[rows_of(me * half, half), :] = own_ref[half : 2 * half, :]
    a_ref[2 * half : middle, :] = own_ref[2 * half : middle, :]
    b_ref[2 * half : middle, :] = own_ref[middle : 3 * half, :]
    a_ref[middle:, :] = own_ref[3 * half + 2 * rank :, :]
    gram_ref[rank:, :] = own_ref[3 * half : 3 * half + 2 * rank, :]
    scaled = (x.astype(F32) * gain2).astype(BF16)
    a_ref[rows_of(it * half, half), :] = dot(scaled, down2_ref[...]).astype(BF16)
    b_ref[rows_of(it * half, half), :] = dot_nt(x, up2_ref[...]).astype(BF16)

    @pl.when(me == 0)
    def _():
        scaled = (up_ref[...].astype(F32) * gain2).astype(BF16)
        gram_ref[:rank, :] = dot(scaled, down2_ref[...]).astype(BF16)

    @pl.when(me != 0)
    def _():
        gram_ref[:rank, :] = dot_nt(up_ref[...], up2_ref[...]).astype(BF16)


def add_kernel(*refs):
    refs[-1][...] = sum(r[...].astype(F32) for r in refs[:-1]).astype(BF16)


def prepare_kernel(down_ref, head_ref, up_ref, down2_ref, up2_ref, gain2_ref, x_ref, down_t_ref, stack_ref):
    rank = up_ref.shape[0]
    half = x_ref.shape[0] // lax.axis_size("section")
    down_t_ref[...] = transposed(down_ref[...])
    stack_ref[:rank, :] = transposed(head_ref[...])
    stack_ref[rank : 2 * rank, :] = up_ref[...]
    stack_ref[2 * rank : 3 * rank, :] = up2_ref[...]
    me = lax.axis_index("section")

    @pl.when(me == 0)
    def _():
        stack_ref[3 * rank : 4 * rank, :] = (down2_ref[...].astype(F32).T * gain2_ref[...].astype(F32)).astype(BF16)

    @pl.when(me != 0)
    def _():
        stack_ref[3 * rank : 4 * rank, :] = up2_ref[...]

    stack_ref[4 * rank :, :] = x_ref[rows_of((1 - me) * half, half), :]


def chain_kernel(width, count, *refs):
    a_refs, b_refs = refs[:count], refs[count : 2 * count]
    gram_ref, gram2_ref, label_ref, valid_ref, mine_ref, theirs_ref = refs[2 * count :]
    rank = gram_ref.shape[1]
    half = label_ref.shape[1]
    me = lax.axis_index("section")
    first = me == 0

    def total(parts, start, size):
        return sum(r[start : start + size, :].astype(F32) for r in parts)

    def spread(row):
        return jnp.broadcast_to(row, (rank, half)).T

    gram, gram2 = gram_ref[...], gram2_ref[...]
    gram0, gram1 = jnp.where(first, gram, gram2), jnp.where(first, gram2, gram)
    m01, b0h, b0b0 = (gram0[i * rank : (i + 1) * rank] for i in range(3))
    b1b0, b1h, b1b1 = (gram1[i * rank : (i + 1) * rank] for i in range(3))
    middle = 5 * half // 2
    tail = total(a_refs, middle, PACK)
    squares0 = spread(tail[:1] + tail[PACK // 2 : PACK // 2 + 1])
    inv0 = lax.rsqrt(squares0 / width + epsilon)
    proj0 = total(a_refs, 0, half)
    pre0 = inv0 * proj0
    sig0 = jax.nn.sigmoid(pre0)
    hidden0 = (pre0 * sig0).astype(BF16)
    hid0 = hidden0.astype(F32)
    proj1 = total(a_refs, half, half) + dot(hidden0, m01)
    cross0 = total(b_refs, 0, half)
    one_b0 = cross0 + dot(hidden0, b0b0)
    squares1 = squares0 + jnp.sum(hid0 * (cross0 + one_b0), axis=1, keepdims=True)
    inv1 = lax.rsqrt(squares1 / width + epsilon)
    pre1 = inv1 * proj1
    sig1 = jax.nn.sigmoid(pre1)
    hidden1 = (pre1 * sig1).astype(BF16)
    hid1 = hidden1.astype(F32)
    one_b1 = total(b_refs, half, half) + dot_nt(hidden0, b1b0)
    two_b0 = one_b0 + dot(hidden1, b1b0)
    two_b1 = one_b1 + dot(hidden1, b1b1)
    squares2 = squares1 + jnp.sum(hid1 * (one_b1 + two_b1), axis=1, keepdims=True)
    inv2 = lax.rsqrt(squares2 / width + epsilon)
    base = jnp.concatenate([total(r, 2 * half, half // 2) for r in (a_refs, b_refs)], axis=0)
    base = base + dot(hidden0, b0h) + dot(hidden1, b1h)
    logits = inv2 * base
    expo = jnp.exp(logits - jnp.max(logits, axis=1, keepdims=True))
    prob = expo / jnp.sum(expo, axis=1, keepdims=True)
    labels = spread(label_ref[pl.ds(me, 1), :].astype(F32))
    valid = spread(valid_ref[pl.ds(me, 1), :].astype(F32))
    classes = lax.broadcasted_iota(jnp.int32, logits.shape, 1).astype(F32)
    cot = (prob - (classes == labels).astype(F32)) * valid
    factor2 = inv2 * inv2 * inv2 / width * jnp.sum(cot * base, axis=1, keepdims=True)
    weighted2 = (inv2 * cot).astype(BF16)
    grad1 = dot_nt(weighted2, b1h) - factor2 * two_b1
    act1 = grad1 * sig1 * (1.0 + pre1 * (1.0 - sig1))
    factor1 = inv1 * inv1 * inv1 / width * jnp.sum(act1 * proj1, axis=1, keepdims=True)
    weighted1 = (inv1 * act1).astype(BF16)
    grad0 = dot_nt(weighted2, b0h) - factor2 * two_b0 + dot_nt(weighted1, m01) - factor1 * one_b0
    act0 = grad0 * sig0 * (1.0 + pre0 * (1.0 - sig0))
    weighted0 = (inv0 * act0).astype(BF16)
    scaled0 = ((factor2 + factor1) * hid0).astype(BF16)
    scaled1 = (factor2 * hid1).astype(BF16)
    front = (hidden0, weighted2, scaled0, weighted0, weighted1, scaled1)
    back = (hidden1, weighted2, scaled1, weighted1, hidden0, hidden0)
    for slot, (a, b) in enumerate(zip(front, back)):
        mine_ref[slot * half : (slot + 1) * half, :] = jnp.where(first, a, b)
        theirs_ref[slot * half : (slot + 1) * half, :] = jnp.where(first, b, a)


def products(made):
    half = made.shape[0] // 6
    first = lax.axis_index("section") == 0
    hidden, last, scaled, weighted, extra1, extra2 = (made[i * half : (i + 1) * half] for i in range(6))
    hidden_t, scaled_t, weighted_t = (transposed(v) for v in (hidden, -scaled, weighted))
    mixes = (
        dot(hidden_t, last),
        dot(scaled_t, hidden),
        dot(jnp.where(first, -hidden_t, scaled_t), extra2),
        dot(jnp.where(first, hidden_t, weighted_t), extra1),
    )
    return mixes, weighted_t, scaled_t


def mine_kernel(made_ref, x_ref, mix_ref, acc_ref, left_ref):
    rank = made_ref.shape[1]
    half = made_ref.shape[0] // 6
    x = x_ref[rows_of(lax.axis_index("section") * half, half), :]
    mixes, weighted_t, scaled_t = products(made_ref[...])
    for i, mix in enumerate(mixes):
        mix_ref[i * rank : (i + 1) * rank, :] = mix
    left_ref[:rank, :] = weighted_t
    left_ref[rank:, :] = scaled_t
    acc_ref[:rank, :] = dot(weighted_t, x)
    acc_ref[rank:, :] = dot(scaled_t, x)


def grad_kernel(
    replicas, sections, made_ref, mix_ref, acc_ref, left_ref, stack_ref, down_t_ref, gain_ref, valid_ref, *refs
):
    out_refs, (all_ref, tall_ref) = refs[:replicas], refs[replicas:]
    rank, features = down_t_ref.shape
    slim = rank // replicas
    section = lax.axis_index("section")
    first = section == 0
    mixes, weighted_t, scaled_t = products(made_ref[...])
    mixes = [(m + mix_ref[i * rank : (i + 1) * rank, :]).astype(BF16) for i, m in enumerate(mixes)]
    for i, mix in enumerate(mixes):
        tall_ref[i * rank : (i + 1) * rank, :] = mix
    tall_ref[rows_of((4 + section) * rank, rank), :] = left_ref[:rank, :]
    tall_ref[rows_of((5 - section) * rank, rank), :] = weighted_t
    tall_ref[rows_of((6 + section) * rank, rank), :] = left_ref[rank:, :]
    tall_ref[rows_of((7 - section) * rank, rank), :] = scaled_t
    head_mix, own_mix, oth_mix, mix = mixes
    none = jnp.zeros_like(mix)
    left = jnp.concatenate([jnp.where(first, none, mix), weighted_t], axis=1)
    grad = acc_ref[:rank, :] + dot(left, stack_ref[3 * rank :, :])
    gain = jnp.sum(grad * down_t_ref[...].astype(F32), axis=0, keepdims=True)
    grad = (grad * gain_ref[...]).astype(BF16)
    left = jnp.concatenate([head_mix, own_mix, oth_mix, jnp.where(first, mix, none), scaled_t], axis=1)
    rest = (acc_ref[rank:, :] + dot(left, stack_ref[...])).astype(BF16)
    for c in range(replicas):
        all_ref[2 * c * slim : (2 * c + 1) * slim, :] = grad[c * slim : (c + 1) * slim]
        all_ref[(2 * c + 1) * slim : (2 * c + 2) * slim, :] = rest[c * slim : (c + 1) * slim]
    count = jnp.sum(valid_ref[...].astype(F32), keepdims=True)
    lines = features // rank
    tail = jnp.concatenate(
        [gain[:, i * rank : (i + 1) * rank] for i in range(lines)] + [jnp.broadcast_to(count, (PACK - lines, rank))],
        axis=0,
    ).astype(BF16)
    place = lax.axis_index("dp")
    for step, out_ref in enumerate(out_refs):
        target = partner(place, step, replicas)
        if step < replicas - sections:
            block = all_ref[rows_of(target * 2 * slim, 2 * slim), :]
            for i in range(lines):
                out_ref[i * 2 * slim : (i + 1) * 2 * slim, :] = block[:, i * rank : (i + 1) * rank]
        else:
            for i in range(8):
                out_ref[i * slim : (i + 1) * slim, :] = tall_ref[rows_of(i * rank + target * slim, slim), :]
        out_ref[-PACK:, :] = tail


def last_kernel(whole, *refs):
    parts, (far_refs, stack_ref, gain_ref, down_out, up_out, gain_out) = refs[:-9], (refs[-9:-5], *refs[-5:])
    near, (a_ref, b_ref) = parts[:whole], parts[whole:]
    rank = a_ref.shape[1]
    slim, features = down_out.shape
    lines = features // rank
    first = lax.axis_index("section") == 0

    def total(start, size):
        return sum(p[start : start + size, :].astype(F32) for p in near)

    def left(ref, i):
        rows = [ref[j * slim : (j + 1) * slim, :] for j in (4 + i, 6 + i)]
        return jnp.concatenate(rows, axis=0)

    tail = sum(p[-PACK:, :].astype(F32) for p in parts)
    scale = 1.0 / tail[lines : lines + 1, :1]
    moved = 0.0
    for i, ref in enumerate((a_ref, b_ref)):
        one, two = left(ref, 0), left(ref, 1)
        moved = moved + dot(jnp.where(first, one, two), far_refs[i][...])
        moved = moved + dot(jnp.where(first, two, one), far_refs[2 + i][...])
    mixes = [
        (a_ref[i * slim : (i + 1) * slim, :].astype(F32) + b_ref[i * slim : (i + 1) * slim, :].astype(F32)).astype(BF16)
        for i in range(4)
    ]
    none = jnp.zeros_like(mixes[3])
    down = moved[:slim] + dot(jnp.where(first, none, mixes[3]), stack_ref[3 * rank : 4 * rank, :])
    down = down * gain_ref[...]
    mixes = jnp.concatenate(mixes[:3] + [jnp.where(first, mixes[3], none)], axis=1)
    up = moved[slim:] + dot(mixes, stack_ref[: 4 * rank, :])
    for i in range(lines):
        lanes = slice(i * rank, (i + 1) * rank)
        down_out[:, lanes] = (total(i * 2 * slim, slim) + down[:, lanes]) * scale
        up_out[:, lanes] = (total((2 * i + 1) * slim, slim) + up[:, lanes]) * scale
        gain_out[:, lanes] = tail[i : i + 1, :] * scale


def local(inputs, adapter_down, adapter_up, gains, head, labels, valid):
    sections, tensors, replicas = (lax.axis_size(a) for a in ("section", "tensor", "dp"))
    features = inputs.shape[2]
    width = features * tensors
    rank = adapter_down.shape[2]
    states = inputs.reshape(-1, features)
    half = states.shape[0] // sections
    assert sections == 2 and half == rank and head.shape[1] == rank and features % rank == 0
    slim = rank // replicas
    lines = features // rank
    down, up = adapter_down[0], adapter_up[0]
    labels, valid = labels.reshape(sections, half), valid.reshape(sections, half)
    shape = jax.ShapeDtypeStruct

    others = []
    for value in (down, up, gains):
        others.append(from_partner(value, "section", 1))
    down2, up2, gains2 = others
    whole = replicas - sections
    assert whole > 0
    small = 2 * rank * rank * features
    wide_gain = call(gain_kernel, shape(gains.shape, F32), 40 * small, gains)
    own, mine = call(
        own_kernel,
        [shape((3 * half + 2 * rank + PACK, rank), BF16), shape((half, features), BF16)],
        5 * small,
        states, down, up, head, wide_gain,
    )
    far = from_partner(mine, "dp", whole)
    lower = 5 * half // 2
    first_part, second_part, gram = call(
        other_kernel,
        [shape((lower + PACK, rank), BF16), shape((lower, rank), BF16), shape((3 * rank, rank), BF16)],
        3 * small,
        states, up, own, down2, up2, gains2,
    )
    doubling = [1 << i for i in range(tensors.bit_length() - 1)]

    def terms(value, steps):
        if tensors & (tensors - 1):
            return [value] + [from_partner(value, "tensor", step) for step in range(1, tensors)]
        for hop, step in enumerate(steps):
            got = from_partner(value, "tensor", step)
            if hop + 1 == len(steps):
                return [value, got]
            value = call(add_kernel, shape(value.shape, BF16), small // 8, value, got)

    gram = terms(gram, doubling)
    second_part = terms(second_part, doubling[::-1])
    first_part = terms(first_part, doubling)
    gram = call(add_kernel, shape(gram[0].shape, BF16), small // 8, *gram)
    down_t, stack = call(
        prepare_kernel,
        [shape((rank, features), BF16), shape((4 * rank + half, features), BF16)],
        small,
        down, head, up, down2, up2, gains2, states,
    )
    gram2 = from_partner(gram, "section", 1)
    made, theirs = call(
        functools.partial(chain_kernel, width, len(first_part)),
        [shape((6 * half, rank), BF16)] * 2,
        16 * 2 * half * rank * rank,
        *first_part, *second_part, gram, gram2, labels, valid,
    )
    met = from_partner(theirs, "section", 1)
    fars = [far, from_partner(far, "dp", 1)]
    mixes, acc, left = call(
        mine_kernel,
        [shape((4 * rank, rank), F32), shape((2 * rank, features), F32), shape((2 * rank, half), BF16)],
        4 * small,
        made, states,
    )
    *parts, _, _ = call(
        functools.partial(grad_kernel, replicas, sections),
        [shape((lines * 2 * slim + PACK, rank), BF16)] * whole
        + [shape((8 * slim + PACK, rank), BF16)] * sections
        + [shape((2 * rank, features), BF16), shape((8 * rank, rank), BF16)],
        16 * small,
        met, mixes, acc, left, stack, down_t, wide_gain, valid,
    )
    for step in range(1, replicas):
        parts[step] = from_partner(parts[step], "dp", step)
    for i in range(2):
        fars.append(from_partner(fars[i], "section", 1))
    down_grad, up_grad, gain_grad = call(
        functools.partial(last_kernel, whole),
        [shape((slim, features), F32), shape((slim, features), F32), shape((1, features), F32)],
        2 * small,
        *parts, *fars, stack, wide_gain,
    )
    return down_grad.T[None], up_grad[None], gain_grad


def solution(mesh):
    return jax.shard_map(
        local,
        mesh=mesh,
        in_specs=(
            P(None, "dp", "tensor"),
            P("section", "tensor", None),
            P("section", None, "tensor"),
            P("section", "tensor"),
            P("tensor", None),
            P(None, "dp"),
            P(None, "dp"),
        ),
        out_specs=(
            P("section", "tensor", "dp"),
            P("section", "dp", "tensor"),
            P("section", "tensor"),
        ),
        check_vma=False,
    )
```

```python
import functools

import jax
import jax.numpy as jnp
from jax import lax
from jax.experimental import pallas as pl
from jax.experimental.pallas import tpu as pltpu
from jax.sharding import PartitionSpec as P


epsilon = 1e-05
F32 = jnp.float32
BF16 = jnp.bfloat16
PACK = 16


def dot(a, b):
    return jnp.dot(a, b, preferred_element_type=F32)


def dot_nt(a, b):
    return lax.dot_general(a, b, (((1,), (1,)), ((), ())), preferred_element_type=F32)


def rows_of(start, count):
    return pl.ds(pl.multiple_of(start, count), count)


def transposed(value):
    return value.astype(F32).T.astype(value.dtype)


def partner(index, step, size):
    if size & (size - 1) == 0:
        return index ^ step
    return (index + step) % size


def from_partner(value, axis, step):
    size = lax.axis_size(axis)
    return lax.ppermute(value, axis, [(i, partner(i, step, size)) for i in range(size)])


def from_section(value, steps):
    size = lax.axis_size("dp")
    pairs = [(s * size + i, s * size + partner(i, step, size)) for s, step in enumerate(steps) for i in range(size)]
    return lax.ppermute(value, ("section", "dp"), pairs)


def high_low(value):
    high = value.astype(BF16).astype(F32)
    return jnp.concatenate([high, value - high], axis=0).astype(BF16)


def call(kernel, out, flops, *args):
    moved = sum(a.size * a.dtype.itemsize for a in args)
    return pl.pallas_call(
        kernel,
        out_shape=out,
        cost_estimate=pl.CostEstimate(flops=flops, bytes_accessed=moved, transcendentals=0),
        compiler_params=pltpu.CompilerParams(vmem_limit_bytes=24 * 2**20),
    )(*args)


def open_kernel(out_ref):
    out_ref[...] = jnp.zeros_like(out_ref)


def own_kernel(x_ref, down_ref, up_ref, head_ref, gain_ref, _, out_ref):
    rank = down_ref.shape[1]
    half = x_ref.shape[0] // lax.axis_size("section")
    x, up, head = x_ref[rows_of(lax.axis_index("section") * half, half), :], up_ref[...], head_ref[...]
    x32 = x.astype(F32)
    scaled = (x32 * gain_ref[...].astype(F32)).astype(BF16)
    out_ref[:half, :] = dot(scaled, down_ref[...]).astype(BF16)
    out_ref[half : 2 * half, :] = dot_nt(x, up).astype(BF16)
    out_ref[2 * half : 3 * half, :] = dot(x, head).astype(BF16)
    out_ref[3 * half : 3 * half + rank, :] = dot(up, head).astype(BF16)
    out_ref[3 * half + rank : 3 * half + 2 * rank, :] = dot_nt(up, up).astype(BF16)
    squares = jnp.sum(x32 * x32, axis=1, keepdims=True)
    squares = jnp.broadcast_to(squares, (half, rank)).T
    out_ref[3 * half + 2 * rank :, :] = high_low(squares[: PACK // 2])


def other_kernel(x_ref, up_ref, own_ref, down2_ref, up2_ref, gain2_ref, a_ref, b_ref):
    rank = down2_ref.shape[1]
    half = x_ref.shape[0] // lax.axis_size("section")
    me = lax.axis_index("section")
    it = 1 - me
    x = x_ref[rows_of(me * half, half), :]
    gain2 = gain2_ref[...].astype(F32)
    b_ref[rows_of(me * half, half), :] = own_ref[:half, :]
    b_ref[rows_of((2 + me) * half, half), :] = own_ref[half : 2 * half, :]
    a_ref[rank : 3 * rank, :] = own_ref[3 * half : 3 * half + 2 * rank, :]
    a_ref[3 * rank : 3 * rank + half, :] = own_ref[2 * half : 3 * half, :]
    a_ref[3 * rank + half :, :] = own_ref[3 * half + 2 * rank :, :]
    scaled = (x.astype(F32) * gain2).astype(BF16)
    b_ref[rows_of(it * half, half), :] = dot(scaled, down2_ref[...]).astype(BF16)
    b_ref[rows_of((2 + it) * half, half), :] = dot_nt(x, up2_ref[...]).astype(BF16)

    @pl.when(me == 0)
    def _():
        scaled = (up_ref[...].astype(F32) * gain2).astype(BF16)
        a_ref[:rank, :] = dot(scaled, down2_ref[...]).astype(BF16)

    @pl.when(me != 0)
    def _():
        a_ref[:rank, :] = dot_nt(up_ref[...], up2_ref[...]).astype(BF16)


def add_kernel(*refs):
    rows = refs[-1].shape[0]
    refs[-1][...] = sum(r[:rows, :].astype(F32) for r in refs[:-1]).astype(BF16)


def prepare_kernel(down_ref, head_ref, up_ref, down2_ref, up2_ref, gain2_ref, x_ref, down_t_ref, stack_ref):
    rank = up_ref.shape[0]
    half = x_ref.shape[0] // lax.axis_size("section")
    down_t_ref[...] = transposed(down_ref[...])
    stack_ref[:rank, :] = transposed(head_ref[...])
    stack_ref[rank : 2 * rank, :] = up_ref[...]
    stack_ref[2 * rank : 3 * rank, :] = up2_ref[...]
    me = lax.axis_index("section")

    @pl.when(me == 0)
    def _():
        stack_ref[3 * rank : 4 * rank, :] = (down2_ref[...].astype(F32).T * gain2_ref[...].astype(F32)).astype(BF16)

    @pl.when(me != 0)
    def _():
        stack_ref[3 * rank : 4 * rank, :] = up2_ref[...]

    stack_ref[4 * rank :, :] = x_ref[rows_of((1 - me) * half, half), :]


def chain_kernel(width, count, *refs):
    a_refs, b_refs = refs[:count], refs[count : 2 * count]
    gram_ref, gram2_ref, label_ref, valid_ref, mine_ref, theirs_ref = refs[2 * count :]
    rank = gram_ref.shape[1]
    half = label_ref.shape[1]
    me = lax.axis_index("section")
    first = me == 0

    def total(parts, start, size):
        return sum(r[start : start + size, :].astype(F32) for r in parts)

    def spread(row):
        return jnp.broadcast_to(row, (rank, half)).T

    gram, gram2 = gram_ref[...], gram2_ref[...]
    gram0, gram1 = jnp.where(first, gram, gram2), jnp.where(first, gram2, gram)
    m01, b0h, b0b0 = (gram0[i * rank : (i + 1) * rank] for i in range(3))
    b1b0, b1h, b1b1 = (gram1[i * rank : (i + 1) * rank] for i in range(3))
    tail = total(a_refs, 3 * rank + half, PACK)
    squares0 = spread(tail[:1] + tail[PACK // 2 : PACK // 2 + 1])
    inv0 = lax.rsqrt(squares0 / width + epsilon)
    proj0 = total(b_refs, 0, half)
    pre0 = inv0 * proj0
    sig0 = jax.nn.sigmoid(pre0)
    hidden0 = (pre0 * sig0).astype(BF16)
    hid0 = hidden0.astype(F32)
    proj1 = total(b_refs, half, half) + dot(hidden0, m01)
    cross0 = total(b_refs, 2 * half, half)
    one_b0 = cross0 + dot(hidden0, b0b0)
    squares1 = squares0 + jnp.sum(hid0 * (cross0 + one_b0), axis=1, keepdims=True)
    inv1 = lax.rsqrt(squares1 / width + epsilon)
    pre1 = inv1 * proj1
    sig1 = jax.nn.sigmoid(pre1)
    hidden1 = (pre1 * sig1).astype(BF16)
    hid1 = hidden1.astype(F32)
    one_b1 = total(b_refs, 3 * half, half) + dot_nt(hidden0, b1b0)
    two_b0 = one_b0 + dot(hidden1, b1b0)
    two_b1 = one_b1 + dot(hidden1, b1b1)
    squares2 = squares1 + jnp.sum(hid1 * (one_b1 + two_b1), axis=1, keepdims=True)
    inv2 = lax.rsqrt(squares2 / width + epsilon)
    base = total(a_refs, 3 * rank, half) + dot(hidden0, b0h) + dot(hidden1, b1h)
    logits = inv2 * base
    expo = jnp.exp(logits - jnp.max(logits, axis=1, keepdims=True))
    prob = expo / jnp.sum(expo, axis=1, keepdims=True)
    labels = spread(label_ref[pl.ds(me, 1), :].astype(F32))
    valid = spread(valid_ref[pl.ds(me, 1), :].astype(F32))
    classes = lax.broadcasted_iota(jnp.int32, logits.shape, 1).astype(F32)
    cot = (prob - (classes == labels).astype(F32)) * valid
    factor2 = inv2 * inv2 * inv2 / width * jnp.sum(cot * base, axis=1, keepdims=True)
    weighted2 = (inv2 * cot).astype(BF16)
    grad1 = dot_nt(weighted2, b1h) - factor2 * two_b1
    act1 = grad1 * sig1 * (1.0 + pre1 * (1.0 - sig1))
    factor1 = inv1 * inv1 * inv1 / width * jnp.sum(act1 * proj1, axis=1, keepdims=True)
    weighted1 = (inv1 * act1).astype(BF16)
    grad0 = dot_nt(weighted2, b0h) - factor2 * two_b0 + dot_nt(weighted1, m01) - factor1 * one_b0
    act0 = grad0 * sig0 * (1.0 + pre0 * (1.0 - sig0))
    weighted0 = (inv0 * act0).astype(BF16)
    scaled0 = ((factor2 + factor1) * hid0).astype(BF16)
    scaled1 = (factor2 * hid1).astype(BF16)
    front = (hidden0, weighted2, scaled0, weighted0, weighted1, scaled1)
    back = (hidden1, weighted2, scaled1, weighted1, hidden0, hidden0)
    for slot, (a, b) in enumerate(zip(front, back)):
        mine_ref[slot * half : (slot + 1) * half, :] = jnp.where(first, a, b)
        theirs_ref[slot * half : (slot + 1) * half, :] = jnp.where(first, b, a)


def products(made):
    half = made.shape[0] // 6
    first = lax.axis_index("section") == 0
    hidden, last, scaled, weighted, extra1, extra2 = (made[i * half : (i + 1) * half] for i in range(6))
    hidden_t, scaled_t, weighted_t = (transposed(v) for v in (hidden, -scaled, weighted))
    mixes = (
        dot(hidden_t, last),
        dot(scaled_t, hidden),
        dot(jnp.where(first, -hidden_t, scaled_t), extra2),
        dot(jnp.where(first, hidden_t, weighted_t), extra1),
    )
    return mixes, weighted_t, scaled_t


def mine_kernel(near, made_ref, x_ref, mix_ref, acc_ref, left_ref):
    rank = made_ref.shape[1]
    half = made_ref.shape[0] // 6
    x = x_ref[rows_of(lax.axis_index("section") * half, half), :]
    mixes, weighted_t, scaled_t = products(made_ref[...])
    for i, mix in enumerate(mixes):
        mix_ref[i * rank : (i + 1) * rank, :] = mix
    left_ref[:rank, :] = weighted_t
    left_ref[rank:, :] = scaled_t
    acc_ref[:rank, :] = dot(weighted_t, x)
    slim = (acc_ref.shape[0] - rank) // len(near)
    place = lax.axis_index("dp")
    for i, step in enumerate(near):
        rows = left_ref[rows_of(rank + partner(place, step, rank // slim) * slim, slim), :]
        acc_ref[rank + i * slim : rank + (i + 1) * slim, :] = dot(rows, x)


def grad_kernel(
    replicas, near, made_ref, mix_ref, acc_ref, left_ref, stack_ref, down_t_ref, gain_ref, valid_ref, *refs
):
    out_refs, (all_ref, tall_ref, wide_ref) = refs[:replicas], refs[replicas:]
    rank, features = down_t_ref.shape
    slim = rank // replicas
    section = lax.axis_index("section")
    first = section == 0
    mixes, weighted_t, scaled_t = products(made_ref[...])
    mixes = [(m + mix_ref[i * rank : (i + 1) * rank, :]).astype(BF16) for i, m in enumerate(mixes)]
    for i, mix in enumerate(mixes):
        tall_ref[i * rank : (i + 1) * rank, :] = mix
    tall_ref[rows_of((4 + section) * rank, rank), :] = left_ref[:rank, :]
    tall_ref[rows_of((5 - section) * rank, rank), :] = weighted_t
    tall_ref[rows_of((6 + section) * rank, rank), :] = left_ref[rank:, :]
    tall_ref[rows_of((7 - section) * rank, rank), :] = scaled_t
    head_mix, own_mix, oth_mix, mix = mixes
    none = jnp.zeros_like(mix)
    left = jnp.concatenate([jnp.where(first, none, mix), weighted_t], axis=1)
    grad = acc_ref[:rank, :] + dot(left, stack_ref[3 * rank :, :])
    gain = jnp.sum(grad * down_t_ref[...].astype(F32), axis=0, keepdims=True)
    grad = (grad * gain_ref[...].astype(F32)).astype(BF16)
    all_ref[...] = grad
    for i, value in enumerate((head_mix, own_mix, oth_mix, jnp.where(first, mix, none), scaled_t)):
        wide_ref[:, i * rank : (i + 1) * rank] = value
    place = lax.axis_index("dp")
    targets = [partner(place, step, replicas) for step in range(replicas)]
    left = jnp.concatenate([wide_ref[rows_of(t * slim, slim), :] for t in (targets[i] for i in near)], axis=0)
    rest = (acc_ref[rank:, :] + dot(left, stack_ref[...])).astype(BF16)
    count = jnp.sum(valid_ref[...].astype(F32), keepdims=True)
    lines = features // rank
    tail = jnp.concatenate(
        [gain[:, i * rank : (i + 1) * rank] for i in range(lines)] + [jnp.broadcast_to(count, (PACK - lines, rank))],
        axis=0,
    ).astype(BF16)
    for step, out_ref in enumerate(out_refs):
        if step in near:
            at = near.index(step) * slim
            block = all_ref[rows_of(targets[step] * slim, slim), :]
            for i in range(lines):
                lanes = slice(i * rank, (i + 1) * rank)
                out_ref[i * 2 * slim : (2 * i + 1) * slim, :] = block[:, lanes]
                out_ref[(2 * i + 1) * slim : (i + 1) * 2 * slim, :] = rest[at : at + slim, lanes]
        else:
            for i in range(8):
                out_ref[i * slim : (i + 1) * slim, :] = tall_ref[rows_of(i * rank + targets[step] * slim, slim), :]
        out_ref[-PACK:, :] = tail


def last_kernel(count, *refs):
    near, fars, refs = refs[:count], refs[count : count + 3], refs[count + 3 :]
    sent_ref, relay_ref, cross_ref, cross2_ref, stack_ref, gain_ref, down_out, up_out, gain_out = refs
    rank = fars[0].shape[1]
    slim, features = down_out.shape
    lines = features // rank
    first = lax.axis_index("section") == 0

    def total(start, size):
        return sum(p[start : start + size, :].astype(F32) for p in near)

    def left(ref):
        rows = [ref[i * slim : (i + 1) * slim, :] for i in range(4, 8)]
        return jnp.concatenate([jnp.concatenate(rows[:2], axis=1), jnp.concatenate(rows[2:], axis=1)], axis=0)

    tail = sum(p[-PACK:, :].astype(F32) for p in near + fars)
    scale = 1.0 / tail[lines : lines + 1, :1]
    left_a, left_b, left_c = (left(r) for r in fars)
    moved = dot(jnp.where(first, left_a, left_c), sent_ref[...]) + dot(jnp.where(first, left_c, left_a), cross_ref[...])
    moved = moved + dot(left_b, jnp.where(first, relay_ref[...], cross2_ref[...]))
    mixes = [sum(r[i * slim : (i + 1) * slim, :].astype(F32) for r in fars).astype(BF16) for i in range(4)]
    none = jnp.zeros_like(mixes[3])
    down = moved[:slim] + dot(jnp.where(first, none, mixes[3]), stack_ref[3 * rank : 4 * rank, :])
    down = down * gain_ref[...].astype(F32)
    mixes = jnp.concatenate(mixes[:3] + [jnp.where(first, mixes[3], none)], axis=1)
    up = moved[slim:] + dot(mixes, stack_ref[: 4 * rank, :])
    for i in range(lines):
        lanes = slice(i * rank, (i + 1) * rank)
        down_out[:, lanes] = (total(i * 2 * slim, slim) + down[:, lanes]) * scale
        up_out[:, lanes] = (total((2 * i + 1) * slim, slim) + up[:, lanes]) * scale
        gain_out[:, lanes] = tail[i : i + 1, :] * scale


def local(inputs, adapter_down, adapter_up, gains, head, labels, valid):
    sections, tensors, replicas = (lax.axis_size(a) for a in ("section", "tensor", "dp"))
    features = inputs.shape[2]
    width = features * tensors
    rank = adapter_down.shape[2]
    states = inputs.reshape(-1, features)
    half = states.shape[0] // sections
    assert sections == 2 and half == rank and head.shape[1] == rank and features % rank == 0
    slim = rank // replicas
    lines = features // rank
    down, up = adapter_down[0], adapter_up[0]
    labels, valid = labels.reshape(sections, half), valid.reshape(sections, half)
    shape = jax.ShapeDtypeStruct

    others = []
    for value in (down, up, gains):
        others.append(from_partner(value, "section", 1))
    down2, up2, gains2 = others
    assert replicas > 3
    far = [replicas - 2, replicas - 1, 1]
    near = [step for step in range(replicas) if step not in far]
    gathered = [from_section(states, [replicas - 2, 1])]
    small = 2 * rank * rank * features
    opened = call(open_kernel, shape((8, rank), F32), 40 * small)
    own = call(
        own_kernel,
        shape((3 * half + 2 * rank + PACK, rank), BF16),
        5 * small,
        states, down, up, head, gains, opened,
    )
    first_part, second_part = call(
        other_kernel,
        [shape((3 * rank + half + PACK, rank), BF16), shape((4 * half, rank), BF16)],
        3 * small,
        states, up, own, down2, up2, gains2,
    )
    doubling = [1 << i for i in range(tensors.bit_length() - 1)]

    def terms(value, steps):
        if tensors & (tensors - 1):
            return [value] + [from_partner(value, "tensor", step) for step in range(1, tensors)]
        for hop, step in enumerate(steps):
            got = from_partner(value, "tensor", step)
            if hop + 1 == len(steps):
                return [value, got]
            value = call(add_kernel, shape(value.shape, BF16), small // 8, value, got)

    first_part = terms(first_part, doubling)
    second_part = terms(second_part, doubling[::-1])
    gram = call(add_kernel, shape((3 * rank, rank), BF16), small // 8, *first_part)
    down_t, stack = call(
        prepare_kernel,
        [shape((rank, features), BF16), shape((4 * rank + half, features), BF16)],
        small,
        down, head, up, down2, up2, gains2, states,
    )
    gram2 = from_partner(gram, "section", 1)
    made, theirs = call(
        functools.partial(chain_kernel, width, len(first_part)),
        [shape((6 * half, rank), BF16)] * 2,
        16 * 2 * half * rank * rank,
        *first_part, *second_part, gram, gram2, labels, valid,
    )
    met = from_partner(theirs, "section", 1)
    gathered.append(from_section(gathered[0], [1]))
    mixes, acc, left = call(
        functools.partial(mine_kernel, near),
        [shape((4 * rank, rank), F32), shape((rank + len(near) * slim, features), F32), shape((2 * rank, half), BF16)],
        4 * small,
        made, states,
    )
    *parts, _, _, _ = call(
        functools.partial(grad_kernel, replicas, near),
        [shape(((lines * 2 if i in near else 8) * slim + PACK, rank), BF16) for i in range(replicas)]
        + [shape((rank, features), BF16), shape((8 * rank, rank), BF16), shape((rank, 5 * rank), BF16)],
        16 * small,
        met, mixes, acc, left, stack, down_t, gains, valid,
    )
    for step in range(1, replicas):
        parts[step] = from_partner(parts[step], "dp", step)
    for i in range(2):
        gathered.append(from_partner(gathered[i], "section", 1))
    down_grad, up_grad, gain_grad = call(
        functools.partial(last_kernel, len(near)),
        [shape((slim, features), F32), shape((slim, features), F32), shape((1, features), F32)],
        2 * small,
        *(parts[i] for i in near + far), *gathered, stack, gains,
    )
    return down_grad.T[None], up_grad[None], gain_grad


def solution(mesh):
    return jax.shard_map(
        local,
        mesh=mesh,
        in_specs=(
            P(None, "dp", "tensor"),
            P("section", "tensor", None),
            P("section", None, "tensor"),
            P("section", "tensor"),
            P("tensor", None),
            P(None, "dp"),
            P(None, "dp"),
        ),
        out_specs=(
            P("section", "tensor", "dp"),
            P("section", "dp", "tensor"),
            P("section", "tensor"),
        ),
        check_vma=False,
    )
```

```python
import functools

import jax
import jax.numpy as jnp
from jax import lax
from jax.experimental import pallas as pl
from jax.experimental.pallas import tpu as pltpu
from jax.sharding import PartitionSpec as P


epsilon = 1e-05
F32 = jnp.float32
BF16 = jnp.bfloat16
PACK = 16


def dot(a, b):
    return jnp.dot(a, b, preferred_element_type=F32)


def dot_nt(a, b):
    return lax.dot_general(a, b, (((1,), (1,)), ((), ())), preferred_element_type=F32)


def rows_of(start, count):
    return pl.ds(pl.multiple_of(start, count), count)


def transposed(value):
    return value.astype(F32).T.astype(value.dtype)


def partner(index, step, size):
    if size & (size - 1) == 0:
        return index ^ step
    return (index + step) % size


def from_partner(value, axis, step):
    size = lax.axis_size(axis)
    return lax.ppermute(value, axis, [(i, partner(i, step, size)) for i in range(size)])


def high_low(value):
    high = value.astype(BF16).astype(F32)
    return jnp.concatenate([high, value - high], axis=0).astype(BF16)


def call(kernel, out, flops, *args):
    moved = sum(a.size * a.dtype.itemsize for a in args)
    return pl.pallas_call(
        kernel,
        out_shape=out,
        cost_estimate=pl.CostEstimate(flops=flops, bytes_accessed=moved, transcendentals=0),
        compiler_params=pltpu.CompilerParams(vmem_limit_bytes=24 * 2**20),
    )(*args)


def open_kernel(out_ref):
    out_ref[...] = jnp.zeros_like(out_ref)


def own_kernel(x_ref, down_ref, up_ref, head_ref, gain_ref, _, out_ref, half_ref):
    rank = down_ref.shape[1]
    half = x_ref.shape[0] // lax.axis_size("section")
    x, up, head = x_ref[rows_of(lax.axis_index("section") * half, half), :], up_ref[...], head_ref[...]
    half_ref[...] = x
    x32 = x.astype(F32)
    scaled = (x32 * gain_ref[...].astype(F32)).astype(BF16)
    out_ref[:half, :] = dot(scaled, down_ref[...]).astype(BF16)
    out_ref[half : 2 * half, :] = dot_nt(x, up).astype(BF16)
    out_ref[2 * half : 3 * half, :] = dot(x, head).astype(BF16)
    out_ref[3 * half : 3 * half + rank, :] = dot(up, head).astype(BF16)
    out_ref[3 * half + rank : 3 * half + 2 * rank, :] = dot_nt(up, up).astype(BF16)
    squares = jnp.sum(x32 * x32, axis=1, keepdims=True)
    squares = jnp.broadcast_to(squares, (half, rank)).T
    out_ref[3 * half + 2 * rank :, :] = high_low(squares[: PACK // 2])


def other_kernel(x_ref, up_ref, own_ref, down2_ref, up2_ref, gain2_ref, a_ref, b_ref):
    rank = down2_ref.shape[1]
    half = x_ref.shape[0] // lax.axis_size("section")
    me = lax.axis_index("section")
    it = 1 - me
    x = x_ref[rows_of(me * half, half), :]
    gain2 = gain2_ref[...].astype(F32)
    b_ref[rows_of(me * half, half), :] = own_ref[:half, :]
    b_ref[rows_of((2 + me) * half, half), :] = own_ref[half : 2 * half, :]
    a_ref[rank : 3 * rank, :] = own_ref[3 * half : 3 * half + 2 * rank, :]
    a_ref[3 * rank : 3 * rank + half, :] = own_ref[2 * half : 3 * half, :]
    a_ref[3 * rank + half :, :] = own_ref[3 * half + 2 * rank :, :]
    scaled = (x.astype(F32) * gain2).astype(BF16)
    b_ref[rows_of(it * half, half), :] = dot(scaled, down2_ref[...]).astype(BF16)
    b_ref[rows_of((2 + it) * half, half), :] = dot_nt(x, up2_ref[...]).astype(BF16)

    @pl.when(me == 0)
    def _():
        scaled = (up_ref[...].astype(F32) * gain2).astype(BF16)
        a_ref[:rank, :] = dot(scaled, down2_ref[...]).astype(BF16)

    @pl.when(me != 0)
    def _():
        a_ref[:rank, :] = dot_nt(up_ref[...], up2_ref[...]).astype(BF16)


def add_kernel(*refs):
    rows = refs[-1].shape[0]
    refs[-1][...] = sum(r[:rows, :].astype(F32) for r in refs[:-1]).astype(BF16)


def prepare_kernel(down_ref, head_ref, up_ref, down2_ref, up2_ref, gain2_ref, x_ref, down_t_ref, stack_ref):
    rank = up_ref.shape[0]
    half = x_ref.shape[0] // lax.axis_size("section")
    down_t_ref[...] = transposed(down_ref[...])
    stack_ref[:rank, :] = transposed(head_ref[...])
    stack_ref[rank : 2 * rank, :] = up_ref[...]
    stack_ref[2 * rank : 3 * rank, :] = up2_ref[...]
    me = lax.axis_index("section")

    @pl.when(me == 0)
    def _():
        stack_ref[3 * rank : 4 * rank, :] = (down2_ref[...].astype(F32).T * gain2_ref[...].astype(F32)).astype(BF16)

    @pl.when(me != 0)
    def _():
        stack_ref[3 * rank : 4 * rank, :] = up2_ref[...]

    stack_ref[4 * rank :, :] = x_ref[rows_of((1 - me) * half, half), :]


def chain_kernel(width, count, *refs):
    a_refs, b_refs = refs[:count], refs[count : 2 * count]
    gram_ref, gram2_ref, label_ref, valid_ref, mine_ref, theirs_ref = refs[2 * count :]
    rank = gram_ref.shape[1]
    half = label_ref.shape[1]
    me = lax.axis_index("section")
    first = me == 0

    def total(parts, start, size):
        return sum(r[start : start + size, :].astype(F32) for r in parts)

    def spread(row):
        return jnp.broadcast_to(row, (rank, half)).T

    gram, gram2 = gram_ref[...], gram2_ref[...]
    gram0, gram1 = jnp.where(first, gram, gram2), jnp.where(first, gram2, gram)
    m01, b0h, b0b0 = (gram0[i * rank : (i + 1) * rank] for i in range(3))
    b1b0, b1h, b1b1 = (gram1[i * rank : (i + 1) * rank] for i in range(3))
    tail = total(a_refs, 3 * rank + half, PACK)
    squares0 = spread(tail[:1] + tail[PACK // 2 : PACK // 2 + 1])
    inv0 = lax.rsqrt(squares0 / width + epsilon)
    proj0 = total(b_refs, 0, half)
    pre0 = inv0 * proj0
    sig0 = jax.nn.sigmoid(pre0)
    hidden0 = (pre0 * sig0).astype(BF16)
    hid0 = hidden0.astype(F32)
    proj1 = total(b_refs, half, half) + dot(hidden0, m01)
    cross0 = total(b_refs, 2 * half, half)
    one_b0 = cross0 + dot(hidden0, b0b0)
    squares1 = squares0 + jnp.sum(hid0 * (cross0 + one_b0), axis=1, keepdims=True)
    inv1 = lax.rsqrt(squares1 / width + epsilon)
    pre1 = inv1 * proj1
    sig1 = jax.nn.sigmoid(pre1)
    hidden1 = (pre1 * sig1).astype(BF16)
    hid1 = hidden1.astype(F32)
    one_b1 = total(b_refs, 3 * half, half) + dot_nt(hidden0, b1b0)
    two_b0 = one_b0 + dot(hidden1, b1b0)
    two_b1 = one_b1 + dot(hidden1, b1b1)
    squares2 = squares1 + jnp.sum(hid1 * (one_b1 + two_b1), axis=1, keepdims=True)
    inv2 = lax.rsqrt(squares2 / width + epsilon)
    base = total(a_refs, 3 * rank, half) + dot(hidden0, b0h) + dot(hidden1, b1h)
    logits = inv2 * base
    expo = jnp.exp(logits - jnp.max(logits, axis=1, keepdims=True))
    prob = expo / jnp.sum(expo, axis=1, keepdims=True)
    labels = spread(label_ref[pl.ds(me, 1), :].astype(F32))
    valid = spread(valid_ref[pl.ds(me, 1), :].astype(F32))
    classes = lax.broadcasted_iota(jnp.int32, logits.shape, 1).astype(F32)
    cot = (prob - (classes == labels).astype(F32)) * valid
    factor2 = inv2 * inv2 * inv2 / width * jnp.sum(cot * base, axis=1, keepdims=True)
    weighted2 = (inv2 * cot).astype(BF16)
    grad1 = dot_nt(weighted2, b1h) - factor2 * two_b1
    act1 = grad1 * sig1 * (1.0 + pre1 * (1.0 - sig1))
    factor1 = inv1 * inv1 * inv1 / width * jnp.sum(act1 * proj1, axis=1, keepdims=True)
    weighted1 = (inv1 * act1).astype(BF16)
    grad0 = dot_nt(weighted2, b0h) - factor2 * two_b0 + dot_nt(weighted1, m01) - factor1 * one_b0
    act0 = grad0 * sig0 * (1.0 + pre0 * (1.0 - sig0))
    weighted0 = (inv0 * act0).astype(BF16)
    scaled0 = ((factor2 + factor1) * hid0).astype(BF16)
    scaled1 = (factor2 * hid1).astype(BF16)
    front = (hidden0, weighted2, scaled0, weighted0, weighted1, scaled1)
    back = (hidden1, weighted2, scaled1, weighted1, hidden0, hidden0)
    for slot, (a, b) in enumerate(zip(front, back)):
        mine_ref[slot * half : (slot + 1) * half, :] = jnp.where(first, a, b)
        theirs_ref[slot * half : (slot + 1) * half, :] = jnp.where(first, b, a)


def products(made):
    half = made.shape[0] // 6
    first = lax.axis_index("section") == 0
    hidden, last, scaled, weighted, extra1, extra2 = (made[i * half : (i + 1) * half] for i in range(6))
    hidden_t, scaled_t, weighted_t = (transposed(v) for v in (hidden, -scaled, weighted))
    mixes = (
        dot(hidden_t, last),
        dot(scaled_t, hidden),
        dot(jnp.where(first, -hidden_t, scaled_t), extra2),
        dot(jnp.where(first, hidden_t, weighted_t), extra1),
    )
    return mixes, weighted_t, scaled_t


def mine_kernel(whole, made_ref, x_ref, mix_ref, acc_ref, left_ref):
    rank = made_ref.shape[1]
    half = made_ref.shape[0] // 6
    x = x_ref[rows_of(lax.axis_index("section") * half, half), :]
    mixes, weighted_t, scaled_t = products(made_ref[...])
    for i, mix in enumerate(mixes):
        mix_ref[i * rank : (i + 1) * rank, :] = mix
    left_ref[:rank, :] = weighted_t
    left_ref[rank:, :] = scaled_t
    acc_ref[:rank, :] = dot(weighted_t, x)
    slim = (acc_ref.shape[0] - rank) // whole
    place = lax.axis_index("dp")
    for step in range(whole):
        rows = left_ref[rows_of(rank + partner(place, step, rank // slim) * slim, slim), :]
        acc_ref[rank + step * slim : rank + (step + 1) * slim, :] = dot(rows, x)


def grad_kernel(
    replicas, sections, made_ref, mix_ref, acc_ref, left_ref, stack_ref, down_t_ref, gain_ref, valid_ref, *refs
):
    out_refs, (all_ref, tall_ref, wide_ref) = refs[:replicas], refs[replicas:]
    whole = replicas - sections
    rank, features = down_t_ref.shape
    slim = rank // replicas
    section = lax.axis_index("section")
    first = section == 0
    mixes, weighted_t, scaled_t = products(made_ref[...])
    mixes = [(m + mix_ref[i * rank : (i + 1) * rank, :]).astype(BF16) for i, m in enumerate(mixes)]
    for i, mix in enumerate(mixes):
        tall_ref[i * rank : (i + 1) * rank, :] = mix
    tall_ref[rows_of((4 + section) * rank, rank), :] = left_ref[:rank, :]
    tall_ref[rows_of((5 - section) * rank, rank), :] = weighted_t
    tall_ref[rows_of((6 + section) * rank, rank), :] = left_ref[rank:, :]
    tall_ref[rows_of((7 - section) * rank, rank), :] = scaled_t
    head_mix, own_mix, oth_mix, mix = mixes
    none = jnp.zeros_like(mix)
    left = jnp.concatenate([jnp.where(first, none, mix), weighted_t], axis=1)
    grad = acc_ref[:rank, :] + dot(left, stack_ref[3 * rank :, :])
    gain = jnp.sum(grad * down_t_ref[...].astype(F32), axis=0, keepdims=True)
    grad = (grad * gain_ref[...].astype(F32)).astype(BF16)
    all_ref[...] = grad
    for i, value in enumerate((head_mix, own_mix, oth_mix, jnp.where(first, mix, none), scaled_t)):
        wide_ref[:, i * rank : (i + 1) * rank] = value
    place = lax.axis_index("dp")
    targets = [partner(place, step, replicas) for step in range(replicas)]
    left = jnp.concatenate([wide_ref[rows_of(t * slim, slim), :] for t in targets[:whole]], axis=0)
    rest = (acc_ref[rank:, :] + dot(left, stack_ref[...])).astype(BF16)
    count = jnp.sum(valid_ref[...].astype(F32), keepdims=True)
    lines = features // rank
    tail = jnp.concatenate(
        [gain[:, i * rank : (i + 1) * rank] for i in range(lines)] + [jnp.broadcast_to(count, (PACK - lines, rank))],
        axis=0,
    ).astype(BF16)
    for step, out_ref in enumerate(out_refs):
        if step < whole:
            block = all_ref[rows_of(targets[step] * slim, slim), :]
            for i in range(lines):
                lanes = slice(i * rank, (i + 1) * rank)
                out_ref[i * 2 * slim : (2 * i + 1) * slim, :] = block[:, lanes]
                out_ref[(2 * i + 1) * slim : (i + 1) * 2 * slim, :] = rest[step * slim : (step + 1) * slim, lanes]
        else:
            for i in range(8):
                out_ref[i * slim : (i + 1) * slim, :] = tall_ref[rows_of(i * rank + targets[step] * slim, slim), :]
        out_ref[-PACK:, :] = tail


def last_kernel(whole, *refs):
    parts, (far_refs, stack_ref, gain_ref, down_out, up_out, gain_out) = refs[:-9], (refs[-9:-5], *refs[-5:])
    near, (a_ref, b_ref) = parts[:whole], parts[whole:]
    rank = a_ref.shape[1]
    slim, features = down_out.shape
    lines = features // rank
    first = lax.axis_index("section") == 0

    def total(start, size):
        return sum(p[start : start + size, :].astype(F32) for p in near)

    def left(ref, i):
        rows = [ref[j * slim : (j + 1) * slim, :] for j in (4 + i, 6 + i)]
        return jnp.concatenate(rows, axis=0)

    tail = sum(p[-PACK:, :].astype(F32) for p in parts)
    scale = 1.0 / tail[lines : lines + 1, :1]
    moved = 0.0
    for i, ref in enumerate((a_ref, b_ref)):
        one, two = left(ref, 0), left(ref, 1)
        moved = moved + dot(jnp.where(first, one, two), far_refs[i][...])
        moved = moved + dot(jnp.where(first, two, one), far_refs[2 + i][...])
    mixes = [
        (a_ref[i * slim : (i + 1) * slim, :].astype(F32) + b_ref[i * slim : (i + 1) * slim, :].astype(F32)).astype(BF16)
        for i in range(4)
    ]
    none = jnp.zeros_like(mixes[3])
    down = moved[:slim] + dot(jnp.where(first, none, mixes[3]), stack_ref[3 * rank : 4 * rank, :])
    down = down * gain_ref[...].astype(F32)
    mixes = jnp.concatenate(mixes[:3] + [jnp.where(first, mixes[3], none)], axis=1)
    up = moved[slim:] + dot(mixes, stack_ref[: 4 * rank, :])
    for i in range(lines):
        lanes = slice(i * rank, (i + 1) * rank)
        down_out[:, lanes] = (total(i * 2 * slim, slim) + down[:, lanes]) * scale
        up_out[:, lanes] = (total((2 * i + 1) * slim, slim) + up[:, lanes]) * scale
        gain_out[:, lanes] = tail[i : i + 1, :] * scale


def local(inputs, adapter_down, adapter_up, gains, head, labels, valid):
    sections, tensors, replicas = (lax.axis_size(a) for a in ("section", "tensor", "dp"))
    features = inputs.shape[2]
    width = features * tensors
    rank = adapter_down.shape[2]
    states = inputs.reshape(-1, features)
    half = states.shape[0] // sections
    assert sections == 2 and half == rank and head.shape[1] == rank and features % rank == 0
    slim = rank // replicas
    lines = features // rank
    down, up = adapter_down[0], adapter_up[0]
    labels, valid = labels.reshape(sections, half), valid.reshape(sections, half)
    shape = jax.ShapeDtypeStruct

    others = []
    for value in (down, up, gains):
        others.append(from_partner(value, "section", 1))
    down2, up2, gains2 = others
    whole = replicas - sections
    assert whole > 0
    small = 2 * rank * rank * features
    opened = call(open_kernel, shape((8, rank), F32), 40 * small)
    own, mine = call(
        own_kernel,
        [shape((3 * half + 2 * rank + PACK, rank), BF16), shape((half, features), BF16)],
        5 * small,
        states, down, up, head, gains, opened,
    )
    far = from_partner(mine, "dp", whole)
    first_part, second_part = call(
        other_kernel,
        [shape((3 * rank + half + PACK, rank), BF16), shape((4 * half, rank), BF16)],
        3 * small,
        states, up, own, down2, up2, gains2,
    )
    doubling = [1 << i for i in range(tensors.bit_length() - 1)]

    def terms(value, steps):
        if tensors & (tensors - 1):
            return [value] + [from_partner(value, "tensor", step) for step in range(1, tensors)]
        for hop, step in enumerate(steps):
            got = from_partner(value, "tensor", step)
            if hop + 1 == len(steps):
                return [value, got]
            value = call(add_kernel, shape(value.shape, BF16), small // 8, value, got)

    first_part = terms(first_part, doubling)
    second_part = terms(second_part, doubling[::-1])
    gram = call(add_kernel, shape((3 * rank, rank), BF16), small // 8, *first_part)
    down_t, stack = call(
        prepare_kernel,
        [shape((rank, features), BF16), shape((4 * rank + half, features), BF16)],
        small,
        down, head, up, down2, up2, gains2, states,
    )
    gram2 = from_partner(gram, "section", 1)
    made, theirs = call(
        functools.partial(chain_kernel, width, len(first_part)),
        [shape((6 * half, rank), BF16)] * 2,
        16 * 2 * half * rank * rank,
        *first_part, *second_part, gram, gram2, labels, valid,
    )
    met = from_partner(theirs, "section", 1)
    fars = [far, from_partner(far, "dp", 1)]
    mixes, acc, left = call(
        functools.partial(mine_kernel, whole),
        [shape((4 * rank, rank), F32), shape((rank + whole * slim, features), F32), shape((2 * rank, half), BF16)],
        4 * small,
        made, states,
    )
    *parts, _, _, _ = call(
        functools.partial(grad_kernel, replicas, sections),
        [shape((lines * 2 * slim + PACK, rank), BF16)] * whole
        + [shape((8 * slim + PACK, rank), BF16)] * sections
        + [shape((rank, features), BF16), shape((8 * rank, rank), BF16), shape((rank, 5 * rank), BF16)],
        16 * small,
        met, mixes, acc, left, stack, down_t, gains, valid,
    )
    for step in range(1, replicas):
        parts[step] = from_partner(parts[step], "dp", step)
    for i in range(2):
        fars.append(from_partner(fars[i], "section", 1))
    down_grad, up_grad, gain_grad = call(
        functools.partial(last_kernel, whole),
        [shape((slim, features), F32), shape((slim, features), F32), shape((1, features), F32)],
        2 * small,
        *parts, *fars, stack, gains,
    )
    return down_grad.T[None], up_grad[None], gain_grad


def solution(mesh):
    return jax.shard_map(
        local,
        mesh=mesh,
        in_specs=(
            P(None, "dp", "tensor"),
            P("section", "tensor", None),
            P("section", None, "tensor"),
            P("section", "tensor"),
            P("tensor", None),
            P(None, "dp"),
            P(None, "dp"),
        ),
        out_specs=(
            P("section", "tensor", "dp"),
            P("section", "dp", "tensor"),
            P("section", "tensor"),
        ),
        check_vma=False,
    )
```

```python
import functools

import jax
import jax.numpy as jnp
from jax import lax
from jax.experimental import pallas as pl
from jax.experimental.pallas import tpu as pltpu
from jax.sharding import PartitionSpec as P


epsilon = 1e-05
F32 = jnp.float32
BF16 = jnp.bfloat16
PACK = 16


def dot(a, b):
    return jnp.dot(a, b, preferred_element_type=F32)


def dot_nt(a, b):
    return lax.dot_general(a, b, (((1,), (1,)), ((), ())), preferred_element_type=F32)


def rows_of(start, count):
    return pl.ds(pl.multiple_of(start, count), count)


def transposed(value):
    return value.astype(F32).T.astype(value.dtype)


def partner(index, step, size):
    if size & (size - 1) == 0:
        return index ^ step
    return (index + step) % size


def from_partner(value, axis, step):
    size = lax.axis_size(axis)
    return lax.ppermute(value, axis, [(i, partner(i, step, size)) for i in range(size)])


def high_low(value):
    high = value.astype(BF16).astype(F32)
    return jnp.concatenate([high, value - high], axis=0).astype(BF16)


def call(kernel, out, flops, *args):
    moved = sum(a.size * a.dtype.itemsize for a in args)
    return pl.pallas_call(
        kernel,
        out_shape=out,
        cost_estimate=pl.CostEstimate(flops=flops, bytes_accessed=moved, transcendentals=0),
        compiler_params=pltpu.CompilerParams(vmem_limit_bytes=24 * 2**20),
    )(*args)


def open_kernel(out_ref):
    out_ref[...] = jnp.zeros_like(out_ref)


def own_kernel(x_ref, down_ref, up_ref, head_ref, gain_ref, _, out_ref, half_ref):
    rank = down_ref.shape[1]
    half = x_ref.shape[0] // lax.axis_size("section")
    x, up, head = x_ref[rows_of(lax.axis_index("section") * half, half), :], up_ref[...], head_ref[...]
    half_ref[...] = x
    x32 = x.astype(F32)
    scaled = (x32 * gain_ref[...].astype(F32)).astype(BF16)
    out_ref[:half, :] = dot(scaled, down_ref[...]).astype(BF16)
    out_ref[half : 2 * half, :] = dot_nt(x, up).astype(BF16)
    out_ref[2 * half : 3 * half, :] = dot(x, head).astype(BF16)
    out_ref[3 * half : 3 * half + rank, :] = dot(up, head).astype(BF16)
    out_ref[3 * half + rank : 3 * half + 2 * rank, :] = dot_nt(up, up).astype(BF16)
    squares = jnp.sum(x32 * x32, axis=1, keepdims=True)
    squares = jnp.broadcast_to(squares, (half, rank)).T
    out_ref[3 * half + 2 * rank :, :] = high_low(squares[: PACK // 2])


def other_kernel(x_ref, up_ref, own_ref, down2_ref, up2_ref, gain2_ref, a_ref, b_ref):
    rank = down2_ref.shape[1]
    half = x_ref.shape[0] // lax.axis_size("section")
    me = lax.axis_index("section")
    it = 1 - me
    x = x_ref[rows_of(me * half, half), :]
    gain2 = gain2_ref[...].astype(F32)
    b_ref[rows_of(me * half, half), :] = own_ref[:half, :]
    b_ref[rows_of((2 + me) * half, half), :] = own_ref[half : 2 * half, :]
    a_ref[rank : 3 * rank, :] = own_ref[3 * half : 3 * half + 2 * rank, :]
    a_ref[3 * rank : 3 * rank + half, :] = own_ref[2 * half : 3 * half, :]
    a_ref[3 * rank + half :, :] = own_ref[3 * half + 2 * rank :, :]
    scaled = (x.astype(F32) * gain2).astype(BF16)
    b_ref[rows_of(it * half, half), :] = dot(scaled, down2_ref[...]).astype(BF16)
    b_ref[rows_of((2 + it) * half, half), :] = dot_nt(x, up2_ref[...]).astype(BF16)

    @pl.when(me == 0)
    def _():
        scaled = (up_ref[...].astype(F32) * gain2).astype(BF16)
        a_ref[:rank, :] = dot(scaled, down2_ref[...]).astype(BF16)

    @pl.when(me != 0)
    def _():
        a_ref[:rank, :] = dot_nt(up_ref[...], up2_ref[...]).astype(BF16)


def add_kernel(*refs):
    rows = refs[-1].shape[0]
    refs[-1][...] = sum(r[:rows, :].astype(F32) for r in refs[:-1]).astype(BF16)


def prepare_kernel(down_ref, head_ref, up_ref, down2_ref, up2_ref, gain2_ref, x_ref, down_t_ref, stack_ref):
    rank = up_ref.shape[0]
    half = x_ref.shape[0] // lax.axis_size("section")
    down_t_ref[...] = transposed(down_ref[...])
    stack_ref[:rank, :] = transposed(head_ref[...])
    stack_ref[rank : 2 * rank, :] = up_ref[...]
    stack_ref[2 * rank : 3 * rank, :] = up2_ref[...]
    me = lax.axis_index("section")

    @pl.when(me == 0)
    def _():
        stack_ref[3 * rank : 4 * rank, :] = (down2_ref[...].astype(F32).T * gain2_ref[...].astype(F32)).astype(BF16)

    @pl.when(me != 0)
    def _():
        stack_ref[3 * rank : 4 * rank, :] = up2_ref[...]

    stack_ref[4 * rank :, :] = x_ref[rows_of((1 - me) * half, half), :]


def chain_kernel(width, count, *refs):
    a_refs, b_refs = refs[:count], refs[count : 2 * count]
    gram_ref, gram2_ref, label_ref, valid_ref, mine_ref, theirs_ref = refs[2 * count :]
    rank = gram_ref.shape[1]
    half = label_ref.shape[1]
    me = lax.axis_index("section")
    first = me == 0

    def total(parts, start, size):
        return sum(r[start : start + size, :].astype(F32) for r in parts)

    def spread(row):
        return jnp.broadcast_to(row, (rank, half)).T

    gram, gram2 = gram_ref[...], gram2_ref[...]
    gram0, gram1 = jnp.where(first, gram, gram2), jnp.where(first, gram2, gram)
    m01, b0h, b0b0 = (gram0[i * rank : (i + 1) * rank] for i in range(3))
    b1b0, b1h, b1b1 = (gram1[i * rank : (i + 1) * rank] for i in range(3))
    tail = total(a_refs, 3 * rank + half, PACK)
    squares0 = spread(tail[:1] + tail[PACK // 2 : PACK // 2 + 1])
    inv0 = lax.rsqrt(squares0 / width + epsilon)
    proj0 = total(b_refs, 0, half)
    pre0 = inv0 * proj0
    sig0 = jax.nn.sigmoid(pre0)
    hidden0 = (pre0 * sig0).astype(BF16)
    hid0 = hidden0.astype(F32)
    proj1 = total(b_refs, half, half) + dot(hidden0, m01)
    cross0 = total(b_refs, 2 * half, half)
    one_b0 = cross0 + dot(hidden0, b0b0)
    squares1 = squares0 + jnp.sum(hid0 * (cross0 + one_b0), axis=1, keepdims=True)
    inv1 = lax.rsqrt(squares1 / width + epsilon)
    pre1 = inv1 * proj1
    sig1 = jax.nn.sigmoid(pre1)
    hidden1 = (pre1 * sig1).astype(BF16)
    hid1 = hidden1.astype(F32)
    one_b1 = total(b_refs, 3 * half, half) + dot_nt(hidden0, b1b0)
    two_b0 = one_b0 + dot(hidden1, b1b0)
    two_b1 = one_b1 + dot(hidden1, b1b1)
    squares2 = squares1 + jnp.sum(hid1 * (one_b1 + two_b1), axis=1, keepdims=True)
    inv2 = lax.rsqrt(squares2 / width + epsilon)
    base = total(a_refs, 3 * rank, half) + dot(hidden0, b0h) + dot(hidden1, b1h)
    logits = inv2 * base
    expo = jnp.exp(logits - jnp.max(logits, axis=1, keepdims=True))
    prob = expo / jnp.sum(expo, axis=1, keepdims=True)
    labels = spread(label_ref[pl.ds(me, 1), :].astype(F32))
    valid = spread(valid_ref[pl.ds(me, 1), :].astype(F32))
    classes = lax.broadcasted_iota(jnp.int32, logits.shape, 1).astype(F32)
    cot = (prob - (classes == labels).astype(F32)) * valid
    factor2 = inv2 * inv2 * inv2 / width * jnp.sum(cot * base, axis=1, keepdims=True)
    weighted2 = (inv2 * cot).astype(BF16)
    grad1 = dot_nt(weighted2, b1h) - factor2 * two_b1
    act1 = grad1 * sig1 * (1.0 + pre1 * (1.0 - sig1))
    factor1 = inv1 * inv1 * inv1 / width * jnp.sum(act1 * proj1, axis=1, keepdims=True)
    weighted1 = (inv1 * act1).astype(BF16)
    grad0 = dot_nt(weighted2, b0h) - factor2 * two_b0 + dot_nt(weighted1, m01) - factor1 * one_b0
    act0 = grad0 * sig0 * (1.0 + pre0 * (1.0 - sig0))
    weighted0 = (inv0 * act0).astype(BF16)
    scaled0 = ((factor2 + factor1) * hid0).astype(BF16)
    scaled1 = (factor2 * hid1).astype(BF16)
    front = (hidden0, weighted2, scaled0, weighted0, weighted1, scaled1)
    back = (hidden1, weighted2, scaled1, weighted1, hidden0, hidden0)
    for slot, (a, b) in enumerate(zip(front, back)):
        mine_ref[slot * half : (slot + 1) * half, :] = jnp.where(first, a, b)
        theirs_ref[slot * half : (slot + 1) * half, :] = jnp.where(first, b, a)


def products(made):
    half = made.shape[0] // 6
    first = lax.axis_index("section") == 0
    hidden, last, scaled, weighted, extra1, extra2 = (made[i * half : (i + 1) * half] for i in range(6))
    hidden_t, scaled_t, weighted_t = (transposed(v) for v in (hidden, -scaled, weighted))
    mixes = (
        dot(hidden_t, last),
        dot(scaled_t, hidden),
        dot(jnp.where(first, -hidden_t, scaled_t), extra2),
        dot(jnp.where(first, hidden_t, weighted_t), extra1),
    )
    return mixes, weighted_t, scaled_t


def mine_kernel(near, made_ref, x_ref, mix_ref, acc_ref, left_ref):
    rank = made_ref.shape[1]
    half = made_ref.shape[0] // 6
    x = x_ref[rows_of(lax.axis_index("section") * half, half), :]
    mixes, weighted_t, scaled_t = products(made_ref[...])
    for i, mix in enumerate(mixes):
        mix_ref[i * rank : (i + 1) * rank, :] = mix
    left_ref[:rank, :] = weighted_t
    left_ref[rank:, :] = scaled_t
    acc_ref[:rank, :] = dot(weighted_t, x)
    slim = (acc_ref.shape[0] - rank) // len(near)
    place = lax.axis_index("dp")
    for i, step in enumerate(near):
        rows = left_ref[rows_of(rank + partner(place, step, rank // slim) * slim, slim), :]
        acc_ref[rank + i * slim : rank + (i + 1) * slim, :] = dot(rows, x)


def grad_kernel(
    replicas, near, made_ref, mix_ref, acc_ref, left_ref, stack_ref, down_t_ref, gain_ref, valid_ref, *refs
):
    out_refs, (all_ref, tall_ref, wide_ref) = refs[:replicas], refs[replicas:]
    rank, features = down_t_ref.shape
    slim = rank // replicas
    section = lax.axis_index("section")
    first = section == 0
    mixes, weighted_t, scaled_t = products(made_ref[...])
    mixes = [(m + mix_ref[i * rank : (i + 1) * rank, :]).astype(BF16) for i, m in enumerate(mixes)]
    for i, mix in enumerate(mixes):
        tall_ref[i * rank : (i + 1) * rank, :] = mix
    tall_ref[rows_of((4 + section) * rank, rank), :] = left_ref[:rank, :]
    tall_ref[rows_of((5 - section) * rank, rank), :] = weighted_t
    tall_ref[rows_of((6 + section) * rank, rank), :] = left_ref[rank:, :]
    tall_ref[rows_of((7 - section) * rank, rank), :] = scaled_t
    head_mix, own_mix, oth_mix, mix = mixes
    none = jnp.zeros_like(mix)
    left = jnp.concatenate([jnp.where(first, none, mix), weighted_t], axis=1)
    grad = acc_ref[:rank, :] + dot(left, stack_ref[3 * rank :, :])
    gain = jnp.sum(grad * down_t_ref[...].astype(F32), axis=0, keepdims=True)
    grad = (grad * gain_ref[...].astype(F32)).astype(BF16)
    all_ref[...] = grad
    for i, value in enumerate((head_mix, own_mix, oth_mix, jnp.where(first, mix, none), scaled_t)):
        wide_ref[:, i * rank : (i + 1) * rank] = value
    place = lax.axis_index("dp")
    targets = [partner(place, step, replicas) for step in range(replicas)]
    left = jnp.concatenate([wide_ref[rows_of(t * slim, slim), :] for t in (targets[i] for i in near)], axis=0)
    rest = (acc_ref[rank:, :] + dot(left, stack_ref[...])).astype(BF16)
    count = jnp.sum(valid_ref[...].astype(F32), keepdims=True)
    lines = features // rank
    tail = jnp.concatenate(
        [gain[:, i * rank : (i + 1) * rank] for i in range(lines)] + [jnp.broadcast_to(count, (PACK - lines, rank))],
        axis=0,
    ).astype(BF16)
    for step, out_ref in enumerate(out_refs):
        if step in near:
            at = near.index(step) * slim
            block = all_ref[rows_of(targets[step] * slim, slim), :]
            for i in range(lines):
                lanes = slice(i * rank, (i + 1) * rank)
                out_ref[i * 2 * slim : (2 * i + 1) * slim, :] = block[:, lanes]
                out_ref[(2 * i + 1) * slim : (i + 1) * 2 * slim, :] = rest[at : at + slim, lanes]
        else:
            for i in range(8):
                out_ref[i * slim : (i + 1) * slim, :] = tall_ref[rows_of(i * rank + targets[step] * slim, slim), :]
        out_ref[-PACK:, :] = tail


def last_kernel(count, *refs):
    near, refs = refs[:count], refs[count:]
    far_ref, sent_ref, cross_ref, stack_ref, gain_ref, down_out, up_out, gain_out = refs
    rank = far_ref.shape[1]
    slim, features = down_out.shape
    lines = features // rank
    first = lax.axis_index("section") == 0

    def total(start, size):
        return sum(p[start : start + size, :].astype(F32) for p in near)

    def left(i):
        return jnp.concatenate([far_ref[j * slim : (j + 1) * slim, :] for j in (4 + i, 6 + i)], axis=0)

    tail = sum(p[-PACK:, :].astype(F32) for p in (*near, far_ref))
    scale = 1.0 / tail[lines : lines + 1, :1]
    one, two = left(0), left(1)
    moved = dot(jnp.where(first, one, two), sent_ref[...]) + dot(jnp.where(first, two, one), cross_ref[...])
    mixes = [far_ref[i * slim : (i + 1) * slim, :] for i in range(4)]
    none = jnp.zeros_like(mixes[3])
    down = moved[:slim] + dot(jnp.where(first, none, mixes[3]), stack_ref[3 * rank : 4 * rank, :])
    down = down * gain_ref[...].astype(F32)
    mixes = jnp.concatenate(mixes[:3] + [jnp.where(first, mixes[3], none)], axis=1)
    up = moved[slim:] + dot(mixes, stack_ref[: 4 * rank, :])
    for i in range(lines):
        lanes = slice(i * rank, (i + 1) * rank)
        down_out[:, lanes] = (total(i * 2 * slim, slim) + down[:, lanes]) * scale
        up_out[:, lanes] = (total((2 * i + 1) * slim, slim) + up[:, lanes]) * scale
        gain_out[:, lanes] = tail[i : i + 1, :] * scale


def local(inputs, adapter_down, adapter_up, gains, head, labels, valid):
    sections, tensors, replicas = (lax.axis_size(a) for a in ("section", "tensor", "dp"))
    features = inputs.shape[2]
    width = features * tensors
    rank = adapter_down.shape[2]
    states = inputs.reshape(-1, features)
    half = states.shape[0] // sections
    assert sections == 2 and half == rank and head.shape[1] == rank and features % rank == 0
    slim = rank // replicas
    lines = features // rank
    down, up = adapter_down[0], adapter_up[0]
    labels, valid = labels.reshape(sections, half), valid.reshape(sections, half)
    shape = jax.ShapeDtypeStruct

    others = []
    for value in (down, up, gains):
        others.append(from_partner(value, "section", 1))
    down2, up2, gains2 = others
    assert replicas > 1
    far = replicas // 2
    near = [step for step in range(replicas) if step != far]
    small = 2 * rank * rank * features
    opened = call(open_kernel, shape((8, rank), F32), 40 * small)
    own, mine = call(
        own_kernel,
        [shape((3 * half + 2 * rank + PACK, rank), BF16), shape((half, features), BF16)],
        5 * small,
        states, down, up, head, gains, opened,
    )
    sent = from_partner(mine, "dp", far)
    first_part, second_part = call(
        other_kernel,
        [shape((3 * rank + half + PACK, rank), BF16), shape((4 * half, rank), BF16)],
        3 * small,
        states, up, own, down2, up2, gains2,
    )
    doubling = [1 << i for i in range(tensors.bit_length() - 1)]

    def terms(value, steps):
        if tensors & (tensors - 1):
            return [value] + [from_partner(value, "tensor", step) for step in range(1, tensors)]
        for hop, step in enumerate(steps):
            got = from_partner(value, "tensor", step)
            if hop + 1 == len(steps):
                return [value, got]
            value = call(add_kernel, shape(value.shape, BF16), small // 8, value, got)

    first_part = terms(first_part, doubling)
    second_part = terms(second_part, doubling[::-1])
    gram = call(add_kernel, shape((3 * rank, rank), BF16), small // 8, *first_part)
    down_t, stack = call(
        prepare_kernel,
        [shape((rank, features), BF16), shape((4 * rank + half, features), BF16)],
        small,
        down, head, up, down2, up2, gains2, states,
    )
    gram2 = from_partner(gram, "section", 1)
    made, theirs = call(
        functools.partial(chain_kernel, width, len(first_part)),
        [shape((6 * half, rank), BF16)] * 2,
        16 * 2 * half * rank * rank,
        *first_part, *second_part, gram, gram2, labels, valid,
    )
    met = from_partner(theirs, "section", 1)
    mixes, acc, left = call(
        functools.partial(mine_kernel, near),
        [shape((4 * rank, rank), F32), shape((rank + len(near) * slim, features), F32), shape((2 * rank, half), BF16)],
        4 * small,
        made, states,
    )
    *parts, _, _, _ = call(
        functools.partial(grad_kernel, replicas, near),
        [shape(((lines * 2 if i in near else 8) * slim + PACK, rank), BF16) for i in range(replicas)]
        + [shape((rank, features), BF16), shape((8 * rank, rank), BF16), shape((rank, 5 * rank), BF16)],
        16 * small,
        met, mixes, acc, left, stack, down_t, gains, valid,
    )
    for step in range(1, replicas):
        parts[step] = from_partner(parts[step], "dp", step)
    cross = from_partner(sent, "section", 1)
    down_grad, up_grad, gain_grad = call(
        functools.partial(last_kernel, len(near)),
        [shape((slim, features), F32), shape((slim, features), F32), shape((1, features), F32)],
        2 * small,
        *(parts[i] for i in near), parts[far], sent, cross, stack, gains,
    )
    return down_grad.T[None], up_grad[None], gain_grad


def solution(mesh):
    return jax.shard_map(
        local,
        mesh=mesh,
        in_specs=(
            P(None, "dp", "tensor"),
            P("section", "tensor", None),
            P("section", None, "tensor"),
            P("section", "tensor"),
            P("tensor", None),
            P(None, "dp"),
            P(None, "dp"),
        ),
        out_specs=(
            P("section", "tensor", "dp"),
            P("section", "dp", "tensor"),
            P("section", "tensor"),
        ),
        check_vma=False,
    )
```

```python
import functools

import jax
import jax.numpy as jnp
from jax import lax
from jax.experimental import pallas as pl
from jax.experimental.pallas import tpu as pltpu
from jax.sharding import PartitionSpec as P


epsilon = 1e-05
F32 = jnp.float32
BF16 = jnp.bfloat16
PACK = 16


def dot(a, b):
    return jnp.dot(a, b, preferred_element_type=F32)


def dot_nt(a, b):
    return lax.dot_general(a, b, (((1,), (1,)), ((), ())), preferred_element_type=F32)


def rows_of(start, count):
    return pl.ds(pl.multiple_of(start, count), count)


def transposed(value):
    return value.astype(F32).T.astype(value.dtype)


def partner(index, step, size):
    if size & (size - 1) == 0:
        return index ^ step
    return (index + step) % size


def from_partner(value, axis, step):
    size = lax.axis_size(axis)
    return lax.ppermute(value, axis, [(i, partner(i, step, size)) for i in range(size)])


def high_low(value):
    high = value.astype(BF16).astype(F32)
    return jnp.concatenate([high, value - high], axis=0).astype(BF16)


def call(kernel, out, flops, *args):
    moved = sum(a.size * a.dtype.itemsize for a in args)
    return pl.pallas_call(
        kernel,
        out_shape=out,
        cost_estimate=pl.CostEstimate(flops=flops, bytes_accessed=moved, transcendentals=0),
        compiler_params=pltpu.CompilerParams(vmem_limit_bytes=24 * 2**20),
    )(*args)


def open_kernel(out_ref):
    out_ref[...] = jnp.zeros_like(out_ref)


def own_kernel(x_ref, down_ref, up_ref, head_ref, gain_ref, _, out_ref, half_ref):
    rank = down_ref.shape[1]
    half = x_ref.shape[0] // lax.axis_size("section")
    x, up, head = x_ref[rows_of(lax.axis_index("section") * half, half), :], up_ref[...], head_ref[...]
    half_ref[...] = x
    x32 = x.astype(F32)
    scaled = (x32 * gain_ref[...].astype(F32)).astype(BF16)
    out_ref[:half, :] = dot(scaled, down_ref[...]).astype(BF16)
    out_ref[half : 2 * half, :] = dot_nt(x, up).astype(BF16)
    out_ref[2 * half : 3 * half, :] = dot(x, head).astype(BF16)
    out_ref[3 * half : 3 * half + rank, :] = dot(up, head).astype(BF16)
    out_ref[3 * half + rank : 3 * half + 2 * rank, :] = dot_nt(up, up).astype(BF16)
    squares = jnp.sum(x32 * x32, axis=1, keepdims=True)
    squares = jnp.broadcast_to(squares, (half, rank)).T
    out_ref[3 * half + 2 * rank :, :] = high_low(squares[: PACK // 2])


def other_kernel(x_ref, up_ref, own_ref, down2_ref, up2_ref, gain2_ref, a_ref, b_ref):
    rank = down2_ref.shape[1]
    half = x_ref.shape[0] // lax.axis_size("section")
    me = lax.axis_index("section")
    it = 1 - me
    x = x_ref[rows_of(me * half, half), :]
    gain2 = gain2_ref[...].astype(F32)
    b_ref[rows_of(me * half, half), :] = own_ref[:half, :]
    b_ref[rows_of((2 + me) * half, half), :] = own_ref[half : 2 * half, :]
    a_ref[rank : 3 * rank, :] = own_ref[3 * half : 3 * half + 2 * rank, :]
    a_ref[3 * rank : 3 * rank + half, :] = own_ref[2 * half : 3 * half, :]
    a_ref[3 * rank + half :, :] = own_ref[3 * half + 2 * rank :, :]
    scaled = (x.astype(F32) * gain2).astype(BF16)
    b_ref[rows_of(it * half, half), :] = dot(scaled, down2_ref[...]).astype(BF16)
    b_ref[rows_of((2 + it) * half, half), :] = dot_nt(x, up2_ref[...]).astype(BF16)

    @pl.when(me == 0)
    def _():
        scaled = (up_ref[...].astype(F32) * gain2).astype(BF16)
        a_ref[:rank, :] = dot(scaled, down2_ref[...]).astype(BF16)

    @pl.when(me != 0)
    def _():
        a_ref[:rank, :] = dot_nt(up_ref[...], up2_ref[...]).astype(BF16)


def add_kernel(*refs):
    rows = refs[-1].shape[0]
    refs[-1][...] = sum(r[:rows, :].astype(F32) for r in refs[:-1]).astype(BF16)


def prepare_kernel(down_ref, head_ref, up_ref, down2_ref, up2_ref, gain2_ref, x_ref, down_t_ref, stack_ref):
    rank = up_ref.shape[0]
    half = x_ref.shape[0] // lax.axis_size("section")
    down_t_ref[...] = transposed(down_ref[...])
    stack_ref[:rank, :] = transposed(head_ref[...])
    stack_ref[rank : 2 * rank, :] = up_ref[...]
    stack_ref[2 * rank : 3 * rank, :] = up2_ref[...]
    me = lax.axis_index("section")

    @pl.when(me == 0)
    def _():
        stack_ref[3 * rank : 4 * rank, :] = (down2_ref[...].astype(F32).T * gain2_ref[...].astype(F32)).astype(BF16)

    @pl.when(me != 0)
    def _():
        stack_ref[3 * rank : 4 * rank, :] = up2_ref[...]

    stack_ref[4 * rank :, :] = x_ref[rows_of((1 - me) * half, half), :]


def chain_kernel(width, count, *refs):
    a_refs, b_refs = refs[:count], refs[count : 2 * count]
    gram_ref, gram2_ref, label_ref, valid_ref, mine_ref, theirs_ref = refs[2 * count :]
    rank = gram_ref.shape[1]
    half = label_ref.shape[1]
    me = lax.axis_index("section")
    first = me == 0

    def total(parts, start, size):
        return sum(r[start : start + size, :].astype(F32) for r in parts)

    def spread(row):
        return jnp.broadcast_to(row, (rank, half)).T

    gram, gram2 = gram_ref[...], gram2_ref[...]
    gram0, gram1 = jnp.where(first, gram, gram2), jnp.where(first, gram2, gram)
    m01, b0h, b0b0 = (gram0[i * rank : (i + 1) * rank] for i in range(3))
    b1b0, b1h, b1b1 = (gram1[i * rank : (i + 1) * rank] for i in range(3))
    tail = total(a_refs, 3 * rank + half, PACK)
    squares0 = spread(tail[:1] + tail[PACK // 2 : PACK // 2 + 1])
    inv0 = lax.rsqrt(squares0 / width + epsilon)
    proj0 = total(b_refs, 0, half)
    pre0 = inv0 * proj0
    sig0 = jax.nn.sigmoid(pre0)
    hidden0 = (pre0 * sig0).astype(BF16)
    hid0 = hidden0.astype(F32)
    proj1 = total(b_refs, half, half) + dot(hidden0, m01)
    cross0 = total(b_refs, 2 * half, half)
    one_b0 = cross0 + dot(hidden0, b0b0)
    squares1 = squares0 + jnp.sum(hid0 * (cross0 + one_b0), axis=1, keepdims=True)
    inv1 = lax.rsqrt(squares1 / width + epsilon)
    pre1 = inv1 * proj1
    sig1 = jax.nn.sigmoid(pre1)
    hidden1 = (pre1 * sig1).astype(BF16)
    hid1 = hidden1.astype(F32)
    one_b1 = total(b_refs, 3 * half, half) + dot_nt(hidden0, b1b0)
    two_b0 = one_b0 + dot(hidden1, b1b0)
    two_b1 = one_b1 + dot(hidden1, b1b1)
    squares2 = squares1 + jnp.sum(hid1 * (one_b1 + two_b1), axis=1, keepdims=True)
    inv2 = lax.rsqrt(squares2 / width + epsilon)
    base = total(a_refs, 3 * rank, half) + dot(hidden0, b0h) + dot(hidden1, b1h)
    logits = inv2 * base
    expo = jnp.exp(logits - jnp.max(logits, axis=1, keepdims=True))
    prob = expo / jnp.sum(expo, axis=1, keepdims=True)
    labels = spread(label_ref[pl.ds(me, 1), :].astype(F32))
    valid = spread(valid_ref[pl.ds(me, 1), :].astype(F32))
    classes = lax.broadcasted_iota(jnp.int32, logits.shape, 1).astype(F32)
    cot = (prob - (classes == labels).astype(F32)) * valid
    factor2 = inv2 * inv2 * inv2 / width * jnp.sum(cot * base, axis=1, keepdims=True)
    weighted2 = (inv2 * cot).astype(BF16)
    grad1 = dot_nt(weighted2, b1h) - factor2 * two_b1
    act1 = grad1 * sig1 * (1.0 + pre1 * (1.0 - sig1))
    factor1 = inv1 * inv1 * inv1 / width * jnp.sum(act1 * proj1, axis=1, keepdims=True)
    weighted1 = (inv1 * act1).astype(BF16)
    grad0 = dot_nt(weighted2, b0h) - factor2 * two_b0 + dot_nt(weighted1, m01) - factor1 * one_b0
    act0 = grad0 * sig0 * (1.0 + pre0 * (1.0 - sig0))
    weighted0 = (inv0 * act0).astype(BF16)
    scaled0 = ((factor2 + factor1) * hid0).astype(BF16)
    scaled1 = (factor2 * hid1).astype(BF16)
    front = (hidden0, weighted2, scaled0, weighted0, weighted1, scaled1)
    back = (hidden1, weighted2, scaled1, weighted1, hidden0, hidden0)
    for slot, (a, b) in enumerate(zip(front, back)):
        mine_ref[slot * half : (slot + 1) * half, :] = jnp.where(first, a, b)
        theirs_ref[slot * half : (slot + 1) * half, :] = jnp.where(first, b, a)


def products(made):
    half = made.shape[0] // 6
    first = lax.axis_index("section") == 0
    hidden, last, scaled, weighted, extra1, extra2 = (made[i * half : (i + 1) * half] for i in range(6))
    hidden_t, scaled_t, weighted_t = (transposed(v) for v in (hidden, -scaled, weighted))
    mixes = (
        dot(hidden_t, last),
        dot(scaled_t, hidden),
        dot(jnp.where(first, -hidden_t, scaled_t), extra2),
        dot(jnp.where(first, hidden_t, weighted_t), extra1),
    )
    return mixes, weighted_t, scaled_t


def mine_kernel(near, made_ref, x_ref, mix_ref, acc_ref, left_ref):
    rank = made_ref.shape[1]
    half = made_ref.shape[0] // 6
    x = x_ref[rows_of(lax.axis_index("section") * half, half), :]
    mixes, weighted_t, scaled_t = products(made_ref[...])
    for i, mix in enumerate(mixes):
        mix_ref[i * rank : (i + 1) * rank, :] = mix
    left_ref[:rank, :] = weighted_t
    left_ref[rank:, :] = scaled_t
    acc_ref[:rank, :] = dot(weighted_t, x)
    slim = (acc_ref.shape[0] - rank) // len(near)
    place = lax.axis_index("dp")
    for i, step in enumerate(near):
        rows = left_ref[rows_of(rank + partner(place, step, rank // slim) * slim, slim), :]
        acc_ref[rank + i * slim : rank + (i + 1) * slim, :] = dot(rows, x)


def down_kernel(
    replicas, far, made_ref, mix_ref, acc_ref, left_ref, stack_ref, down_t_ref, gain_ref, valid_ref,
    far_ref, grad_ref, wide_ref, tail_ref, tall_ref
):
    rank, features = down_t_ref.shape
    slim = rank // replicas
    lines = features // rank
    section = lax.axis_index("section")
    first = section == 0
    mixes, weighted_t, scaled_t = products(made_ref[...])
    mixes = [(m + mix_ref[i * rank : (i + 1) * rank, :]).astype(BF16) for i, m in enumerate(mixes)]
    for i, mix in enumerate(mixes):
        tall_ref[i * rank : (i + 1) * rank, :] = mix
    tall_ref[rows_of((4 + section) * rank, rank), :] = left_ref[:rank, :]
    tall_ref[rows_of((5 - section) * rank, rank), :] = weighted_t
    tall_ref[rows_of((6 + section) * rank, rank), :] = left_ref[rank:, :]
    tall_ref[rows_of((7 - section) * rank, rank), :] = scaled_t
    none = jnp.zeros_like(mixes[3])
    left = jnp.concatenate([jnp.where(first, none, mixes[3]), weighted_t], axis=1)
    grad = acc_ref[:rank, :] + dot(left, stack_ref[3 * rank :, :])
    gain = jnp.sum(grad * down_t_ref[...].astype(F32), axis=0, keepdims=True)
    grad_ref[...] = (grad * gain_ref[...].astype(F32)).astype(BF16)
    for i, value in enumerate((*mixes[:3], jnp.where(first, mixes[3], none), scaled_t)):
        wide_ref[:, i * rank : (i + 1) * rank] = value
    count = jnp.sum(valid_ref[...].astype(F32), keepdims=True)
    tail = jnp.concatenate(
        [gain[:, i * rank : (i + 1) * rank] for i in range(lines)] + [jnp.broadcast_to(count, (PACK - lines, rank))],
        axis=0,
    ).astype(BF16)
    tail_ref[...] = tail
    target = partner(lax.axis_index("dp"), far, replicas)
    for i in range(8):
        far_ref[i * slim : (i + 1) * slim, :] = tall_ref[rows_of(i * rank + target * slim, slim), :]
    far_ref[-PACK:, :] = tail


def up_kernel(replicas, near, acc_ref, grad_ref, wide_ref, tail_ref, stack_ref, *out_refs):
    rank, features = grad_ref.shape
    slim = rank // replicas
    place = lax.axis_index("dp")
    targets = [partner(place, step, replicas) for step in near]
    left = jnp.concatenate([wide_ref[rows_of(t * slim, slim), :] for t in targets], axis=0)
    rest = (acc_ref[rank:, :] + dot(left, stack_ref[...])).astype(BF16)
    for at, (target, out_ref) in enumerate(zip(targets, out_refs)):
        block = grad_ref[rows_of(target * slim, slim), :]
        for i in range(features // rank):
            lanes = slice(i * rank, (i + 1) * rank)
            out_ref[i * 2 * slim : (2 * i + 1) * slim, :] = block[:, lanes]
            out_ref[(2 * i + 1) * slim : (i + 1) * 2 * slim, :] = rest[at * slim : (at + 1) * slim, lanes]
        out_ref[-PACK:, :] = tail_ref[...]


def far_kernel(far_ref, sent_ref, cross_ref, stack_ref, gain_ref, out_ref):
    rank = far_ref.shape[1]
    slim = out_ref.shape[0] // 2
    first = lax.axis_index("section") == 0
    one, two = (
        jnp.concatenate([far_ref[j * slim : (j + 1) * slim, :] for j in (4 + i, 6 + i)], axis=0) for i in range(2)
    )
    moved = dot(jnp.where(first, one, two), sent_ref[...]) + dot(jnp.where(first, two, one), cross_ref[...])
    mixes = [far_ref[i * slim : (i + 1) * slim, :] for i in range(4)]
    none = jnp.zeros_like(mixes[3])
    down = moved[:slim] + dot(jnp.where(first, none, mixes[3]), stack_ref[3 * rank : 4 * rank, :])
    out_ref[:slim, :] = down * gain_ref[...].astype(F32)
    mixes = jnp.concatenate(mixes[:3] + [jnp.where(first, mixes[3], none)], axis=1)
    out_ref[slim:, :] = moved[slim:] + dot(mixes, stack_ref[: 4 * rank, :])


def last_kernel(*refs):
    near, (far_ref, moved_ref, down_out, up_out, gain_out) = refs[:-5], refs[-5:]
    rank = far_ref.shape[1]
    slim, features = down_out.shape
    lines = features // rank

    def total(start, size):
        return sum(p[start : start + size, :].astype(F32) for p in near)

    tail = sum(p[-PACK:, :].astype(F32) for p in (*near, far_ref))
    scale = 1.0 / tail[lines : lines + 1, :1]
    for i in range(lines):
        lanes = slice(i * rank, (i + 1) * rank)
        down_out[:, lanes] = (total(i * 2 * slim, slim) + moved_ref[:slim, lanes]) * scale
        up_out[:, lanes] = (total((2 * i + 1) * slim, slim) + moved_ref[slim:, lanes]) * scale
        gain_out[:, lanes] = tail[i : i + 1, :] * scale


def local(inputs, adapter_down, adapter_up, gains, head, labels, valid):
    sections, tensors, replicas = (lax.axis_size(a) for a in ("section", "tensor", "dp"))
    features = inputs.shape[2]
    width = features * tensors
    rank = adapter_down.shape[2]
    states = inputs.reshape(-1, features)
    half = states.shape[0] // sections
    assert sections == 2 and half == rank and head.shape[1] == rank and features % rank == 0
    slim = rank // replicas
    lines = features // rank
    down, up = adapter_down[0], adapter_up[0]
    labels, valid = labels.reshape(sections, half), valid.reshape(sections, half)
    shape = jax.ShapeDtypeStruct

    others = []
    for value in (down, up, gains):
        others.append(from_partner(value, "section", 1))
    down2, up2, gains2 = others
    assert replicas > 1
    far = replicas // 2
    near = [step for step in range(replicas) if step != far]
    small = 2 * rank * rank * features
    opened = call(open_kernel, shape((8, rank), F32), 40 * small)
    own, mine = call(
        own_kernel,
        [shape((3 * half + 2 * rank + PACK, rank), BF16), shape((half, features), BF16)],
        5 * small,
        states, down, up, head, gains, opened,
    )
    sent = from_partner(mine, "dp", far)
    first_part, second_part = call(
        other_kernel,
        [shape((3 * rank + half + PACK, rank), BF16), shape((4 * half, rank), BF16)],
        3 * small,
        states, up, own, down2, up2, gains2,
    )
    doubling = [1 << i for i in range(tensors.bit_length() - 1)]

    def terms(value, steps):
        if tensors & (tensors - 1):
            return [value] + [from_partner(value, "tensor", step) for step in range(1, tensors)]
        for hop, step in enumerate(steps):
            got = from_partner(value, "tensor", step)
            if hop + 1 == len(steps):
                return [value, got]
            value = call(add_kernel, shape(value.shape, BF16), small // 8, value, got)

    first_part = terms(first_part, doubling)
    second_part = terms(second_part, doubling[::-1])
    gram = call(add_kernel, shape((3 * rank, rank), BF16), small // 8, *first_part)
    down_t, stack = call(
        prepare_kernel,
        [shape((rank, features), BF16), shape((4 * rank + half, features), BF16)],
        small,
        down, head, up, down2, up2, gains2, states,
    )
    gram2 = from_partner(gram, "section", 1)
    made, theirs = call(
        functools.partial(chain_kernel, width, len(first_part)),
        [shape((6 * half, rank), BF16)] * 2,
        16 * 2 * half * rank * rank,
        *first_part, *second_part, gram, gram2, labels, valid,
    )
    met = from_partner(theirs, "section", 1)
    mixes, acc, left = call(
        functools.partial(mine_kernel, near),
        [shape((4 * rank, rank), F32), shape((rank + len(near) * slim, features), F32), shape((2 * rank, half), BF16)],
        4 * small,
        made, states,
    )
    away, grad, wide, tail, _ = call(
        functools.partial(down_kernel, replicas, far),
        [
            shape((8 * slim + PACK, rank), BF16),
            shape((rank, features), BF16),
            shape((rank, 5 * rank), BF16),
            shape((PACK, rank), BF16),
            shape((8 * rank, rank), BF16),
        ],
        8 * small,
        met, mixes, acc, left, stack, down_t, gains, valid,
    )
    away = from_partner(away, "dp", far)
    *parts, = call(
        functools.partial(up_kernel, replicas, near),
        [shape((lines * 2 * slim + PACK, rank), BF16)] * len(near),
        8 * small,
        acc, grad, wide, tail, stack,
    )
    for i, step in enumerate(near):
        if step > 0:
            parts[i] = from_partner(parts[i], "dp", step)
    cross = from_partner(sent, "section", 1)
    moved = call(
        far_kernel, shape((2 * slim, features), F32), 2 * small, away, sent, cross, stack, gains
    )
    down_grad, up_grad, gain_grad = call(
        last_kernel,
        [shape((slim, features), F32), shape((slim, features), F32), shape((1, features), F32)],
        small,
        *parts, away, moved,
    )
    return down_grad.T[None], up_grad[None], gain_grad


def solution(mesh):
    return jax.shard_map(
        local,
        mesh=mesh,
        in_specs=(
            P(None, "dp", "tensor"),
            P("section", "tensor", None),
            P("section", None, "tensor"),
            P("section", "tensor"),
            P("tensor", None),
            P(None, "dp"),
            P(None, "dp"),
        ),
        out_specs=(
            P("section", "tensor", "dp"),
            P("section", "dp", "tensor"),
            P("section", "tensor"),
        ),
        check_vma=False,
    )
```

```python
import functools

import jax
import jax.numpy as jnp
from jax import lax
from jax.experimental import pallas as pl
from jax.experimental.pallas import tpu as pltpu
from jax.sharding import PartitionSpec as P


epsilon = 1e-05
F32 = jnp.float32
BF16 = jnp.bfloat16
PACK = 16


def dot(a, b):
    return jnp.dot(a, b, preferred_element_type=F32)


def dot_nt(a, b):
    return lax.dot_general(a, b, (((1,), (1,)), ((), ())), preferred_element_type=F32)


def rows_of(start, count):
    return pl.ds(pl.multiple_of(start, count), count)


def transposed(value):
    return value.astype(F32).T.astype(value.dtype)


def partner(index, step, size):
    if size & (size - 1) == 0:
        return index ^ step
    return (index + step) % size


def from_partner(value, axis, step):
    size = lax.axis_size(axis)
    return lax.ppermute(value, axis, [(i, partner(i, step, size)) for i in range(size)])


def high_low(value):
    high = value.astype(BF16).astype(F32)
    return jnp.concatenate([high, value - high], axis=0).astype(BF16)


def call(kernel, out, flops, *args):
    moved = sum(a.size * a.dtype.itemsize for a in args)
    return pl.pallas_call(
        kernel,
        out_shape=out,
        cost_estimate=pl.CostEstimate(flops=flops, bytes_accessed=moved, transcendentals=0),
        compiler_params=pltpu.CompilerParams(vmem_limit_bytes=24 * 2**20),
    )(*args)


def open_kernel(out_ref):
    out_ref[...] = jnp.zeros_like(out_ref)


def own_kernel(x_ref, down_ref, up_ref, head_ref, gain_ref, _, out_ref, half_ref):
    rank = down_ref.shape[1]
    half = x_ref.shape[0] // lax.axis_size("section")
    x, up, head = x_ref[rows_of(lax.axis_index("section") * half, half), :], up_ref[...], head_ref[...]
    half_ref[...] = x
    x32 = x.astype(F32)
    scaled = (x32 * gain_ref[...].astype(F32)).astype(BF16)
    out_ref[:half, :] = dot(scaled, down_ref[...]).astype(BF16)
    out_ref[half : 2 * half, :] = dot_nt(x, up).astype(BF16)
    out_ref[2 * half : 3 * half, :] = dot(x, head).astype(BF16)
    out_ref[3 * half : 3 * half + rank, :] = dot(up, head).astype(BF16)
    out_ref[3 * half + rank : 3 * half + 2 * rank, :] = dot_nt(up, up).astype(BF16)
    squares = jnp.sum(x32 * x32, axis=1, keepdims=True)
    squares = jnp.broadcast_to(squares, (half, rank)).T
    out_ref[3 * half + 2 * rank :, :] = high_low(squares[: PACK // 2])


def other_kernel(x_ref, up_ref, own_ref, down2_ref, up2_ref, gain2_ref, a_ref, b_ref):
    rank = down2_ref.shape[1]
    half = x_ref.shape[0] // lax.axis_size("section")
    me = lax.axis_index("section")
    it = 1 - me
    x = x_ref[rows_of(me * half, half), :]
    gain2 = gain2_ref[...].astype(F32)
    b_ref[rows_of(me * half, half), :] = own_ref[:half, :]
    b_ref[rows_of((2 + me) * half, half), :] = own_ref[half : 2 * half, :]
    a_ref[rank : 3 * rank, :] = own_ref[3 * half : 3 * half + 2 * rank, :]
    a_ref[3 * rank : 3 * rank + half, :] = own_ref[2 * half : 3 * half, :]
    a_ref[3 * rank + half :, :] = own_ref[3 * half + 2 * rank :, :]
    scaled = (x.astype(F32) * gain2).astype(BF16)
    b_ref[rows_of(it * half, half), :] = dot(scaled, down2_ref[...]).astype(BF16)
    b_ref[rows_of((2 + it) * half, half), :] = dot_nt(x, up2_ref[...]).astype(BF16)

    @pl.when(me == 0)
    def _():
        scaled = (up_ref[...].astype(F32) * gain2).astype(BF16)
        a_ref[:rank, :] = dot(scaled, down2_ref[...]).astype(BF16)

    @pl.when(me != 0)
    def _():
        a_ref[:rank, :] = dot_nt(up_ref[...], up2_ref[...]).astype(BF16)


def add_kernel(*refs):
    rows = refs[-1].shape[0]
    refs[-1][...] = sum(r[:rows, :].astype(F32) for r in refs[:-1]).astype(BF16)


def prepare_kernel(down_ref, head_ref, up_ref, down2_ref, up2_ref, gain2_ref, x_ref, down_t_ref, stack_ref):
    rank = up_ref.shape[0]
    half = x_ref.shape[0] // lax.axis_size("section")
    down_t_ref[...] = transposed(down_ref[...])
    stack_ref[:rank, :] = transposed(head_ref[...])
    stack_ref[rank : 2 * rank, :] = up_ref[...]
    stack_ref[2 * rank : 3 * rank, :] = up2_ref[...]
    me = lax.axis_index("section")

    @pl.when(me == 0)
    def _():
        stack_ref[3 * rank : 4 * rank, :] = (down2_ref[...].astype(F32).T * gain2_ref[...].astype(F32)).astype(BF16)

    @pl.when(me != 0)
    def _():
        stack_ref[3 * rank : 4 * rank, :] = up2_ref[...]

    stack_ref[4 * rank :, :] = x_ref[rows_of((1 - me) * half, half), :]


def chain_kernel(width, count, *refs):
    a_refs, b_refs = refs[:count], refs[count : 2 * count]
    gram_ref, gram2_ref, label_ref, valid_ref, mine_ref, theirs_ref = refs[2 * count :]
    rank = gram_ref.shape[1]
    half = label_ref.shape[1]
    me = lax.axis_index("section")
    first = me == 0

    def total(parts, start, size):
        return sum(r[start : start + size, :].astype(F32) for r in parts)

    def spread(row):
        return jnp.broadcast_to(row, (rank, half)).T

    gram, gram2 = gram_ref[...], gram2_ref[...]
    gram0, gram1 = jnp.where(first, gram, gram2), jnp.where(first, gram2, gram)
    m01, b0h, b0b0 = (gram0[i * rank : (i + 1) * rank] for i in range(3))
    b1b0, b1h, b1b1 = (gram1[i * rank : (i + 1) * rank] for i in range(3))
    tail = total(a_refs, 3 * rank + half, PACK)
    squares0 = spread(tail[:1] + tail[PACK // 2 : PACK // 2 + 1])
    inv0 = lax.rsqrt(squares0 / width + epsilon)
    proj0 = total(b_refs, 0, half)
    pre0 = inv0 * proj0
    sig0 = jax.nn.sigmoid(pre0)
    hidden0 = (pre0 * sig0).astype(BF16)
    hid0 = hidden0.astype(F32)
    proj1 = total(b_refs, half, half) + dot(hidden0, m01)
    cross0 = total(b_refs, 2 * half, half)
    one_b0 = cross0 + dot(hidden0, b0b0)
    squares1 = squares0 + jnp.sum(hid0 * (cross0 + one_b0), axis=1, keepdims=True)
    squares1 = jnp.maximum(squares1, 0.0)
    inv1 = lax.rsqrt(squares1 / width + epsilon)
    pre1 = inv1 * proj1
    sig1 = jax.nn.sigmoid(pre1)
    hidden1 = (pre1 * sig1).astype(BF16)
    hid1 = hidden1.astype(F32)
    one_b1 = total(b_refs, 3 * half, half) + dot_nt(hidden0, b1b0)
    two_b0 = one_b0 + dot(hidden1, b1b0)
    two_b1 = one_b1 + dot(hidden1, b1b1)
    squares2 = squares1 + jnp.sum(hid1 * (one_b1 + two_b1), axis=1, keepdims=True)
    squares2 = jnp.maximum(squares2, 0.0)
    inv2 = lax.rsqrt(squares2 / width + epsilon)
    base = total(a_refs, 3 * rank, half) + dot(hidden0, b0h) + dot(hidden1, b1h)
    logits = inv2 * base
    expo = jnp.exp(logits - jnp.max(logits, axis=1, keepdims=True))
    prob = expo / jnp.sum(expo, axis=1, keepdims=True)
    labels = spread(label_ref[pl.ds(me, 1), :].astype(F32))
    valid = spread(valid_ref[pl.ds(me, 1), :].astype(F32))
    classes = lax.broadcasted_iota(jnp.int32, logits.shape, 1).astype(F32)
    cot = (prob - (classes == labels).astype(F32)) * valid
    factor2 = inv2 * inv2 * inv2 / width * jnp.sum(cot * base, axis=1, keepdims=True)
    weighted2 = (inv2 * cot).astype(BF16)
    grad1 = dot_nt(weighted2, b1h) - factor2 * two_b1
    act1 = grad1 * sig1 * (1.0 + pre1 * (1.0 - sig1))
    factor1 = inv1 * inv1 * inv1 / width * jnp.sum(act1 * proj1, axis=1, keepdims=True)
    weighted1 = (inv1 * act1).astype(BF16)
    grad0 = dot_nt(weighted2, b0h) - factor2 * two_b0 + dot_nt(weighted1, m01) - factor1 * one_b0
    act0 = grad0 * sig0 * (1.0 + pre0 * (1.0 - sig0))
    weighted0 = (inv0 * act0).astype(BF16)
    scaled0 = ((factor2 + factor1) * hid0).astype(BF16)
    scaled1 = (factor2 * hid1).astype(BF16)
    front = (hidden0, weighted2, scaled0, weighted0, weighted1, scaled1)
    back = (hidden1, weighted2, scaled1, weighted1, hidden0, hidden0)
    for slot, (a, b) in enumerate(zip(front, back)):
        mine_ref[slot * half : (slot + 1) * half, :] = jnp.where(first, a, b)
        theirs_ref[slot * half : (slot + 1) * half, :] = jnp.where(first, b, a)


def products(made):
    half = made.shape[0] // 6
    first = lax.axis_index("section") == 0
    hidden, last, scaled, weighted, extra1, extra2 = (made[i * half : (i + 1) * half] for i in range(6))
    hidden_t, scaled_t, weighted_t = (transposed(v) for v in (hidden, -scaled, weighted))
    mixes = (
        dot(hidden_t, last),
        dot(scaled_t, hidden),
        dot(jnp.where(first, -hidden_t, scaled_t), extra2),
        dot(jnp.where(first, hidden_t, weighted_t), extra1),
    )
    return mixes, weighted_t, scaled_t


def mine_kernel(near, made_ref, x_ref, mix_ref, acc_ref, left_ref):
    rank = made_ref.shape[1]
    half = made_ref.shape[0] // 6
    x = x_ref[rows_of(lax.axis_index("section") * half, half), :]
    mixes, weighted_t, scaled_t = products(made_ref[...])
    for i, mix in enumerate(mixes):
        mix_ref[i * rank : (i + 1) * rank, :] = mix
    left_ref[:rank, :] = weighted_t
    left_ref[rank:, :] = scaled_t
    acc_ref[:rank, :] = dot(weighted_t, x)
    slim = (acc_ref.shape[0] - rank) // len(near)
    place = lax.axis_index("dp")
    for i, step in enumerate(near):
        rows = left_ref[rows_of(rank + partner(place, step, rank // slim) * slim, slim), :]
        acc_ref[rank + i * slim : rank + (i + 1) * slim, :] = dot(rows, x)


def down_kernel(
    replicas, far, made_ref, mix_ref, acc_ref, left_ref, stack_ref, down_t_ref, gain_ref, valid_ref,
    far_ref, grad_ref, wide_ref, tail_ref, tall_ref
):
    rank, features = down_t_ref.shape
    slim = rank // replicas
    lines = features // rank
    section = lax.axis_index("section")
    first = section == 0
    mixes, weighted_t, scaled_t = products(made_ref[...])
    mixes = [(m + mix_ref[i * rank : (i + 1) * rank, :]).astype(BF16) for i, m in enumerate(mixes)]
    for i, mix in enumerate(mixes):
        tall_ref[i * rank : (i + 1) * rank, :] = mix
    tall_ref[rows_of((4 + section) * rank, rank), :] = left_ref[:rank, :]
    tall_ref[rows_of((5 - section) * rank, rank), :] = weighted_t
    tall_ref[rows_of((6 + section) * rank, rank), :] = left_ref[rank:, :]
    tall_ref[rows_of((7 - section) * rank, rank), :] = scaled_t
    none = jnp.zeros_like(mixes[3])
    left = jnp.concatenate([jnp.where(first, none, mixes[3]), weighted_t], axis=1)
    grad = acc_ref[:rank, :] + dot(left, stack_ref[3 * rank :, :])
    gain = jnp.sum(grad * down_t_ref[...].astype(F32), axis=0, keepdims=True)
    grad_ref[...] = (grad * gain_ref[...].astype(F32)).astype(BF16)
    for i, value in enumerate((*mixes[:3], jnp.where(first, mixes[3], none), scaled_t)):
        wide_ref[:, i * rank : (i + 1) * rank] = value
    count = jnp.broadcast_to(jnp.sum(valid_ref[...].astype(F32), keepdims=True), (PACK - lines, rank))
    high = count.astype(BF16).astype(F32)
    count = jnp.where(lax.broadcasted_iota(jnp.int32, count.shape, 0) == 0, high, count - high)
    tail = jnp.concatenate([gain[:, i * rank : (i + 1) * rank] for i in range(lines)] + [count], axis=0).astype(BF16)
    tail_ref[...] = tail
    target = partner(lax.axis_index("dp"), far, replicas)
    for i in range(8):
        far_ref[i * slim : (i + 1) * slim, :] = tall_ref[rows_of(i * rank + target * slim, slim), :]
    far_ref[-PACK:, :] = tail


def up_kernel(replicas, near, acc_ref, grad_ref, wide_ref, tail_ref, stack_ref, *out_refs):
    rank, features = grad_ref.shape
    slim = rank // replicas
    place = lax.axis_index("dp")
    targets = [partner(place, step, replicas) for step in near]
    left = jnp.concatenate([wide_ref[rows_of(t * slim, slim), :] for t in targets], axis=0)
    rest = (acc_ref[rank:, :] + dot(left, stack_ref[...])).astype(BF16)
    for at, (target, out_ref) in enumerate(zip(targets, out_refs)):
        block = grad_ref[rows_of(target * slim, slim), :]
        for i in range(features // rank):
            lanes = slice(i * rank, (i + 1) * rank)
            out_ref[i * 2 * slim : (2 * i + 1) * slim, :] = block[:, lanes]
            out_ref[(2 * i + 1) * slim : (i + 1) * 2 * slim, :] = rest[at * slim : (at + 1) * slim, lanes]
        out_ref[-PACK:, :] = tail_ref[...]


def far_kernel(far_ref, sent_ref, cross_ref, stack_ref, gain_ref, out_ref):
    rank = far_ref.shape[1]
    slim = out_ref.shape[0] // 2
    first = lax.axis_index("section") == 0
    one, two = (
        jnp.concatenate([far_ref[j * slim : (j + 1) * slim, :] for j in (4 + i, 6 + i)], axis=0) for i in range(2)
    )
    moved = dot(jnp.where(first, one, two), sent_ref[...]) + dot(jnp.where(first, two, one), cross_ref[...])
    mixes = [far_ref[i * slim : (i + 1) * slim, :] for i in range(4)]
    none = jnp.zeros_like(mixes[3])
    down = moved[:slim] + dot(jnp.where(first, none, mixes[3]), stack_ref[3 * rank : 4 * rank, :])
    out_ref[:slim, :] = down * gain_ref[...].astype(F32)
    mixes = jnp.concatenate(mixes[:3] + [jnp.where(first, mixes[3], none)], axis=1)
    out_ref[slim:, :] = moved[slim:] + dot(mixes, stack_ref[: 4 * rank, :])


def last_kernel(*refs):
    near, (far_ref, moved_ref, down_out, up_out, gain_out) = refs[:-5], refs[-5:]
    rank = far_ref.shape[1]
    slim, features = down_out.shape
    lines = features // rank

    def total(start, size):
        return sum(p[start : start + size, :].astype(F32) for p in near)

    tail = sum(p[-PACK:, :].astype(F32) for p in (*near, far_ref))
    scale = 1.0 / (tail[lines : lines + 1, :1] + tail[lines + 1 : lines + 2, :1])
    for i in range(lines):
        lanes = slice(i * rank, (i + 1) * rank)
        down_out[:, lanes] = (total(i * 2 * slim, slim) + moved_ref[:slim, lanes]) * scale
        up_out[:, lanes] = (total((2 * i + 1) * slim, slim) + moved_ref[slim:, lanes]) * scale
        gain_out[:, lanes] = tail[i : i + 1, :] * scale


def local(inputs, adapter_down, adapter_up, gains, head, labels, valid):
    sections, tensors, replicas = (lax.axis_size(a) for a in ("section", "tensor", "dp"))
    features = inputs.shape[2]
    width = features * tensors
    rank = adapter_down.shape[2]
    states = inputs.reshape(-1, features)
    half = states.shape[0] // sections
    assert sections == 2 and half == rank and head.shape[1] == rank
    assert features % rank == 0 and features // rank < PACK - 1
    slim = rank // replicas
    lines = features // rank
    down, up = adapter_down[0], adapter_up[0]
    labels, valid = labels.reshape(sections, half), valid.reshape(sections, half)
    shape = jax.ShapeDtypeStruct

    others = []
    for value in (down, up, gains):
        others.append(from_partner(value, "section", 1))
    down2, up2, gains2 = others
    assert replicas > 1
    far = replicas // 2
    near = [step for step in range(replicas) if step != far]
    small = 2 * rank * rank * features
    opened = call(open_kernel, shape((8, rank), F32), 40 * small)
    own, mine = call(
        own_kernel,
        [shape((3 * half + 2 * rank + PACK, rank), BF16), shape((half, features), BF16)],
        5 * small,
        states, down, up, head, gains, opened,
    )
    sent = from_partner(mine, "dp", far)
    first_part, second_part = call(
        other_kernel,
        [shape((3 * rank + half + PACK, rank), BF16), shape((4 * half, rank), BF16)],
        3 * small,
        states, up, own, down2, up2, gains2,
    )
    doubling = [1 << i for i in range(tensors.bit_length() - 1)]

    def terms(value, steps):
        if tensors & (tensors - 1):
            return [value] + [from_partner(value, "tensor", step) for step in range(1, tensors)]
        for hop, step in enumerate(steps):
            got = from_partner(value, "tensor", step)
            if hop + 1 == len(steps):
                return [value, got]
            value = call(add_kernel, shape(value.shape, BF16), small // 8, value, got)

    first_part = terms(first_part, doubling)
    second_part = terms(second_part, doubling[::-1])
    gram = call(add_kernel, shape((3 * rank, rank), BF16), small // 8, *first_part)
    down_t, stack = call(
        prepare_kernel,
        [shape((rank, features), BF16), shape((4 * rank + half, features), BF16)],
        small,
        down, head, up, down2, up2, gains2, states,
    )
    gram2 = from_partner(gram, "section", 1)
    made, theirs = call(
        functools.partial(chain_kernel, width, len(first_part)),
        [shape((6 * half, rank), BF16)] * 2,
        16 * 2 * half * rank * rank,
        *first_part, *second_part, gram, gram2, labels, valid,
    )
    met = from_partner(theirs, "section", 1)
    mixes, acc, left = call(
        functools.partial(mine_kernel, near),
        [shape((4 * rank, rank), F32), shape((rank + len(near) * slim, features), F32), shape((2 * rank, half), BF16)],
        4 * small,
        made, states,
    )
    away, grad, wide, tail, _ = call(
        functools.partial(down_kernel, replicas, far),
        [
            shape((8 * slim + PACK, rank), BF16),
            shape((rank, features), BF16),
            shape((rank, 5 * rank), BF16),
            shape((PACK, rank), BF16),
            shape((8 * rank, rank), BF16),
        ],
        8 * small,
        met, mixes, acc, left, stack, down_t, gains, valid,
    )
    away = from_partner(away, "dp", far)
    *parts, = call(
        functools.partial(up_kernel, replicas, near),
        [shape((lines * 2 * slim + PACK, rank), BF16)] * len(near),
        8 * small,
        acc, grad, wide, tail, stack,
    )
    for i, step in enumerate(near):
        if step > 0:
            parts[i] = from_partner(parts[i], "dp", step)
    cross = from_partner(sent, "section", 1)
    moved = call(
        far_kernel, shape((2 * slim, features), F32), 2 * small, away, sent, cross, stack, gains
    )
    down_grad, up_grad, gain_grad = call(
        last_kernel,
        [shape((slim, features), F32), shape((slim, features), F32), shape((1, features), F32)],
        small,
        *parts, away, moved,
    )
    return down_grad.T[None], up_grad[None], gain_grad


def solution(mesh):
    return jax.shard_map(
        local,
        mesh=mesh,
        in_specs=(
            P(None, "dp", "tensor"),
            P("section", "tensor", None),
            P("section", None, "tensor"),
            P("section", "tensor"),
            P("tensor", None),
            P(None, "dp"),
            P(None, "dp"),
        ),
        out_specs=(
            P("section", "tensor", "dp"),
            P("section", "dp", "tensor"),
            P("section", "tensor"),
        ),
        check_vma=False,
    )
```
